256 devices in a mesh: spin: 2 (over core), band: 16 (over x, z_hi), grid: 8 (over z_lo, y).
Axes of the slice: x: 4, y: 4, z: 8 (z_hi: 4, z_lo: 2; z = z_hi * 2 + z_lo), core: 2. Of those that a mesh axis runs over, the one named last changes fastest.
Arguments:
- orbitals: bfloat16 [2, 128, 128, 128, 128], P('spin', 'band', 'grid'), may hold values from -0.14941406 to 0.14941406
- partial_bands: int32 [2, 2], P('spin'), may hold values from 0 to 127
- core_density: float32 [128, 128, 128], P('grid'), may hold values from 0.002 to 0.2
Outputs:
- potential: float32 [2, 128, 128, 128], P('spin', 'grid', 'band')
The draws below stay inside these ranges and needn't reach their ends.
Inputs may be any that keep to these rules, and one draw needn't show every extreme that they name: `partial_bands`: row s holds, for spin s, the first half-occupied band and the count of half-occupied bands; bands past 128 - 1 do not exist.
All inputs are finite; a program needn't handle non-finite values.
Results may differ from the reference program's by a relative error of at most 0.0003.
Values sent between devices are 32-bit elements; how exact they have to be, the bound alone decides.
A program may use at most 128 MiB of HBM per device.

```python
import math
import jax
import jax.numpy as jnp
from jax import lax

NX = 128
NY = 128
NZ = 128
SPINS = 2
BANDS = 128


def set_ends(drawn, own_key, smallest, high):
    extent = drawn.shape
    spot = [jax.random.randint(jax.random.fold_in(own_key, axis), (), 0, extent[axis]) for axis in range(len(extent))]
    drawn = drawn.at[tuple(spot)].set(smallest)
    longest = extent.index(max(extent))
    spot[longest] = (spot[longest] + 1) % extent[longest]
    return drawn.at[tuple(spot)].set(high)


def shard_levels(own_key, shape, pieces, least, top_value):
    def one(axis_at, parts):
        steps = jax.random.uniform(jax.random.fold_in(jax.random.fold_in(own_key, 6), axis_at), (parts,), jnp.float32, least / len(pieces), top_value / len(pieces))
        return jnp.repeat(jnp.exp(steps), shape[axis_at] // parts).reshape((-1,) + (1,) * (len(shape) - axis_at - 1))

    factor_of = one(*pieces[0])
    for cut in pieces[1:]:
        factor_of = factor_of * one(*cut)
    return factor_of


def noise(key, shape, scale, reach, cuts=(), kind=jnp.bfloat16):
    drawn = scale * jax.random.normal(key, shape, jnp.float32)
    if cuts:
        drawn = drawn * shard_levels(key, shape, cuts, -0.22, 0.18)
    return jnp.clip(drawn, -reach, reach).astype(kind)


def setup_inputs(seed: int = 0) -> dict:
    arg_keys = jax.random.split(jax.random.key(seed), 4)
    return {
        "orbitals": noise(arg_keys[0], (SPINS, BANDS, NX, NY, NZ), 0.025, 0.14941406, ((0, 2), (1, 16), (2, 8))),
        "partial_bands": set_ends(jax.random.randint(arg_keys[1], (SPINS, 2), 0, BANDS), jax.random.fold_in(arg_keys[1], 1), 0, BANDS - 1).astype(jnp.int32),
        "core_density": jnp.clip(jnp.exp(math.log(0.2) - 4.6051702 * jax.random.uniform(arg_keys[2], (NX, NY, NZ), jnp.float32) ** shard_levels(arg_keys[2], (NX, NY, NZ), ((0, 8),), -0.2, 0.2)), 0.002, 0.2),
    }


KAPPA = 0.804
MU_X = 0.2195149727645171
BETA = 0.06672455060314922
GAMMA = (1.0 - math.log(2.0)) / math.pi ** 2
FZ_NORM = 2.0 ** (4.0 / 3.0) - 2.0
FPP_ZERO = 1.709921

def pw_fit(radius, amp, alpha, beta_one, beta_two, beta_three, beta_four):
    root = jnp.sqrt(radius)
    denom = 2.0 * amp * (beta_one * root + beta_two * radius + beta_three * radius * root + beta_four * radius * radius)
    return -2.0 * amp * (1.0 + alpha * radius) * jnp.log(1.0 + 1.0 / denom)

def exchange_part(double, sigma_four):
    kfermi = (3.0 * math.pi ** 2 * double) ** (1.0 / 3.0)
    scaled = sigma_four / (4.0 * kfermi * kfermi * double * double)
    enhance = 1.0 + KAPPA - KAPPA / (1.0 + MU_X * scaled / KAPPA)
    return -0.75 / math.pi * kfermi * double * enhance

def xc_energy(n_up, n_down, s_uu, s_ud, s_dd):
    exch = 0.5 * (exchange_part(2.0 * n_up, 4.0 * s_uu) + exchange_part(2.0 * n_down, 4.0 * s_dd))
    total = n_up + n_down
    zeta = (n_up - n_down) / total
    radius = (3.0 / (4.0 * math.pi * total)) ** (1.0 / 3.0)
    ec_para = pw_fit(radius, 0.031091, 0.2137, 7.5957, 3.5876, 1.6382, 0.49294)
    ec_ferro = pw_fit(radius, 0.015545, 0.20548, 14.1189, 6.1977, 3.3662, 0.62517)
    neg_stiff = pw_fit(radius, 0.016887, 0.11125, 10.357, 3.6231, 0.88026, 0.49671)
    plus_z = 1.0 + zeta
    minus_z = 1.0 - zeta
    fzeta = (plus_z ** (4.0 / 3.0) + minus_z ** (4.0 / 3.0) - 2.0) / FZ_NORM
    zeta_four = zeta ** 4
    ec_lda = ec_para - neg_stiff * fzeta / FPP_ZERO * (1.0 - zeta_four) + (ec_ferro - ec_para) * fzeta * zeta_four
    phi = 0.5 * (plus_z ** (2.0 / 3.0) + minus_z ** (2.0 / 3.0))
    phi_cube = phi * phi * phi
    kfermi = (3.0 * math.pi ** 2 * total) ** (1.0 / 3.0)
    screen_sq = 4.0 * kfermi / math.pi
    sigma = s_uu + 2.0 * s_ud + s_dd
    tsq = sigma / (4.0 * phi * phi * screen_sq * total * total)
    amp = BETA / GAMMA / (jnp.exp(-ec_lda / (GAMMA * phi_cube)) - 1.0)
    atsq = amp * tsq
    gradient_term = GAMMA * phi_cube * jnp.log(1.0 + BETA / GAMMA * tsq * (1.0 + atsq) / (1.0 + atsq + atsq * atsq))
    return exch + total * (ec_lda + gradient_term)

def spectral(field, axis):
    length = field.shape[axis]
    index = jnp.arange(length, dtype=jnp.int32)
    mode = jnp.where(index < length // 2, index, index - length)
    mode = jnp.where(index == length // 2, 0, mode)
    wave = 2.0 * math.pi / length * mode.astype(jnp.float32)
    shape = [1, 1, 1]
    shape[axis] = length
    spec = jnp.fft.fft(field, axis=axis)
    return jnp.real(jnp.fft.ifft(spec * (1j * wave.reshape(shape)), axis=axis)).astype(jnp.float32)

def reference(orbitals, partial_bands, core_density):
    band_ids = jnp.arange(BANDS, dtype=jnp.int32)

    def spin_density(spin_id):
        first = partial_bands[spin_id, 0]
        span = partial_bands[spin_id, 1]
        weights = jnp.where((band_ids >= first) & (band_ids < first + span), 0.5, 1.0).astype(jnp.float32)

        def accumulate(total, item):
            weight, orbital = item
            values = orbital.astype(jnp.float32)
            return (total + weight * values * values, None)
        start = jnp.zeros((NX, NY, NZ), jnp.float32)
        total, unused = lax.scan(accumulate, start, (weights, orbitals[spin_id]))
        return total + 0.5 * core_density
    dens_up = spin_density(0)
    dens_down = spin_density(1)
    grad_up = [spectral(dens_up, axis) for axis in range(3)]
    grad_down = [spectral(dens_down, axis) for axis in range(3)]
    s_uu = grad_up[0] * grad_up[0] + grad_up[1] * grad_up[1] + grad_up[2] * grad_up[2]
    s_ud = grad_up[0] * grad_down[0] + grad_up[1] * grad_down[1] + grad_up[2] * grad_down[2]
    s_dd = grad_down[0] * grad_down[0] + grad_down[1] * grad_down[1] + grad_down[2] * grad_down[2]
    energy, pull = jax.vjp(xc_energy, dens_up, dens_down, s_uu, s_ud, s_dd)
    derivs = pull(jnp.ones_like(energy))
    div_up = jnp.zeros_like(dens_up)
    div_down = jnp.zeros_like(dens_up)
    for axis in range(3):
        flux_up = 2.0 * derivs[2] * grad_up[axis] + derivs[3] * grad_down[axis]
        flux_down = 2.0 * derivs[4] * grad_down[axis] + derivs[3] * grad_up[axis]
        div_up = div_up + spectral(flux_up, axis)
        div_down = div_down + spectral(flux_down, axis)
    return jnp.stack([derivs[0] - div_up, derivs[1] - div_down])
```

```python
import math

import jax
import jax.numpy as jnp
import numpy as np
from jax import lax
from jax.experimental import pallas as pl
from jax.experimental.pallas import tpu as pltpu
from jax.sharding import PartitionSpec as P

KAPPA = 0.804
MU_X = 0.2195149727645171
BETA = 0.06672455060314922
GAMMA = (1.0 - math.log(2.0)) / math.pi**2
FZ_NORM = 2.0 ** (4.0 / 3.0) - 2.0
FPP_ZERO = 1.709921

MESH = pl.DeviceIdType.MESH
F32 = jnp.float32
N = 128
XR = 16
NX4 = 4
NZ4 = 4
BAND = NX4 * NZ4
GRID = 8
YB = N // BAND
YQ = N // NX4
CH = 4
CR = XR // CH
HR = CR // 2


def derivative_matrix():
    j = np.arange(N)
    k = j[:, None] - j[None, :]
    ang = np.where(k == 0, 1.0, np.pi * k / N)
    sign = np.where(k % 2 == 0, 1.0, -1.0)
    half = np.pi / N
    return np.where(k == 0, 0.0, half * sign / np.tan(ang)).astype(np.float32)


def pw_fit(r, root, amp, alpha, b1, b2, b3, b4):
    denom = (2.0 * amp) * (root * (b1 + root * (b2 + root * (b3 + root * b4))))
    slope = (2.0 * amp) * (0.5 * b1 / root + (b2 + root * (1.5 * b3 + root * (2.0 * b4))))
    log = jnp.log(1.0 + 1.0 / denom)
    front = (-2.0 * amp) * (1.0 + alpha * r)
    value = front * log
    deriv = (-2.0 * amp * alpha) * log - front * slope / (denom * (denom + 1.0))
    return value, deriv


def cbrt(x):
    return jnp.exp(jnp.log(x) * (1.0 / 3.0))


def xc_derivs(own, other, s_own, s_mix, s_other):
    total = own + other
    inv_n = 1.0 / total
    c_own = cbrt(own)
    c_other = cbrt(other)
    c_tot = cbrt(total)
    inv_c = 1.0 / c_tot
    double = 2.0 * own
    kf = (6.0 * math.pi**2) ** (1.0 / 3.0) * c_own
    inv_kn = 1.0 / (kf * double)
    s2 = s_own * inv_kn * inv_kn
    inv_den = 1.0 / (1.0 + (MU_X / KAPPA) * s2)
    enh = (1.0 + KAPPA) - KAPPA * inv_den
    enh_d = MU_X * inv_den * inv_den
    dn_x = (-1.0 / math.pi) * kf * (enh - 2.0 * s2 * enh_d)
    ds_x = (-3.0 / (8.0 * math.pi)) * enh_d * inv_kn
    two13 = 2.0 ** (1.0 / 3.0)
    plus = double * inv_n
    minus = 2.0 * other * inv_n
    zeta = (own - other) * inv_n
    plus13 = two13 * c_own * inv_c
    minus13 = two13 * c_other * inv_c
    radius = (3.0 / (4.0 * math.pi)) ** (1.0 / 3.0) * inv_c
    root = jnp.sqrt(radius)
    ec0, ec0_r = pw_fit(radius, root, 0.031091, 0.2137, 7.5957, 3.5876, 1.6382, 0.49294)
    ec1, ec1_r = pw_fit(radius, root, 0.015545, 0.20548, 14.1189, 6.1977, 3.3662, 0.62517)
    ac, ac_r = pw_fit(radius, root, 0.016887, 0.11125, 10.357, 3.6231, 0.88026, 0.49671)
    fz = (plus * plus13 + minus * minus13 - 2.0) * (1.0 / FZ_NORM)
    fz_d = (4.0 / 3.0 / FZ_NORM) * (plus13 - minus13)
    z2 = zeta * zeta
    z3 = z2 * zeta
    z4 = z2 * z2
    w1 = (-1.0 / FPP_ZERO) * (1.0 - z4)
    diff = ec1 - ec0
    mix = ac * w1 + diff * z4
    ec = ec0 + fz * mix
    ec_r = ec0_r + fz * (ac_r * w1 + (ec1_r - ec0_r) * z4)
    ec_z = fz_d * mix + 4.0 * z3 * fz * (ac * (1.0 / FPP_ZERO) + diff)
    phi = 0.5 * (plus13 * plus13 + minus13 * minus13)
    phi_d = (1.0 / 3.0) * (1.0 / plus13 - 1.0 / minus13)
    inv_phi = 1.0 / phi
    phi3 = phi * phi * phi
    kf_tot = (3.0 * math.pi**2) ** (1.0 / 3.0)
    tfac = (math.pi / (16.0 * kf_tot)) * inv_phi * inv_phi * inv_c * inv_n * inv_n
    sigma = s_own + 2.0 * s_mix + s_other
    t2 = sigma * tfac
    inv_gp3 = (1.0 / GAMMA) * inv_phi * inv_phi * inv_phi
    ex = jnp.exp(-ec * inv_gp3)
    amp = (BETA / GAMMA) / (ex - 1.0)
    y = amp * t2
    den = 1.0 + y + y * y
    inv_d = 1.0 / den
    ct = (BETA / GAMMA) * t2
    q = ct * (1.0 + y) * inv_d
    grad_h = GAMMA * phi3 * jnp.log(1.0 + q)
    scale = GAMMA * phi3 / (1.0 + q) * inv_d * inv_d
    h_t = scale * ((BETA / GAMMA) * (1.0 + 2.0 * y))
    h_a = -scale * (ct * t2) * (y * (2.0 + y))
    h_ec = h_a * (amp * amp * ex * (GAMMA / BETA) * inv_gp3)
    h_phi = inv_phi * (3.0 * (grad_h - ec * h_ec) - 2.0 * t2 * h_t)
    one_ec = 1.0 + h_ec
    e_n = ec + grad_h - (1.0 / 3.0) * radius * ec_r * one_ec - (7.0 / 3.0) * t2 * h_t
    e_z = ec_z * one_ec + phi_d * h_phi
    dn = dn_x + e_n + e_z * minus
    ds_c = total * h_t * tfac
    return dn, ds_x + ds_c, 2.0 * ds_c


def kernel(
    orb_hbm, bands_ref, core_hbm, dmat_ref, out_ref,
    orb, part, core, x_in, x_out, summed, z_in,
    dens, dens_o, grad, grad_o, flux, turned, x_line, x_res, x_back, y_line, y_res, y_back,
    orb_sem, core_sem, xs_sem, xr_sem, zs_sem, zr_sem, ps_sem, pr_sem, ys_sem, yr_sem, gs_sem, gr_sem,
):
    spin = lax.axis_index("spin")
    band = lax.axis_index("band")
    grid = lax.axis_index("grid")
    bx = band // NZ4
    bz = lax.rem(band, NZ4)
    sends = []

    def at_band(x, z):
        return (spin, lax.rem(x, NX4) * NZ4 + lax.rem(z, NZ4), grid)

    def copy(src, dst, send_sem, recv_sem, device):
        return pltpu.make_async_remote_copy(
            src_ref=src, dst_ref=dst, send_sem=send_sem, recv_sem=recv_sem,
            device_id=device, device_id_type=MESH,
        )

    def send(*args):
        c = copy(*args)
        c.start()
        sends.append(c)

    def arrived(dst, recv_sem):
        copy(dst, dst, recv_sem, recv_sem, (spin, band, grid)).wait_recv()

    order = (2, 1, 3, 0)

    def y_of(r):
        return pl.multiple_of(lax.rem(bx + r, NX4) * YQ, YQ)

    def load(c, r):
        window = (slice(None), pl.ds(c * CR, CR), pl.ds(y_of(r), YQ), slice(None))
        return pltpu.make_async_copy(
            orb_hbm.at[(0, *window)], orb.at[:, pl.ds(c * CR, CR), pl.ds(r * YQ, YQ), :],
            orb_sem.at[c, r],
        )

    for c in range(CH):
        for r in order:
            load(c, r).start()
    y_own = pl.multiple_of(band * YB, YB)
    core_copy = pltpu.make_async_copy(core_hbm.at[:, pl.ds(y_own, YB), :], core, core_sem)
    core_copy.start()

    barrier = pltpu.get_barrier_semaphore()
    peers = [at_band(bx + 1, bz), at_band(bx + 3, bz)]
    peers += [at_band(bx, bz + d) for d in (1, 2, 3)]
    peers += [(spin, band, lax.rem(grid + d, GRID)) for d in range(1, GRID)]
    peers += [(1 - spin, band, grid)]
    for peer in peers:
        pl.semaphore_signal(barrier, inc=1, device_id=peer, device_id_type=MESH)

    first = bands_ref[0, 0]
    last = first + bands_ref[0, 1]
    weights = []
    for b in range(8):
        ident = band * 8 + b
        weights.append(jnp.where((ident >= first) & (ident < last), 0.5, 1.0).astype(F32))

    def density(c, r):
        load(c, r).wait()
        rows, ys = slice(c * CR, (c + 1) * CR), slice(r * YQ, (r + 1) * YQ)
        acc = None
        for b in range(8):
            v = orb[b, rows, ys, :].astype(F32)
            term = weights[b] * (v * v)
            acc = term if acc is None else acc + term
        part[r, rows] = acc

    plus, minus = at_band(bx + 1, bz), at_band(bx + 3, bz)

    def half(c, h):
        return pl.ds(c * CR + h * HR, HR)

    def x_send(stream, c, src):
        target = minus if stream % 2 else plus
        send(src, x_in.at[stream, c], xs_sem.at[stream, c], xr_sem.at[stream, c], target)

    def far(c):
        density(c, 2)
        x_send(0, c, part.at[2, half(c, 0)])
        x_send(1, c, part.at[2, half(c, 1)])

    def direct(c):
        density(c, 1)
        x_send(2, c, part.at[1, half(c, 1)])
        density(c, 3)
        x_send(3, c, part.at[3, half(c, 0)])

    def relay(c):
        for side, r in ((0, 1), (1, 3)):
            arrived(x_in.at[side, c], xr_sem.at[side, c])
            x_out[side, c] = part[r, half(c, side)] + x_in[side, c]
            x_send(4 + side, c, x_out.at[side, c])

    def finish(c):
        density(c, 0)
        for stream in (2, 3, 4, 5):
            arrived(x_in.at[stream, c], xr_sem.at[stream, c])
        summed[half(c, 0)] = part[0, half(c, 0)] + x_in[4, c] + x_in[3, c]
        summed[half(c, 1)] = part[0, half(c, 1)] + x_in[5, c] + x_in[2, c]
        rows = pl.ds(c * CR, CR)
        for d in (2, 1, 3):
            z = lax.rem(bz + d, NZ4)
            ys = pl.ds(pl.multiple_of(z * YB, YB), YB)
            send(
                summed.at[rows, ys, :], z_in.at[d, rows], zs_sem.at[c, d], zr_sem.at[c, d],
                at_band(bx, z),
            )

    far_first = True
    density(0, 2)
    pl.semaphore_wait(barrier, len(peers))
    x_send(0, 0, part.at[2, half(0, 0)])
    x_send(1, 0, part.at[2, half(0, 1)])
    direct(0)
    far(1)
    relay(0)
    for c in range(1, CH):
        direct(c)
        if c + 1 < CH:
            far(c + 1)
        relay(c)
        finish(c - 1)
    finish(CH - 1)

    y_mine = pl.ds(pl.multiple_of(bz * YB, YB), YB)
    core_copy.wait()
    base = summed[:, y_mine, :] + 0.5 * core[...]
    for c in range(CH):
        for d in (1, 2, 3):
            arrived(z_in.at[d, pl.ds(c * CR, CR)], zr_sem.at[c, d])
    own = base + z_in[1] + z_in[2] + z_in[3]
    dens[...] = own.reshape(N, N)

    partner = (1 - spin, band, grid)
    offsets = [(dx, dz) for dx in (2, 1, 3, 0) for dz in (2, 1, 3, 0) if (dx, dz) != (0, 0)]
    g_offsets = (3, 5, 2, 6, 1, 7, 4)

    def dot(a, b):
        return jnp.dot(a, b, precision=lax.Precision.HIGHEST, preferred_element_type=F32)

    def band_rows(b):
        return pl.ds(pl.multiple_of(b * YB, YB), YB)

    def grid_rows(g):
        return pl.ds(pl.multiple_of(g * XR, XR), XR)

    def y_exchange(src, dst, k):
        for dx, dz in offsets:
            d = dx * NZ4 + dz
            p = lax.rem(bx + dx, NX4) * NZ4 + lax.rem(bz + dz, NZ4)
            send(
                src.at[band_rows(p), :], dst.at[band_rows(band), :],
                ys_sem.at[k, d], yr_sem.at[k, d], (spin, p, grid),
            )
        dst[band_rows(band), :] = src[band_rows(band), :]

    def y_wait(dst, k):
        for dx, dz in offsets:
            d = dx * NZ4 + dz
            p = lax.rem(bx + NX4 - dx, NX4) * NZ4 + lax.rem(bz + NZ4 - dz, NZ4)
            arrived(dst.at[band_rows(p), :], yr_sem.at[k, d])

    def x_exchange(src, dst, k):
        for d in g_offsets:
            g = lax.rem(grid + d, GRID)
            send(
                src.at[grid_rows(g), :], dst.at[grid_rows(grid), :],
                gs_sem.at[k, d], gr_sem.at[k, d], (spin, band, g),
            )
        dst[grid_rows(grid), :] = src[grid_rows(grid), :]

    def x_wait(dst, k):
        for d in g_offsets:
            arrived(dst.at[grid_rows(lax.rem(grid + GRID - d, GRID)), :], gr_sem.at[k, d])

    def turn(src, dst):
        for i in range(YB):
            dst[i * XR : (i + 1) * XR, :] = src[pl.ds(i, XR, stride=YB), :]

    def turned_back(ref, xr):
        return ref[pl.ds(xr, YB, stride=XR), :]

    dmat = dmat_ref[...]

    def pencils(y_src, x_src, k):
        y_exchange(y_src, y_line.at[k], 2 * k)
        turn(x_src, turned.at[k])
        x_exchange(turned.at[k], x_line.at[k], 2 * k)

    def lines_x(k):
        x_wait(x_line.at[k], 2 * k)
        x_res[k] = dot(dmat, x_line[k])
        x_exchange(x_res.at[k], x_back.at[k], 2 * k + 1)

    def lines_y(k):
        y_wait(y_line.at[k], 2 * k)
        y_res[k] = dot(dmat, y_line[k])
        y_exchange(y_res.at[k], y_back.at[k], 2 * k + 1)

    pencils(dens, dens, 0)
    send(dens, dens_o, ps_sem.at[0], pr_sem.at[0], partner)
    grad[2] = -dot(dens[...], dmat)
    send(grad.at[2], grad_o.at[2], ps_sem.at[1], pr_sem.at[1], partner)
    lines_x(0)
    lines_y(0)
    x_wait(x_back.at[0], 1)
    for i in range(XR):
        grad[0, i * YB : (i + 1) * YB, :] = turned_back(x_back.at[0], i)
    send(grad.at[0], grad_o.at[0], ps_sem.at[2], pr_sem.at[2], partner)
    y_wait(y_back.at[0], 1)
    send(y_back.at[0], grad_o.at[1], ps_sem.at[3], pr_sem.at[3], partner)
    arrived(dens_o, pr_sem.at[0])
    arrived(grad_o.at[2], pr_sem.at[1])
    arrived(grad_o.at[0], pr_sem.at[2])
    arrived(grad_o.at[1], pr_sem.at[3])

    step = 16
    for i in range(0, N, step):
        rows = slice(i, i + step)
        g = (grad[0, rows, :], y_back[0, rows, :], grad[2, rows, :])
        h = (grad_o[0, rows, :], grad_o[1, rows, :], grad_o[2, rows, :])
        s_own = g[0] * g[0] + g[1] * g[1] + g[2] * g[2]
        s_mix = g[0] * h[0] + g[1] * h[1] + g[2] * h[2]
        s_other = h[0] * h[0] + h[1] * h[1] + h[2] * h[2]
        dn, ds, dm = xc_derivs(dens[rows, :], dens_o[rows, :], s_own, s_mix, s_other)
        for a in range(3):
            flux[a, rows, :] = 2.0 * ds * g[a] + dm * h[a]
        flux[3, rows, :] = dn

    pencils(flux.at[1], flux.at[0], 1)
    flux[3] = flux[3] + dot(flux[2], dmat)
    lines_x(1)
    lines_y(1)
    x_wait(x_back.at[1], 3)
    for i in range(XR):
        rows = slice(i * YB, (i + 1) * YB)
        flux[3, rows, :] = flux[3, rows, :] - turned_back(x_back.at[1], i)
    y_wait(y_back.at[1], 3)
    out_ref[0] = (flux[3] - y_back[1]).reshape(XR, YB, N)
    for c in sends:
        c.wait_send()


def per_device(orbitals, partial_bands, core_density, dmat):
    vm = pltpu.VMEM
    sem = pltpu.SemaphoreType.DMA
    anyspace = pl.BlockSpec(memory_space=pl.ANY)
    return pl.pallas_call(
        kernel,
        out_shape=jax.ShapeDtypeStruct((1, XR, YB, N), F32),
        in_specs=[
            anyspace,
            pl.BlockSpec(memory_space=pltpu.SMEM),
            anyspace,
            pl.BlockSpec(memory_space=pltpu.VMEM),
        ],
        out_specs=pl.BlockSpec(memory_space=pltpu.VMEM),
        scratch_shapes=[
            vm((8, XR, N, N), jnp.bfloat16),
            vm((NX4, XR, YQ, N), F32),
            vm((XR, YB, N), F32),
            vm((6, CH, HR, YQ, N), F32),
            vm((2, CH, HR, YQ, N), F32),
            vm((XR, YQ, N), F32),
            vm((NZ4, XR, YB, N), F32),
            vm((N, N), F32),
            vm((N, N), F32),
            vm((3, N, N), F32),
            vm((3, N, N), F32),
            vm((4, N, N), F32),
            vm((2, N, N), F32),
            vm((2, N, N), F32),
            vm((2, N, N), F32),
            vm((2, N, N), F32),
            vm((2, N, N), F32),
            vm((2, N, N), F32),
            vm((2, N, N), F32),
            sem((CH, NX4)),
            sem,
            sem((6, CH)),
            sem((6, CH)),
            sem((CH, NZ4)),
            sem((CH, NZ4)),
            sem((4,)),
            sem((4,)),
            sem((4, BAND)),
            sem((4, BAND)),
            sem((4, GRID)),
            sem((4, GRID)),
        ],
        compiler_params=pltpu.CompilerParams(collective_id=0, has_side_effects=True),
    )(orbitals, partial_bands, core_density, dmat)


def solution(mesh):
    in_specs = (P("spin", "band", "grid", None, None), P("spin", None), P("grid", None, None))
    out_specs = P("spin", "grid", "band", None)

    def step(orbitals, partial_bands, core_density):
        dmat = jnp.asarray(derivative_matrix())
        return jax.shard_map(
            per_device, mesh=mesh, in_specs=(*in_specs, P(None, None)), out_specs=out_specs,
            check_vma=False,
        )(orbitals, partial_bands, core_density, dmat)

    return step
```

```python
import math

import jax
import jax.numpy as jnp
import numpy as np
from jax import lax
from jax.experimental import pallas as pl
from jax.experimental.pallas import tpu as pltpu
from jax.sharding import PartitionSpec as P

KAPPA = 0.804
MU_X = 0.2195149727645171
BETA = 0.06672455060314922
GAMMA = (1.0 - math.log(2.0)) / math.pi**2
FZ_NORM = 2.0 ** (4.0 / 3.0) - 2.0
FPP_ZERO = 1.709921

MESH = pl.DeviceIdType.MESH
F32 = jnp.float32
N = 128
XR = 16
NX4 = 4
NZ4 = 4
BAND = NX4 * NZ4
GRID = 8
YB = N // BAND
YQ = N // NX4
CH = 4
CR = XR // CH
HR = CR // 2


def derivative_matrix():
    j = np.arange(N)
    k = j[:, None] - j[None, :]
    ang = np.where(k == 0, 1.0, np.pi * k / N)
    sign = np.where(k % 2 == 0, 1.0, -1.0)
    half = np.pi / N
    return np.where(k == 0, 0.0, half * sign / np.tan(ang)).astype(np.float32)


def pw_fit(r, root, amp, alpha, b1, b2, b3, b4):
    denom = (2.0 * amp) * (root * (b1 + root * (b2 + root * (b3 + root * b4))))
    slope = (2.0 * amp) * (0.5 * b1 / root + (b2 + root * (1.5 * b3 + root * (2.0 * b4))))
    log = jnp.log(1.0 + 1.0 / denom)
    front = (-2.0 * amp) * (1.0 + alpha * r)
    value = front * log
    deriv = (-2.0 * amp * alpha) * log - front * slope / (denom * (denom + 1.0))
    return value, deriv


def cbrt(x):
    return jnp.exp(jnp.log(x) * (1.0 / 3.0))


def xc_derivs(own, other, s_own, s_mix, s_other):
    total = own + other
    inv_n = 1.0 / total
    c_own = cbrt(own)
    c_other = cbrt(other)
    c_tot = cbrt(total)
    inv_c = 1.0 / c_tot
    double = 2.0 * own
    kf = (6.0 * math.pi**2) ** (1.0 / 3.0) * c_own
    inv_kn = 1.0 / (kf * double)
    s2 = s_own * inv_kn * inv_kn
    inv_den = 1.0 / (1.0 + (MU_X / KAPPA) * s2)
    enh = (1.0 + KAPPA) - KAPPA * inv_den
    enh_d = MU_X * inv_den * inv_den
    dn_x = (-1.0 / math.pi) * kf * (enh - 2.0 * s2 * enh_d)
    ds_x = (-3.0 / (8.0 * math.pi)) * enh_d * inv_kn
    two13 = 2.0 ** (1.0 / 3.0)
    plus = double * inv_n
    minus = 2.0 * other * inv_n
    zeta = (own - other) * inv_n
    plus13 = two13 * c_own * inv_c
    minus13 = two13 * c_other * inv_c
    radius = (3.0 / (4.0 * math.pi)) ** (1.0 / 3.0) * inv_c
    root = jnp.sqrt(radius)
    ec0, ec0_r = pw_fit(radius, root, 0.031091, 0.2137, 7.5957, 3.5876, 1.6382, 0.49294)
    ec1, ec1_r = pw_fit(radius, root, 0.015545, 0.20548, 14.1189, 6.1977, 3.3662, 0.62517)
    ac, ac_r = pw_fit(radius, root, 0.016887, 0.11125, 10.357, 3.6231, 0.88026, 0.49671)
    fz = (plus * plus13 + minus * minus13 - 2.0) * (1.0 / FZ_NORM)
    fz_d = (4.0 / 3.0 / FZ_NORM) * (plus13 - minus13)
    z2 = zeta * zeta
    z3 = z2 * zeta
    z4 = z2 * z2
    w1 = (-1.0 / FPP_ZERO) * (1.0 - z4)
    diff = ec1 - ec0
    mix = ac * w1 + diff * z4
    ec = ec0 + fz * mix
    ec_r = ec0_r + fz * (ac_r * w1 + (ec1_r - ec0_r) * z4)
    ec_z = fz_d * mix + 4.0 * z3 * fz * (ac * (1.0 / FPP_ZERO) + diff)
    phi = 0.5 * (plus13 * plus13 + minus13 * minus13)
    phi_d = (1.0 / 3.0) * (1.0 / plus13 - 1.0 / minus13)
    inv_phi = 1.0 / phi
    phi3 = phi * phi * phi
    kf_tot = (3.0 * math.pi**2) ** (1.0 / 3.0)
    tfac = (math.pi / (16.0 * kf_tot)) * inv_phi * inv_phi * inv_c * inv_n * inv_n
    sigma = s_own + 2.0 * s_mix + s_other
    t2 = sigma * tfac
    inv_gp3 = (1.0 / GAMMA) * inv_phi * inv_phi * inv_phi
    ex = jnp.exp(-ec * inv_gp3)
    amp = (BETA / GAMMA) / (ex - 1.0)
    y = amp * t2
    den = 1.0 + y + y * y
    inv_d = 1.0 / den
    ct = (BETA / GAMMA) * t2
    q = ct * (1.0 + y) * inv_d
    grad_h = GAMMA * phi3 * jnp.log(1.0 + q)
    scale = GAMMA * phi3 / (1.0 + q) * inv_d * inv_d
    h_t = scale * ((BETA / GAMMA) * (1.0 + 2.0 * y))
    h_a = -scale * (ct * t2) * (y * (2.0 + y))
    h_ec = h_a * (amp * amp * ex * (GAMMA / BETA) * inv_gp3)
    h_phi = inv_phi * (3.0 * (grad_h - ec * h_ec) - 2.0 * t2 * h_t)
    one_ec = 1.0 + h_ec
    e_n = ec + grad_h - (1.0 / 3.0) * radius * ec_r * one_ec - (7.0 / 3.0) * t2 * h_t
    e_z = ec_z * one_ec + phi_d * h_phi
    dn = dn_x + e_n + e_z * minus
    ds_c = total * h_t * tfac
    return dn, ds_x + ds_c, 2.0 * ds_c


def kernel(
    orb_hbm, bands_ref, core_hbm, dmat_hbm, out_ref,
    orb, dmat_ref, part, core, x_in, x_out, summed, z_in,
    dens, dens_o, grad, grad_o, flux, turned, x_line, x_res, x_back, y_line, y_res, y_back,
    orb_sem, core_sem, dmat_sem, xs_sem, xr_sem, zs_sem, zr_sem, ps_sem, pr_sem, ys_sem, yr_sem, gs_sem, gr_sem,
):
    spin = lax.axis_index("spin")
    band = lax.axis_index("band")
    grid = lax.axis_index("grid")
    bx = band // NZ4
    bz = lax.rem(band, NZ4)
    sends = []

    def at_band(x, z):
        return (spin, lax.rem(x, NX4) * NZ4 + lax.rem(z, NZ4), grid)

    def copy(src, dst, send_sem, recv_sem, device):
        return pltpu.make_async_remote_copy(
            src_ref=src, dst_ref=dst, send_sem=send_sem, recv_sem=recv_sem,
            device_id=device, device_id_type=MESH,
        )

    def send(*args):
        c = copy(*args)
        c.start()
        sends.append(c)

    def drain():
        for c in sends:
            c.wait_send()
        sends.clear()

    def arrived(dst, recv_sem):
        copy(dst, dst, recv_sem, recv_sem, (spin, band, grid)).wait_recv()

    order = (2, 1, 3, 0)

    def y_of(r):
        return pl.multiple_of(lax.rem(bx + r, NX4) * YQ, YQ)

    def load(c, r):
        window = (slice(None), pl.ds(c * CR, CR), pl.ds(y_of(r), YQ), slice(None))
        return pltpu.make_async_copy(
            orb_hbm.at[(0, *window)], orb.at[:, pl.ds(c * CR, CR), pl.ds(r * YQ, YQ), :],
            orb_sem.at[c, r],
        )

    for c in range(CH):
        for r in order:
            load(c, r).start()
    y_own = pl.multiple_of(band * YB, YB)
    core_copy = pltpu.make_async_copy(core_hbm.at[:, pl.ds(y_own, YB), :], core, core_sem)
    core_copy.start()
    dmat_copy = pltpu.make_async_copy(dmat_hbm, dmat_ref, dmat_sem)
    dmat_copy.start()

    barrier = pltpu.get_barrier_semaphore()
    peers = [at_band(bx + 1, bz), at_band(bx + 3, bz)]
    peers += [at_band(bx, bz + d) for d in (1, 2, 3)]
    peers += [(spin, band, lax.rem(grid + d, GRID)) for d in range(1, GRID)]
    peers += [(1 - spin, band, grid)]
    for peer in peers:
        pl.semaphore_signal(barrier, inc=1, device_id=peer, device_id_type=MESH)

    first = bands_ref[0, 0]
    last = first + bands_ref[0, 1]
    weights = []
    for b in range(8):
        ident = band * 8 + b
        weights.append(jnp.where((ident >= first) & (ident < last), 0.5, 1.0).astype(F32))

    def density(c, r):
        load(c, r).wait()
        rows, ys = slice(c * CR, (c + 1) * CR), slice(r * YQ, (r + 1) * YQ)
        acc = None
        for b in range(8):
            v = orb[b, rows, ys, :].astype(F32)
            term = weights[b] * (v * v)
            acc = term if acc is None else acc + term
        part[r, rows] = acc

    plus, minus = at_band(bx + 1, bz), at_band(bx + 3, bz)

    def half(c, h):
        return pl.ds(c * CR + h * HR, HR)

    def x_send(stream, c, src):
        target = minus if stream % 2 else plus
        send(src, x_in.at[stream, c], xs_sem.at[stream, c], xr_sem.at[stream, c], target)

    def far(c):
        x_send(0, c, part.at[2, half(c, 0)])
        x_send(1, c, part.at[2, half(c, 1)])

    def direct(c):
        density(c, 1)
        x_send(2, c, part.at[1, half(c, 1)])
        density(c, 3)
        x_send(3, c, part.at[3, half(c, 0)])

    def relay(c):
        for side, r in ((0, 1), (1, 3)):
            arrived(x_in.at[side, c], xr_sem.at[side, c])
            x_out[side, c] = part[r, half(c, side)] + x_in[side, c]
            x_send(4 + side, c, x_out.at[side, c])

    def finish(c):
        for stream in (2, 3, 4, 5):
            arrived(x_in.at[stream, c], xr_sem.at[stream, c])
        summed[half(c, 0)] = part[0, half(c, 0)] + x_in[4, c] + x_in[3, c]
        summed[half(c, 1)] = part[0, half(c, 1)] + x_in[5, c] + x_in[2, c]
        rows = pl.ds(c * CR, CR)
        for d in (2, 1, 3):
            z = lax.rem(bz + d, NZ4)
            ys = pl.ds(pl.multiple_of(z * YB, YB), YB)
            send(
                summed.at[rows, ys, :], z_in.at[d, rows], zs_sem.at[c, d], zr_sem.at[c, d],
                at_band(bx, z),
            )

    with jax.named_scope("first_piece"):
        density(0, 2)
    with jax.named_scope("barrier"):
        pl.semaphore_wait(barrier, len(peers))
    with jax.named_scope("rs_head"):
        for c in range(CH):
            if c:
                density(c, 2)
            far(c)
        direct(0)
    for c in range(CH):
        with jax.named_scope(f"relay{c}"):
            relay(c)
        if c + 1 < CH:
            direct(c + 1)
    for c in range(CH):
        density(c, 0)
    dmat_copy.wait()
    core_copy.wait()
    for c in range(CH):
        with jax.named_scope(f"finish{c}"):
            finish(c)

    y_mine = pl.ds(pl.multiple_of(bz * YB, YB), YB)
    base = summed[:, y_mine, :] + 0.5 * core[...]
    with jax.named_scope("z_wait"):
        for c in range(CH):
            for d in (1, 2, 3):
                arrived(z_in.at[d, pl.ds(c * CR, CR)], zr_sem.at[c, d])
    own = base + z_in[1] + z_in[2] + z_in[3]
    dens[...] = own.reshape(N, N)

    partner = (1 - spin, band, grid)
    offsets = [(dx, dz) for dx in (2, 1, 3, 0) for dz in (2, 1, 3, 0) if (dx, dz) != (0, 0)]
    g_offsets = (3, 5, 2, 6, 1, 7, 4)

    def dot(a, b):
        return jnp.dot(a, b, precision=lax.Precision.HIGHEST, preferred_element_type=F32)

    def band_rows(b):
        return pl.ds(pl.multiple_of(b * YB, YB), YB)

    def grid_rows(g):
        return pl.ds(pl.multiple_of(g * XR, XR), XR)

    def y_exchange(src, dst, k):
        for dx, dz in offsets:
            d = dx * NZ4 + dz
            p = lax.rem(bx + dx, NX4) * NZ4 + lax.rem(bz + dz, NZ4)
            send(
                src.at[band_rows(p), :], dst.at[band_rows(band), :],
                ys_sem.at[k, d], yr_sem.at[k, d], (spin, p, grid),
            )
        dst[band_rows(band), :] = src[band_rows(band), :]

    def y_wait(dst, k):
        for dx, dz in offsets:
            d = dx * NZ4 + dz
            p = lax.rem(bx + NX4 - dx, NX4) * NZ4 + lax.rem(bz + NZ4 - dz, NZ4)
            arrived(dst.at[band_rows(p), :], yr_sem.at[k, d])

    def x_exchange(src, dst, k):
        for d in g_offsets:
            g = lax.rem(grid + d, GRID)
            send(
                src.at[grid_rows(g), :], dst.at[grid_rows(grid), :],
                gs_sem.at[k, d], gr_sem.at[k, d], (spin, band, g),
            )
        dst[grid_rows(grid), :] = src[grid_rows(grid), :]

    def x_wait(dst, k):
        for d in g_offsets:
            arrived(dst.at[grid_rows(lax.rem(grid + GRID - d, GRID)), :], gr_sem.at[k, d])

    def turn(src, dst):
        for i in range(YB):
            dst[i * XR : (i + 1) * XR, :] = src[pl.ds(i, XR, stride=YB), :]

    def turned_back(ref, xr):
        return ref[pl.ds(xr, YB, stride=XR), :]

    dmat = dmat_ref[...]

    def pencils(y_src, x_src, k):
        y_exchange(y_src, y_line.at[k], 2 * k)
        turn(x_src, turned.at[k])
        x_exchange(turned.at[k], x_line.at[k], 2 * k)

    def lines_x(k):
        x_res[k] = dot(dmat, x_line[k])
        x_exchange(x_res.at[k], x_back.at[k], 2 * k + 1)

    def lines_y(k):
        y_res[k] = dot(dmat, y_line[k])
        y_exchange(y_res.at[k], y_back.at[k], 2 * k + 1)

    n_reduce = len(sends)
    with jax.named_scope("fwd0"):
        pencils(dens, dens, 0)
        send(dens, dens_o, ps_sem.at[0], pr_sem.at[0], partner)
        grad[2] = -dot(dens[...], dmat)
        send(grad.at[2], grad_o.at[2], ps_sem.at[1], pr_sem.at[1], partner)
    with jax.named_scope("drain0"):
        for c in sends[:n_reduce]:
            c.wait_send()
        del sends[:n_reduce]
    with jax.named_scope("x_wait0"):
        x_wait(x_line.at[0], 0)
    with jax.named_scope("x_lines0"):
        lines_x(0)
    with jax.named_scope("y_wait0"):
        y_wait(y_line.at[0], 0)
    with jax.named_scope("y_lines0"):
        lines_y(0)
    with jax.named_scope("x_back0"):
        x_wait(x_back.at[0], 1)
        for i in range(XR):
            grad[0, i * YB : (i + 1) * YB, :] = turned_back(x_back.at[0], i)
        send(grad.at[0], grad_o.at[0], ps_sem.at[2], pr_sem.at[2], partner)
    with jax.named_scope("y_back0"):
        y_wait(y_back.at[0], 1)
    with jax.named_scope("swap"):
        n_first = len(sends)
        send(y_back.at[0], grad_o.at[1], ps_sem.at[3], pr_sem.at[3], partner)
        arrived(dens_o, pr_sem.at[0])
        arrived(grad_o.at[2], pr_sem.at[1])
        arrived(grad_o.at[0], pr_sem.at[2])
        arrived(grad_o.at[1], pr_sem.at[3])

    with jax.named_scope("xc"):
        step = 16
        for i in range(0, N, step):
            rows = slice(i, i + step)
            g = (grad[0, rows, :], y_back[0, rows, :], grad[2, rows, :])
            h = (grad_o[0, rows, :], grad_o[1, rows, :], grad_o[2, rows, :])
            s_own = g[0] * g[0] + g[1] * g[1] + g[2] * g[2]
            s_mix = g[0] * h[0] + g[1] * h[1] + g[2] * h[2]
            s_other = h[0] * h[0] + h[1] * h[1] + h[2] * h[2]
            dn, ds, dm = xc_derivs(dens[rows, :], dens_o[rows, :], s_own, s_mix, s_other)
            for a in range(3):
                flux[a, rows, :] = 2.0 * ds * g[a] + dm * h[a]
            flux[3, rows, :] = dn

    with jax.named_scope("fwd1"):
        pencils(flux.at[1], flux.at[0], 1)
        flux[3] = flux[3] + dot(flux[2], dmat)
    with jax.named_scope("drain1"):
        for c in sends[:n_first]:
            c.wait_send()
        del sends[:n_first]
    with jax.named_scope("x_wait1"):
        x_wait(x_line.at[1], 2)
    with jax.named_scope("x_lines1"):
        lines_x(1)
    with jax.named_scope("y_wait1"):
        y_wait(y_line.at[1], 2)
    with jax.named_scope("y_lines1"):
        lines_y(1)
    with jax.named_scope("drain2"):
        drain()
    with jax.named_scope("x_back1"):
        x_wait(x_back.at[1], 3)
        for i in range(XR):
            rows = slice(i * YB, (i + 1) * YB)
            flux[3, rows, :] = flux[3, rows, :] - turned_back(x_back.at[1], i)
    with jax.named_scope("y_back1"):
        y_wait(y_back.at[1], 3)
    with jax.named_scope("tail"):
        out_ref[0] = (flux[3] - y_back[1]).reshape(XR, YB, N)
    with jax.named_scope("drain"):
        drain()


def per_device(orbitals, partial_bands, core_density, dmat):
    vm = pltpu.VMEM
    sem = pltpu.SemaphoreType.DMA
    anyspace = pl.BlockSpec(memory_space=pltpu.HBM)
    return pl.pallas_call(
        kernel,
        out_shape=jax.ShapeDtypeStruct((1, XR, YB, N), F32),
        in_specs=[
            anyspace,
            pl.BlockSpec(memory_space=pltpu.SMEM),
            anyspace,
            anyspace,
        ],
        out_specs=pl.BlockSpec(memory_space=pltpu.VMEM),
        scratch_shapes=[
            vm((8, XR, N, N), jnp.bfloat16),
            vm((N, N), F32),
            vm((NX4, XR, YQ, N), F32),
            vm((XR, YB, N), F32),
            vm((6, CH, HR, YQ, N), F32),
            vm((2, CH, HR, YQ, N), F32),
            vm((XR, YQ, N), F32),
            vm((NZ4, XR, YB, N), F32),
            vm((N, N), F32),
            vm((N, N), F32),
            vm((3, N, N), F32),
            vm((3, N, N), F32),
            vm((4, N, N), F32),
            vm((2, N, N), F32),
            vm((2, N, N), F32),
            vm((2, N, N), F32),
            vm((2, N, N), F32),
            vm((2, N, N), F32),
            vm((2, N, N), F32),
            vm((2, N, N), F32),
            sem((CH, NX4)),
            sem,
            sem,
            sem((6, CH)),
            sem((6, CH)),
            sem((CH, NZ4)),
            sem((CH, NZ4)),
            sem((4,)),
            sem((4,)),
            sem((4, BAND)),
            sem((4, BAND)),
            sem((4, GRID)),
            sem((4, GRID)),
        ],
        compiler_params=pltpu.CompilerParams(
            collective_id=0, has_side_effects=True, vmem_limit_bytes=60000 * 1024
        ),
    )(orbitals, partial_bands, core_density, dmat)


def solution(mesh):
    in_specs = (P("spin", "band", "grid", None, None), P("spin", None), P("grid", None, None))
    out_specs = P("spin", "grid", "band", None)

    def step(orbitals, partial_bands, core_density):
        dmat = jnp.asarray(derivative_matrix())
        return jax.shard_map(
            per_device, mesh=mesh, in_specs=(*in_specs, P(None, None)), out_specs=out_specs,
            check_vma=False,
        )(orbitals, partial_bands, core_density, dmat)

    return step
```

```python
import math

import jax
import jax.numpy as jnp
from jax import lax
from jax.experimental import pallas as pl
from jax.experimental.pallas import tpu as pltpu
from jax.sharding import PartitionSpec as P

KAPPA = 0.804
MU_X = 0.2195149727645171
BETA = 0.06672455060314922
GAMMA = (1.0 - math.log(2.0)) / math.pi**2
FZ_NORM = 2.0 ** (4.0 / 3.0) - 2.0
FPP_ZERO = 1.709921

MESH = pl.DeviceIdType.MESH
F32 = jnp.float32
N = 128
XR = 16
NX4 = 4
NZ4 = 4
BAND = NX4 * NZ4
GRID = 8
YB = N // BAND
YQ = N // NX4
CH = 4
CR = XR // CH
HR = CR // 2


def derivative_matrix():
    k = lax.broadcasted_iota(jnp.int32, (N, N), 0) - lax.broadcasted_iota(jnp.int32, (N, N), 1)
    far = jnp.abs(k)
    near = jnp.minimum(far, N - far)
    angle = (math.pi / N) * jnp.maximum(near, 1).astype(F32)
    size = (math.pi / N) * jnp.cos(angle) / jnp.sin(angle)
    flips = (k < 0).astype(jnp.int32) + (far > N // 2).astype(jnp.int32) + (far & 1)
    signed = jnp.where((flips & 1) == 1, -size, size)
    return jnp.where(k == 0, 0.0, signed)


def pw_fit(r, root, amp, alpha, b1, b2, b3, b4):
    denom = (2.0 * amp) * (root * (b1 + root * (b2 + root * (b3 + root * b4))))
    slope = (2.0 * amp) * (0.5 * b1 / root + (b2 + root * (1.5 * b3 + root * (2.0 * b4))))
    log = jnp.log(1.0 + 1.0 / denom)
    front = (-2.0 * amp) * (1.0 + alpha * r)
    value = front * log
    deriv = (-2.0 * amp * alpha) * log - front * slope / (denom * (denom + 1.0))
    return value, deriv


def cbrt(x):
    return jnp.exp(jnp.log(x) * (1.0 / 3.0))


def xc_derivs(own, other, s_own, s_mix, s_other):
    total = own + other
    inv_n = 1.0 / total
    c_own = cbrt(own)
    c_other = cbrt(other)
    c_tot = cbrt(total)
    inv_c = 1.0 / c_tot
    double = 2.0 * own
    kf = (6.0 * math.pi**2) ** (1.0 / 3.0) * c_own
    inv_kn = 1.0 / (kf * double)
    s2 = s_own * inv_kn * inv_kn
    inv_den = 1.0 / (1.0 + (MU_X / KAPPA) * s2)
    enh = (1.0 + KAPPA) - KAPPA * inv_den
    enh_d = MU_X * inv_den * inv_den
    dn_x = (-1.0 / math.pi) * kf * (enh - 2.0 * s2 * enh_d)
    ds_x = (-3.0 / (8.0 * math.pi)) * enh_d * inv_kn
    two13 = 2.0 ** (1.0 / 3.0)
    plus = double * inv_n
    minus = 2.0 * other * inv_n
    zeta = (own - other) * inv_n
    plus13 = two13 * c_own * inv_c
    minus13 = two13 * c_other * inv_c
    radius = (3.0 / (4.0 * math.pi)) ** (1.0 / 3.0) * inv_c
    root = jnp.sqrt(radius)
    ec0, ec0_r = pw_fit(radius, root, 0.031091, 0.2137, 7.5957, 3.5876, 1.6382, 0.49294)
    ec1, ec1_r = pw_fit(radius, root, 0.015545, 0.20548, 14.1189, 6.1977, 3.3662, 0.62517)
    ac, ac_r = pw_fit(radius, root, 0.016887, 0.11125, 10.357, 3.6231, 0.88026, 0.49671)
    fz = (plus * plus13 + minus * minus13 - 2.0) * (1.0 / FZ_NORM)
    fz_d = (4.0 / 3.0 / FZ_NORM) * (plus13 - minus13)
    z2 = zeta * zeta
    z3 = z2 * zeta
    z4 = z2 * z2
    w1 = (-1.0 / FPP_ZERO) * (1.0 - z4)
    diff = ec1 - ec0
    mix = ac * w1 + diff * z4
    ec = ec0 + fz * mix
    ec_r = ec0_r + fz * (ac_r * w1 + (ec1_r - ec0_r) * z4)
    ec_z = fz_d * mix + 4.0 * z3 * fz * (ac * (1.0 / FPP_ZERO) + diff)
    phi = 0.5 * (plus13 * plus13 + minus13 * minus13)
    phi_d = (1.0 / 3.0) * (1.0 / plus13 - 1.0 / minus13)
    inv_phi = 1.0 / phi
    phi3 = phi * phi * phi
    kf_tot = (3.0 * math.pi**2) ** (1.0 / 3.0)
    tfac = (math.pi / (16.0 * kf_tot)) * inv_phi * inv_phi * inv_c * inv_n * inv_n
    sigma = s_own + 2.0 * s_mix + s_other
    t2 = sigma * tfac
    inv_gp3 = (1.0 / GAMMA) * inv_phi * inv_phi * inv_phi
    ex = jnp.exp(-ec * inv_gp3)
    amp = (BETA / GAMMA) / (ex - 1.0)
    y = amp * t2
    den = 1.0 + y + y * y
    inv_d = 1.0 / den
    ct = (BETA / GAMMA) * t2
    q = ct * (1.0 + y) * inv_d
    grad_h = GAMMA * phi3 * jnp.log(1.0 + q)
    scale = GAMMA * phi3 / (1.0 + q) * inv_d * inv_d
    h_t = scale * ((BETA / GAMMA) * (1.0 + 2.0 * y))
    h_a = -scale * (ct * t2) * (y * (2.0 + y))
    h_ec = h_a * (amp * amp * ex * (GAMMA / BETA) * inv_gp3)
    h_phi = inv_phi * (3.0 * (grad_h - ec * h_ec) - 2.0 * t2 * h_t)
    one_ec = 1.0 + h_ec
    e_n = ec + grad_h - (1.0 / 3.0) * radius * ec_r * one_ec - (7.0 / 3.0) * t2 * h_t
    e_z = ec_z * one_ec + phi_d * h_phi
    dn = dn_x + e_n + e_z * minus
    ds_c = total * h_t * tfac
    return dn, ds_x + ds_c, 2.0 * ds_c


def kernel(
    orb_hbm, bands_hbm, core_hbm, out_ref,
    orb, dmat_ref, bands_ref, part, core, x_in, x_out, summed, z_in,
    dens, grad, grad_o, flux, turned, x_line, x_res, x_back, y_line, y_res, y_back,
    orb_sem, core_sem, bands_sem, xs_sem, xr_sem, zs_sem, zr_sem, ps_sem, pr_sem, ys_sem, yr_sem, gs_sem, gr_sem,
):
    spin = lax.axis_index("spin")
    band = lax.axis_index("band")
    grid = lax.axis_index("grid")
    bx = band // NZ4
    bz = lax.rem(band, NZ4)

    def at_band(x, z):
        return (spin, lax.rem(x, NX4) * NZ4 + lax.rem(z, NZ4), grid)

    def copy(src, dst, send_sem, recv_sem, device):
        return pltpu.make_async_remote_copy(
            src_ref=src, dst_ref=dst, send_sem=send_sem, recv_sem=recv_sem,
            device_id=device, device_id_type=MESH,
        )

    def send(*args):
        copy(*args).start()

    def sent(like, send_sem):
        copy(like, like, send_sem, send_sem, (spin, band, grid)).wait_send()

    def arrived(like, recv_sem):
        copy(like, like, recv_sem, recv_sem, (spin, band, grid)).wait_recv()

    bands_copy = pltpu.make_async_copy(bands_hbm, bands_ref, bands_sem)
    bands_copy.start()

    def y_of(r):
        return pl.multiple_of(lax.rem(bx + r, NX4) * YQ, YQ)

    def load(k):
        x0, rows, r = ((0, CR, 2), (CR, XR - CR, 2), (0, XR, 1), (0, XR, 3), (0, XR, 0))[k]
        return pltpu.make_async_copy(
            orb_hbm.at[0, :, pl.ds(x0, rows), pl.ds(y_of(r), YQ), :],
            orb.at[:, pl.ds(x0, rows), pl.ds(r * YQ, YQ), :],
            orb_sem.at[k],
        )

    for k in range(5):
        load(k).start()
    y_own = pl.multiple_of(band * YB, YB)
    core_copy = pltpu.make_async_copy(core_hbm.at[:, pl.ds(y_own, YB), :], core, core_sem)
    core_copy.start()

    barrier = pltpu.get_barrier_semaphore()
    peers = [at_band(bx + 1, bz), at_band(bx + 3, bz)]
    peers += [at_band(bx, bz + d) for d in (1, 2, 3)]
    peers += [(spin, band, lax.rem(grid + d, GRID)) for d in range(1, GRID)]
    peers += [(1 - spin, band, grid)]
    for peer in peers:
        pl.semaphore_signal(barrier, inc=1, device_id=peer, device_id_type=MESH)

    def density(c, r):
        rows, ys = slice(c * CR, (c + 1) * CR), slice(r * YQ, (r + 1) * YQ)
        acc = None
        for b in range(8):
            v = orb[b, rows, ys, :].astype(F32)
            term = weights[b] * (v * v)
            acc = term if acc is None else acc + term
        part[r, rows] = acc

    plus, minus = at_band(bx + 1, bz), at_band(bx + 3, bz)

    def half(c, h):
        return pl.ds(c * CR + h * HR, HR)

    def x_send(stream, c, src):
        target = minus if stream % 2 else plus
        send(src, x_in.at[c, stream], xs_sem, xr_sem.at[c, int(stream > 1)], target)

    def far(c):
        x_send(0, c, part.at[2, half(c, 0)])
        x_send(1, c, part.at[2, half(c, 1)])

    def direct(c):
        density(c, 1)
        x_send(2, c, part.at[1, half(c, 1)])
        density(c, 3)
        x_send(3, c, part.at[3, half(c, 0)])

    def relay(c):
        arrived(x_in.at[c, 0:2], xr_sem.at[c, 0])
        for side, r in ((0, 1), (1, 3)):
            x_out[side, c] = part[r, half(c, side)] + x_in[c, side]
            x_send(4 + side, c, x_out.at[side, c])

    def finish(c):
        arrived(x_in.at[c, 2:6], xr_sem.at[c, 1])
        summed[half(c, 0)] = part[0, half(c, 0)] + x_in[c, 4] + x_in[c, 3]
        summed[half(c, 1)] = part[0, half(c, 1)] + x_in[c, 5] + x_in[c, 2]
        rows = pl.ds(c * CR, CR)
        for d in (2, 1, 3):
            z = lax.rem(bz + d, NZ4)
            ys = pl.ds(pl.multiple_of(z * YB, YB), YB)
            send(
                summed.at[rows, ys, :], z_in.at[d - 1, rows], zs_sem, zr_sem,
                at_band(bx, z),
            )

    with jax.named_scope("first_piece"):
        bands_copy.wait()
        first = bands_ref[0, 0]
        last = first + bands_ref[0, 1]
        weights = []
        for b in range(8):
            ident = band * 8 + b
            weights.append(jnp.where((ident >= first) & (ident < last), 0.5, 1.0).astype(F32))
        load(0).wait()
        density(0, 2)
    with jax.named_scope("barrier"):
        pl.semaphore_wait(barrier, len(peers))
    with jax.named_scope("rs_head"):
        for c in range(CH):
            if c == 1:
                load(1).wait()
            if c:
                density(c, 2)
            far(c)
        load(2).wait()
        load(3).wait()
        direct(0)
    with jax.named_scope("dmat"):
        dmat_ref[...] = derivative_matrix()
    for c in range(CH):
        with jax.named_scope(f"relay{c}"):
            relay(c)
        if c + 1 < CH:
            direct(c + 1)
    load(4).wait()
    for c in range(CH):
        density(c, 0)
    core_copy.wait()
    for c in range(CH):
        with jax.named_scope(f"finish{c}"):
            finish(c)

    y_mine = pl.ds(pl.multiple_of(bz * YB, YB), YB)
    base = summed[:, y_mine, :] + 0.5 * core[...]
    with jax.named_scope("z_wait"):
        arrived(z_in, zr_sem)
    own = base + z_in[0] + z_in[1] + z_in[2]
    dens[...] = own.reshape(N, N)

    partner = (1 - spin, band, grid)
    offsets = [(dx, dz) for dx in (2, 1, 3, 0) for dz in (2, 1, 3, 0) if (dx, dz) != (0, 0)]
    g_offsets = (3, 5, 2, 6, 1, 7, 4)

    def dot(a, b):
        return jnp.dot(a, b, precision=lax.Precision.HIGHEST, preferred_element_type=F32)

    def band_rows(b):
        return pl.ds(pl.multiple_of(b * YB, YB), YB)

    def grid_rows(g):
        return pl.ds(pl.multiple_of(g * XR, XR), XR)

    def y_exchange(src, dst, k):
        for dx, dz in offsets:
            p = lax.rem(bx + dx, NX4) * NZ4 + lax.rem(bz + dz, NZ4)
            send(
                src.at[band_rows(p), :], dst.at[band_rows(band), :],
                ys_sem.at[k], yr_sem.at[k], (spin, p, grid),
            )
        dst[band_rows(band), :] = src[band_rows(band), :]

    def y_wait(dst, k):
        arrived(dst.at[0 : N - YB, :], yr_sem.at[k])

    def x_exchange(src, dst, k):
        for d in g_offsets:
            g = lax.rem(grid + d, GRID)
            send(
                src.at[grid_rows(g), :], dst.at[grid_rows(grid), :],
                gs_sem.at[k], gr_sem.at[k], (spin, band, g),
            )
        dst[grid_rows(grid), :] = src[grid_rows(grid), :]

    def x_wait(dst, k):
        arrived(dst.at[0 : N - XR, :], gr_sem.at[k])

    def turn(src, dst):
        for i in range(YB):
            dst[i * XR : (i + 1) * XR, :] = src[pl.ds(i, XR, stride=YB), :]

    def turned_back(ref, xr):
        return ref[pl.ds(xr, YB, stride=XR), :]

    dmat = dmat_ref[...]

    def pencils(y_src, x_src, k):
        y_exchange(y_src, y_line.at[k], 2 * k)
        turn(x_src, turned.at[k])
        x_exchange(turned.at[k], x_line.at[k], 2 * k)

    def lines_x(k):
        x_res[k] = dot(dmat, x_line[k])
        x_exchange(x_res.at[k], x_back.at[k], 2 * k + 1)

    def lines_y(k):
        y_res[k] = dot(dmat, y_line[k])
        y_exchange(y_res.at[k], y_back.at[k], 2 * k + 1)

    with jax.named_scope("fwd0"):
        pencils(dens, dens, 0)
        send(dens, grad_o.at[3], ps_sem, pr_sem, partner)
        grad[2] = -dot(dens[...], dmat)
        send(grad.at[2], grad_o.at[2], ps_sem, pr_sem, partner)
    with jax.named_scope("drain0"):
        sent(part.at[0:3], xs_sem)
        sent(z_in, zs_sem)
    with jax.named_scope("x_wait0"):
        x_wait(x_line.at[0], 0)
    with jax.named_scope("x_lines0"):
        lines_x(0)
    with jax.named_scope("y_wait0"):
        y_wait(y_line.at[0], 0)
    with jax.named_scope("y_lines0"):
        lines_y(0)
    with jax.named_scope("x_back0"):
        x_wait(x_back.at[0], 1)
        for i in range(XR):
            grad[0, i * YB : (i + 1) * YB, :] = turned_back(x_back.at[0], i)
        send(grad.at[0], grad_o.at[0], ps_sem, pr_sem, partner)
    with jax.named_scope("y_back0"):
        y_wait(y_back.at[0], 1)
    with jax.named_scope("swap"):
        send(y_back.at[0], grad_o.at[1], ps_sem, pr_sem, partner)
        arrived(grad_o, pr_sem)

    with jax.named_scope("xc"):
        step = 16
        for i in range(0, N, step):
            rows = slice(i, i + step)
            g = (grad[0, rows, :], y_back[0, rows, :], grad[2, rows, :])
            h = (grad_o[0, rows, :], grad_o[1, rows, :], grad_o[2, rows, :])
            s_own = g[0] * g[0] + g[1] * g[1] + g[2] * g[2]
            s_mix = g[0] * h[0] + g[1] * h[1] + g[2] * h[2]
            s_other = h[0] * h[0] + h[1] * h[1] + h[2] * h[2]
            dn, ds, dm = xc_derivs(dens[rows, :], grad_o[3, rows, :], s_own, s_mix, s_other)
            for a in range(3):
                flux[a, rows, :] = 2.0 * ds * g[a] + dm * h[a]
            flux[3, rows, :] = dn

    with jax.named_scope("fwd1"):
        pencils(flux.at[1], flux.at[0], 1)
        flux[3] = flux[3] + dot(flux[2], dmat)
    with jax.named_scope("drain1"):
        for k in (0, 1):
            sent(y_line.at[k, 0 : N - YB, :], ys_sem.at[k])
            sent(x_line.at[k, 0 : N - XR, :], gs_sem.at[k])
        sent(grad_o, ps_sem)
    with jax.named_scope("x_wait1"):
        x_wait(x_line.at[1], 2)
    with jax.named_scope("x_lines1"):
        lines_x(1)
    with jax.named_scope("y_wait1"):
        y_wait(y_line.at[1], 2)
    with jax.named_scope("y_lines1"):
        lines_y(1)
    with jax.named_scope("drain2"):
        for k in (2, 3):
            sent(y_line.at[0, 0 : N - YB, :], ys_sem.at[k])
            sent(x_line.at[0, 0 : N - XR, :], gs_sem.at[k])
    with jax.named_scope("x_back1"):
        x_wait(x_back.at[1], 3)
        for i in range(XR):
            rows = slice(i * YB, (i + 1) * YB)
            flux[3, rows, :] = flux[3, rows, :] - turned_back(x_back.at[1], i)
    with jax.named_scope("y_back1"):
        y_wait(y_back.at[1], 3)
    with jax.named_scope("tail"):
        out_ref[0] = (flux[3] - y_back[1]).reshape(XR, YB, N)


def per_device(orbitals, partial_bands, core_density):
    vm = pltpu.VMEM
    sem = pltpu.SemaphoreType.DMA
    anyspace = pl.BlockSpec(memory_space=pltpu.HBM)
    return pl.pallas_call(
        kernel,
        out_shape=jax.ShapeDtypeStruct((1, XR, YB, N), F32),
        in_specs=[anyspace] * 3,
        out_specs=pl.BlockSpec(memory_space=pltpu.VMEM),
        scratch_shapes=[
            vm((8, XR, N, N), jnp.bfloat16),
            vm((N, N), F32),
            pltpu.SMEM((1, 2), jnp.int32),
            vm((NX4, XR, YQ, N), F32),
            vm((XR, YB, N), F32),
            vm((CH, 6, HR, YQ, N), F32),
            vm((2, CH, HR, YQ, N), F32),
            vm((XR, YQ, N), F32),
            vm((NZ4 - 1, XR, YB, N), F32),
            vm((N, N), F32),
            vm((3, N, N), F32),
            vm((4, N, N), F32),
            vm((4, N, N), F32),
            vm((2, N, N), F32),
            vm((2, N, N), F32),
            vm((2, N, N), F32),
            vm((2, N, N), F32),
            vm((2, N, N), F32),
            vm((2, N, N), F32),
            vm((2, N, N), F32),
            sem((5,)),
            sem,
            sem,
            sem,
            sem((CH, 2)),
            sem,
            sem,
            sem,
            sem,
            sem((4,)),
            sem((4,)),
            sem((4,)),
            sem((4,)),
        ],
        compiler_params=pltpu.CompilerParams(
            collective_id=0, has_side_effects=True, vmem_limit_bytes=60000 * 1024
        ),
    )(orbitals, partial_bands, core_density)


def solution(mesh):
    in_specs = (P("spin", "band", "grid", None, None), P("spin", None), P("grid", None, None))
    out_specs = P("spin", "grid", "band", None)

    return jax.shard_map(
        per_device, mesh=mesh, in_specs=in_specs, out_specs=out_specs, check_vma=False
    )
```

```python
import math

import jax
import jax.numpy as jnp
from jax import lax
from jax.experimental import pallas as pl
from jax.experimental.pallas import tpu as pltpu
from jax.sharding import PartitionSpec as P

KAPPA = 0.804
MU_X = 0.2195149727645171
BETA = 0.06672455060314922
GAMMA = (1.0 - math.log(2.0)) / math.pi**2
FZ_NORM = 2.0 ** (4.0 / 3.0) - 2.0
FPP_ZERO = 1.709921

MESH = pl.DeviceIdType.MESH
F32 = jnp.float32
N = 128
XR = 16
NX4 = 4
NZ4 = 4
BAND = NX4 * NZ4
GRID = 8
YB = N // BAND
YQ = N // NX4
CR = 4
CH = 3
XF = CH * CR
HR = CR // 2


def derivative_matrix():
    k = lax.broadcasted_iota(jnp.int32, (N, N), 0) - lax.broadcasted_iota(jnp.int32, (N, N), 1)
    far = jnp.abs(k)
    near = jnp.minimum(far, N - far)
    angle = (math.pi / N) * jnp.maximum(near, 1).astype(F32)
    size = (math.pi / N) * jnp.cos(angle) / jnp.sin(angle)
    flips = (k < 0).astype(jnp.int32) + (far > N // 2).astype(jnp.int32) + (far & 1)
    signed = jnp.where((flips & 1) == 1, -size, size)
    return jnp.where(k == 0, 0.0, signed)


def pw_fit(r, root, amp, alpha, b1, b2, b3, b4):
    denom = (2.0 * amp) * (root * (b1 + root * (b2 + root * (b3 + root * b4))))
    slope = (2.0 * amp) * (0.5 * b1 / root + (b2 + root * (1.5 * b3 + root * (2.0 * b4))))
    log = jnp.log(1.0 + 1.0 / denom)
    front = (-2.0 * amp) * (1.0 + alpha * r)
    value = front * log
    deriv = (-2.0 * amp * alpha) * log - front * slope / (denom * (denom + 1.0))
    return value, deriv


def cbrt(x):
    return jnp.exp(jnp.log(x) * (1.0 / 3.0))


def xc_derivs(own, other, s_own, s_mix, s_other):
    total = own + other
    inv_n = 1.0 / total
    c_own = cbrt(own)
    c_other = cbrt(other)
    c_tot = cbrt(total)
    inv_c = 1.0 / c_tot
    double = 2.0 * own
    kf = (6.0 * math.pi**2) ** (1.0 / 3.0) * c_own
    inv_kn = 1.0 / (kf * double)
    s2 = s_own * inv_kn * inv_kn
    inv_den = 1.0 / (1.0 + (MU_X / KAPPA) * s2)
    enh = (1.0 + KAPPA) - KAPPA * inv_den
    enh_d = MU_X * inv_den * inv_den
    dn_x = (-1.0 / math.pi) * kf * (enh - 2.0 * s2 * enh_d)
    ds_x = (-3.0 / (8.0 * math.pi)) * enh_d * inv_kn
    two13 = 2.0 ** (1.0 / 3.0)
    plus = double * inv_n
    minus = 2.0 * other * inv_n
    zeta = (own - other) * inv_n
    plus13 = two13 * c_own * inv_c
    minus13 = two13 * c_other * inv_c
    radius = (3.0 / (4.0 * math.pi)) ** (1.0 / 3.0) * inv_c
    root = jnp.sqrt(radius)
    ec0, ec0_r = pw_fit(radius, root, 0.031091, 0.2137, 7.5957, 3.5876, 1.6382, 0.49294)
    ec1, ec1_r = pw_fit(radius, root, 0.015545, 0.20548, 14.1189, 6.1977, 3.3662, 0.62517)
    ac, ac_r = pw_fit(radius, root, 0.016887, 0.11125, 10.357, 3.6231, 0.88026, 0.49671)
    fz = (plus * plus13 + minus * minus13 - 2.0) * (1.0 / FZ_NORM)
    fz_d = (4.0 / 3.0 / FZ_NORM) * (plus13 - minus13)
    z2 = zeta * zeta
    z3 = z2 * zeta
    z4 = z2 * z2
    w1 = (-1.0 / FPP_ZERO) * (1.0 - z4)
    diff = ec1 - ec0
    mix = ac * w1 + diff * z4
    ec = ec0 + fz * mix
    ec_r = ec0_r + fz * (ac_r * w1 + (ec1_r - ec0_r) * z4)
    ec_z = fz_d * mix + 4.0 * z3 * fz * (ac * (1.0 / FPP_ZERO) + diff)
    phi = 0.5 * (plus13 * plus13 + minus13 * minus13)
    phi_d = (1.0 / 3.0) * (1.0 / plus13 - 1.0 / minus13)
    inv_phi = 1.0 / phi
    phi3 = phi * phi * phi
    kf_tot = (3.0 * math.pi**2) ** (1.0 / 3.0)
    tfac = (math.pi / (16.0 * kf_tot)) * inv_phi * inv_phi * inv_c * inv_n * inv_n
    sigma = s_own + 2.0 * s_mix + s_other
    t2 = sigma * tfac
    inv_gp3 = (1.0 / GAMMA) * inv_phi * inv_phi * inv_phi
    ex = jnp.exp(-ec * inv_gp3)
    amp = (BETA / GAMMA) / (ex - 1.0)
    y = amp * t2
    den = 1.0 + y + y * y
    inv_d = 1.0 / den
    ct = (BETA / GAMMA) * t2
    q = ct * (1.0 + y) * inv_d
    grad_h = GAMMA * phi3 * jnp.log(1.0 + q)
    scale = GAMMA * phi3 / (1.0 + q) * inv_d * inv_d
    h_t = scale * ((BETA / GAMMA) * (1.0 + 2.0 * y))
    h_a = -scale * (ct * t2) * (y * (2.0 + y))
    h_ec = h_a * (amp * amp * ex * (GAMMA / BETA) * inv_gp3)
    h_phi = inv_phi * (3.0 * (grad_h - ec * h_ec) - 2.0 * t2 * h_t)
    one_ec = 1.0 + h_ec
    e_n = ec + grad_h - (1.0 / 3.0) * radius * ec_r * one_ec - (7.0 / 3.0) * t2 * h_t
    e_z = ec_z * one_ec + phi_d * h_phi
    dn = dn_x + e_n + e_z * minus
    ds_c = total * h_t * tfac
    return dn, ds_x + ds_c, 2.0 * ds_c


def kernel(
    orb_hbm, bands_hbm, core_hbm, out_ref,
    orb, dmat_ref, bands_ref, part, core, x_in, x_out, summed, z_in, zf_in, zf_sum, xf_in,
    dens, grad, grad_o, flux, turned, x_line, x_res, x_back, y_line, y_res, y_back,
    orb_sem, core_sem, bands_sem, xs_sem, xr_sem, zs_sem, zr_sem, fs_sem, fr_sem, ps_sem, pr_sem, ys_sem, yr_sem, gs_sem, gr_sem,
):
    spin = lax.axis_index("spin")
    band = lax.axis_index("band")
    grid = lax.axis_index("grid")
    bx = band // NZ4
    bz = lax.rem(band, NZ4)

    def at_band(x, z):
        return (spin, lax.rem(x, NX4) * NZ4 + lax.rem(z, NZ4), grid)

    def copy(src, dst, send_sem, recv_sem, device):
        return pltpu.make_async_remote_copy(
            src_ref=src, dst_ref=dst, send_sem=send_sem, recv_sem=recv_sem,
            device_id=device, device_id_type=MESH,
        )

    def send(*args):
        copy(*args).start()

    def sent(like, send_sem):
        copy(like, like, send_sem, send_sem, (spin, band, grid)).wait_send()

    def arrived(like, recv_sem):
        copy(like, like, recv_sem, recv_sem, (spin, band, grid)).wait_recv()

    bands_copy = pltpu.make_async_copy(bands_hbm, bands_ref, bands_sem)
    bands_copy.start()

    def y_of(r):
        return pl.multiple_of(lax.rem(bx + r, NX4) * YQ, YQ)

    pieces = [(0, CR, 2), (CR, XF - CR, 2)]
    pieces += [(XF, XR - XF, r) for r in range(NX4)]
    pieces += [(0, XF, r) for r in (1, 3, 0)]

    def load(k):
        x0, rows, r = pieces[k]
        return pltpu.make_async_copy(
            orb_hbm.at[0, :, pl.ds(x0, rows), pl.ds(y_of(r), YQ), :],
            orb.at[:, pl.ds(x0, rows), pl.ds(r * YQ, YQ), :],
            orb_sem.at[k],
        )

    for k in range(len(pieces)):
        load(k).start()
    y_own = pl.multiple_of(band * YB, YB)
    core_copy = pltpu.make_async_copy(core_hbm.at[:, pl.ds(y_own, YB), :], core, core_sem)
    core_copy.start()

    barrier = pltpu.get_barrier_semaphore()
    peers = [at_band(bx + d, bz) for d in (1, 2, 3)]
    peers += [at_band(bx, bz + d) for d in (1, 2, 3)]
    peers += [(spin, band, lax.rem(grid + d, GRID)) for d in range(1, GRID)]
    peers += [(1 - spin, band, grid)]
    for peer in peers:
        pl.semaphore_signal(barrier, inc=1, device_id=peer, device_id_type=MESH)

    def density(x0, r, weights):
        rows, ys = slice(x0, x0 + CR), slice(r * YQ, (r + 1) * YQ)
        acc = None
        for b in range(8):
            v = orb[b, rows, ys, :].astype(F32)
            term = weights[b] * (v * v)
            acc = term if acc is None else acc + term
        part[r, rows] = acc

    plus, minus = at_band(bx + 1, bz), at_band(bx + 3, bz)

    def half(c, h):
        return pl.ds(c * CR + h * HR, HR)

    def x_send(stream, c, src):
        target = minus if stream % 2 else plus
        send(src, x_in.at[c, stream], xs_sem, xr_sem.at[c, int(stream > 1)], target)

    def far(c):
        x_send(0, c, part.at[2, half(c, 0)])
        x_send(1, c, part.at[2, half(c, 1)])

    def direct(c):
        x_send(2, c, part.at[1, half(c, 1)])
        x_send(3, c, part.at[3, half(c, 0)])

    def relay(c):
        arrived(x_in.at[c, 0:2], xr_sem.at[c, 0])
        for side, r in ((0, 1), (1, 3)):
            x_out[side, c] = part[r, half(c, side)] + x_in[c, side]
            x_send(4 + side, c, x_out.at[side, c])

    def finish(c):
        arrived(x_in.at[c, 2:6], xr_sem.at[c, 1])
        summed[half(c, 0)] = part[0, half(c, 0)] + x_in[c, 4] + x_in[c, 3]
        summed[half(c, 1)] = part[0, half(c, 1)] + x_in[c, 5] + x_in[c, 2]
        rows = pl.ds(c * CR, CR)
        for d in (2, 1, 3):
            z = lax.rem(bz + d, NZ4)
            ys = pl.ds(pl.multiple_of(z * YB, YB), YB)
            send(
                summed.at[rows, ys, :], z_in.at[d - 1, rows], zs_sem, zr_sem,
                at_band(bx, z),
            )

    with jax.named_scope("first_piece"):
        bands_copy.wait()
        first = bands_ref[0, 0]
        last = first + bands_ref[0, 1]
        weights = []
        for b in range(8):
            ident = band * 8 + b
            weights.append(jnp.where((ident >= first) & (ident < last), 0.5, 1.0).astype(F32))

    def dens_far(c):
        if c < 2:
            load(c).wait()
        density(c * CR, 2, weights)

    def dens_zf():
        for r in range(NX4):
            load(2 + r).wait()
            density(XF, r, weights)

    def dens_near(c):
        for k, r in ((6, 1), (7, 3)):
            if c == 0:
                load(k).wait()
            density(c * CR, r, weights)

    def dens_own():
        load(8).wait()
        for c in range(CH):
            density(c * CR, 0, weights)

    def early(body):
        pl.when(spin == 0)(body)

    @pl.when(spin == 1)
    def _():
        for c in range(CH):
            dens_far(c)
        dens_zf()
        for c in range(CH):
            dens_near(c)
        dens_own()
        dmat_ref[...] = derivative_matrix()

    early(lambda: dens_far(0))
    with jax.named_scope("barrier"):
        pl.semaphore_wait(barrier, len(peers))
    with jax.named_scope("rs_head"):
        far(0)
        early(lambda: dens_far(1))
        far(1)
        early(lambda: dens_far(2))
        far(2)
        early(dens_zf)
        zf_rows = pl.ds(XF, XR - XF)
        for d in (2, 1, 3):
            z = lax.rem(bz + d, NZ4)
            ys = pl.ds(pl.multiple_of(z * YB, YB), YB)
            send(part.at[:, zf_rows, ys, :], zf_in.at[d - 1], fs_sem.at[0], fr_sem.at[0], at_band(bx, z))
        early(lambda: dens_near(0))
        direct(0)

        def rest():
            for c in range(1, CH):
                dens_near(c)
            dens_own()
            dmat_ref[...] = derivative_matrix()

        early(rest)
    for c in range(CH):
        with jax.named_scope(f"relay{c}"):
            relay(c)
        if c + 1 < CH:
            direct(c + 1)
    core_copy.wait()
    for c in range(CH):
        with jax.named_scope(f"finish{c}"):
            finish(c)

    y_mine = pl.ds(pl.multiple_of(bz * YB, YB), YB)
    with jax.named_scope("zf_wait"):
        arrived(zf_in, fr_sem.at[0])
        zf_sum[...] = part[:, XF:XR, y_mine, :] + zf_in[0] + zf_in[1] + zf_in[2]
        for r in (2, 1, 3):
            send(zf_sum.at[r], xf_in.at[r - 1], fs_sem.at[1], fr_sem.at[1], at_band(bx + r, bz))
    base = summed[:, y_mine, :] + 0.5 * core[0:XF]
    base_f = zf_sum[0] + 0.5 * core[XF:XR]
    with jax.named_scope("z_wait"):
        arrived(z_in, zr_sem)
    own = base + z_in[0] + z_in[1] + z_in[2]
    dens[0 : XF * YB, :] = own.reshape(XF * YB, N)
    with jax.named_scope("xf_wait"):
        arrived(xf_in, fr_sem.at[1])
    own_f = base_f + xf_in[0] + xf_in[1] + xf_in[2]
    dens[XF * YB : N, :] = own_f.reshape((XR - XF) * YB, N)

    partner = (1 - spin, band, grid)
    offsets = [(dx, dz) for dx in (2, 1, 3, 0) for dz in (2, 1, 3, 0) if (dx, dz) != (0, 0)]
    g_offsets = (3, 5, 2, 6, 1, 7, 4)

    def dot(a, b):
        return jnp.dot(a, b, precision=lax.Precision.HIGHEST, preferred_element_type=F32)

    def band_rows(b):
        return pl.ds(pl.multiple_of(b * YB, YB), YB)

    def grid_rows(g):
        return pl.ds(pl.multiple_of(g * XR, XR), XR)

    def y_exchange(src, dst, k):
        for dx, dz in offsets:
            p = lax.rem(bx + dx, NX4) * NZ4 + lax.rem(bz + dz, NZ4)
            send(
                src.at[band_rows(p), :], dst.at[band_rows(band), :],
                ys_sem.at[k], yr_sem.at[k], (spin, p, grid),
            )
        dst[band_rows(band), :] = src[band_rows(band), :]

    def y_wait(dst, k):
        arrived(dst.at[0 : N - YB, :], yr_sem.at[k])

    def x_exchange(src, dst, k):
        for d in g_offsets:
            g = lax.rem(grid + d, GRID)
            send(
                src.at[grid_rows(g), :], dst.at[grid_rows(grid), :],
                gs_sem.at[k], gr_sem.at[k], (spin, band, g),
            )
        dst[grid_rows(grid), :] = src[grid_rows(grid), :]

    def x_wait(dst, k):
        arrived(dst.at[0 : N - XR, :], gr_sem.at[k])

    def turn(src, dst):
        for i in range(YB):
            dst[i * XR : (i + 1) * XR, :] = src[pl.ds(i, XR, stride=YB), :]

    def turned_back(ref, xr):
        return ref[pl.ds(xr, YB, stride=XR), :]

    dmat = dmat_ref[...]

    def pencils(y_src, x_src, k):
        y_exchange(y_src, y_line.at[k], 2 * k)
        turn(x_src, turned.at[k])
        x_exchange(turned.at[k], x_line.at[k], 2 * k)

    def lines_x(k):
        x_res[k] = dot(dmat, x_line[k])
        x_exchange(x_res.at[k], x_back.at[k], 2 * k + 1)

    def lines_y(k):
        y_res[k] = dot(dmat, y_line[k])
        y_exchange(y_res.at[k], y_back.at[k], 2 * k + 1)

    with jax.named_scope("fwd0"):
        pencils(dens, dens, 0)
        send(dens, grad_o.at[3], ps_sem, pr_sem, partner)
        grad[2] = -dot(dens[...], dmat)
        send(grad.at[2], grad_o.at[2], ps_sem, pr_sem, partner)
    with jax.named_scope("drain0"):
        sent(part.at[0:3, 0:XF], xs_sem)
        sent(z_in, zs_sem)
        sent(zf_in, fs_sem.at[0])
        sent(xf_in, fs_sem.at[1])
    with jax.named_scope("x_wait0"):
        x_wait(x_line.at[0], 0)
    with jax.named_scope("x_lines0"):
        lines_x(0)
    with jax.named_scope("y_wait0"):
        y_wait(y_line.at[0], 0)
    with jax.named_scope("y_lines0"):
        lines_y(0)
    with jax.named_scope("x_back0"):
        x_wait(x_back.at[0], 1)
        for i in range(XR):
            grad[0, i * YB : (i + 1) * YB, :] = turned_back(x_back.at[0], i)
        send(grad.at[0], grad_o.at[0], ps_sem, pr_sem, partner)
    with jax.named_scope("y_back0"):
        y_wait(y_back.at[0], 1)
    with jax.named_scope("swap"):
        send(y_back.at[0], grad_o.at[1], ps_sem, pr_sem, partner)
        arrived(grad_o, pr_sem)

    with jax.named_scope("xc"):
        step = 16
        for i in range(0, N, step):
            rows = slice(i, i + step)
            g = (grad[0, rows, :], y_back[0, rows, :], grad[2, rows, :])
            h = (grad_o[0, rows, :], grad_o[1, rows, :], grad_o[2, rows, :])
            s_own = g[0] * g[0] + g[1] * g[1] + g[2] * g[2]
            s_mix = g[0] * h[0] + g[1] * h[1] + g[2] * h[2]
            s_other = h[0] * h[0] + h[1] * h[1] + h[2] * h[2]
            dn, ds, dm = xc_derivs(dens[rows, :], grad_o[3, rows, :], s_own, s_mix, s_other)
            for a in range(3):
                flux[a, rows, :] = 2.0 * ds * g[a] + dm * h[a]
            flux[3, rows, :] = dn

    with jax.named_scope("fwd1"):
        pencils(flux.at[1], flux.at[0], 1)
        flux[3] = flux[3] + dot(flux[2], dmat)
    with jax.named_scope("drain1"):
        for k in (0, 1):
            sent(y_line.at[k, 0 : N - YB, :], ys_sem.at[k])
            sent(x_line.at[k, 0 : N - XR, :], gs_sem.at[k])
        sent(grad_o, ps_sem)
    with jax.named_scope("x_wait1"):
        x_wait(x_line.at[1], 2)
    with jax.named_scope("x_lines1"):
        lines_x(1)
    with jax.named_scope("y_wait1"):
        y_wait(y_line.at[1], 2)
    with jax.named_scope("y_lines1"):
        lines_y(1)
    with jax.named_scope("drain2"):
        for k in (2, 3):
            sent(y_line.at[0, 0 : N - YB, :], ys_sem.at[k])
            sent(x_line.at[0, 0 : N - XR, :], gs_sem.at[k])
    with jax.named_scope("x_back1"):
        x_wait(x_back.at[1], 3)
        for i in range(XR):
            rows = slice(i * YB, (i + 1) * YB)
            flux[3, rows, :] = flux[3, rows, :] - turned_back(x_back.at[1], i)
    with jax.named_scope("y_back1"):
        y_wait(y_back.at[1], 3)
    with jax.named_scope("tail"):
        out_ref[0] = (flux[3] - y_back[1]).reshape(XR, YB, N)


def per_device(orbitals, partial_bands, core_density):
    vm = pltpu.VMEM
    sem = pltpu.SemaphoreType.DMA
    anyspace = pl.BlockSpec(memory_space=pltpu.HBM)
    return pl.pallas_call(
        kernel,
        out_shape=jax.ShapeDtypeStruct((1, XR, YB, N), F32),
        in_specs=[anyspace] * 3,
        out_specs=pl.BlockSpec(memory_space=pltpu.VMEM),
        scratch_shapes=[
            vm((8, XR, N, N), jnp.bfloat16),
            vm((N, N), F32),
            pltpu.SMEM((1, 2), jnp.int32),
            vm((NX4, XR, YQ, N), F32),
            vm((XR, YB, N), F32),
            vm((CH, 6, HR, YQ, N), F32),
            vm((2, CH, HR, YQ, N), F32),
            vm((XF, YQ, N), F32),
            vm((NZ4 - 1, XF, YB, N), F32),
            vm((NZ4 - 1, NX4, XR - XF, YB, N), F32),
            vm((NX4, XR - XF, YB, N), F32),
            vm((NX4 - 1, XR - XF, YB, N), F32),
            vm((N, N), F32),
            vm((3, N, N), F32),
            vm((4, N, N), F32),
            vm((4, N, N), F32),
            vm((2, N, N), F32),
            vm((2, N, N), F32),
            vm((2, N, N), F32),
            vm((2, N, N), F32),
            vm((2, N, N), F32),
            vm((2, N, N), F32),
            vm((2, N, N), F32),
            sem((9,)),
            sem,
            sem,
            sem,
            sem((CH, 2)),
            sem,
            sem,
            sem((2,)),
            sem((2,)),
            sem,
            sem,
            sem((4,)),
            sem((4,)),
            sem((4,)),
            sem((4,)),
        ],
        compiler_params=pltpu.CompilerParams(
            collective_id=0, has_side_effects=True, vmem_limit_bytes=54400 * 1024
        ),
    )(orbitals, partial_bands, core_density)


def solution(mesh):
    in_specs = (P("spin", "band", "grid", None, None), P("spin", None), P("grid", None, None))
    out_specs = P("spin", "grid", "band", None)

    return jax.shard_map(
        per_device, mesh=mesh, in_specs=in_specs, out_specs=out_specs, check_vma=False
    )
```

```python
import math

import jax
import jax.numpy as jnp
from jax import lax
from jax.experimental import pallas as pl
from jax.experimental.pallas import tpu as pltpu
from jax.sharding import PartitionSpec as P

KAPPA = 0.804
MU_X = 0.2195149727645171
BETA = 0.06672455060314922
GAMMA = (1.0 - math.log(2.0)) / math.pi**2
FZ_NORM = 2.0 ** (4.0 / 3.0) - 2.0
FPP_ZERO = 1.709921

MESH = pl.DeviceIdType.MESH
F32 = jnp.float32
N = 128
XR = 16
NX4 = 4
NZ4 = 4
GY = 4
GRID = 2 * GY
BAND = NX4 * NZ4
YB = N // BAND
YQ = N // NX4
CH = 3
HOPS = 5


def derivative_matrix():
    k = lax.broadcasted_iota(jnp.int32, (N, N), 0) - lax.broadcasted_iota(jnp.int32, (N, N), 1)
    far = jnp.abs(k)
    near = jnp.minimum(far, N - far)
    angle = (math.pi / N) * jnp.maximum(near, 1).astype(F32)
    size = (math.pi / N) * jnp.cos(angle) / jnp.sin(angle)
    flips = (k < 0).astype(jnp.int32) + (far > N // 2).astype(jnp.int32) + (far & 1)
    signed = jnp.where((flips & 1) == 1, -size, size)
    return jnp.where(k == 0, 0.0, signed)


def pw_fit(r, root, amp, alpha, b1, b2, b3, b4):
    denom = (2.0 * amp) * (root * (b1 + root * (b2 + root * (b3 + root * b4))))
    slope = (2.0 * amp) * (0.5 * b1 / root + (b2 + root * (1.5 * b3 + root * (2.0 * b4))))
    log = jnp.log(1.0 + 1.0 / denom)
    front = (-2.0 * amp) * (1.0 + alpha * r)
    value = front * log
    deriv = (-2.0 * amp * alpha) * log - front * slope / (denom * (denom + 1.0))
    return value, deriv


def cbrt(x):
    return jnp.exp(jnp.log(x) * (1.0 / 3.0))


def xc_derivs(own, other, s_own, s_mix, s_other):
    total = own + other
    inv_n = 1.0 / total
    c_own = cbrt(own)
    c_other = cbrt(other)
    c_tot = cbrt(total)
    inv_c = 1.0 / c_tot
    double = 2.0 * own
    kf = (6.0 * math.pi**2) ** (1.0 / 3.0) * c_own
    inv_kn = 1.0 / (kf * double)
    s2 = s_own * inv_kn * inv_kn
    inv_den = 1.0 / (1.0 + (MU_X / KAPPA) * s2)
    enh = (1.0 + KAPPA) - KAPPA * inv_den
    enh_d = MU_X * inv_den * inv_den
    dn_x = (-1.0 / math.pi) * kf * (enh - 2.0 * s2 * enh_d)
    ds_x = (-3.0 / (8.0 * math.pi)) * enh_d * inv_kn
    two13 = 2.0 ** (1.0 / 3.0)
    plus = double * inv_n
    minus = 2.0 * other * inv_n
    zeta = (own - other) * inv_n
    plus13 = two13 * c_own * inv_c
    minus13 = two13 * c_other * inv_c
    radius = (3.0 / (4.0 * math.pi)) ** (1.0 / 3.0) * inv_c
    root = jnp.sqrt(radius)
    ec0, ec0_r = pw_fit(radius, root, 0.031091, 0.2137, 7.5957, 3.5876, 1.6382, 0.49294)
    ec1, ec1_r = pw_fit(radius, root, 0.015545, 0.20548, 14.1189, 6.1977, 3.3662, 0.62517)
    ac, ac_r = pw_fit(radius, root, 0.016887, 0.11125, 10.357, 3.6231, 0.88026, 0.49671)
    fz = (plus * plus13 + minus * minus13 - 2.0) * (1.0 / FZ_NORM)
    fz_d = (4.0 / 3.0 / FZ_NORM) * (plus13 - minus13)
    z2 = zeta * zeta
    z3 = z2 * zeta
    z4 = z2 * z2
    w1 = (-1.0 / FPP_ZERO) * (1.0 - z4)
    diff = ec1 - ec0
    mix = ac * w1 + diff * z4
    ec = ec0 + fz * mix
    ec_r = ec0_r + fz * (ac_r * w1 + (ec1_r - ec0_r) * z4)
    ec_z = fz_d * mix + 4.0 * z3 * fz * (ac * (1.0 / FPP_ZERO) + diff)
    phi = 0.5 * (plus13 * plus13 + minus13 * minus13)
    phi_d = (1.0 / 3.0) * (1.0 / plus13 - 1.0 / minus13)
    inv_phi = 1.0 / phi
    phi3 = phi * phi * phi
    kf_tot = (3.0 * math.pi**2) ** (1.0 / 3.0)
    tfac = (math.pi / (16.0 * kf_tot)) * inv_phi * inv_phi * inv_c * inv_n * inv_n
    sigma = s_own + 2.0 * s_mix + s_other
    t2 = sigma * tfac
    inv_gp3 = (1.0 / GAMMA) * inv_phi * inv_phi * inv_phi
    ex = jnp.exp(-ec * inv_gp3)
    amp = (BETA / GAMMA) / (ex - 1.0)
    y = amp * t2
    den = 1.0 + y + y * y
    inv_d = 1.0 / den
    ct = (BETA / GAMMA) * t2
    q = ct * (1.0 + y) * inv_d
    grad_h = GAMMA * phi3 * jnp.log(1.0 + q)
    scale = GAMMA * phi3 / (1.0 + q) * inv_d * inv_d
    h_t = scale * ((BETA / GAMMA) * (1.0 + 2.0 * y))
    h_a = -scale * (ct * t2) * (y * (2.0 + y))
    h_ec = h_a * (amp * amp * ex * (GAMMA / BETA) * inv_gp3)
    h_phi = inv_phi * (3.0 * (grad_h - ec * h_ec) - 2.0 * t2 * h_t)
    one_ec = 1.0 + h_ec
    e_n = ec + grad_h - (1.0 / 3.0) * radius * ec_r * one_ec - (7.0 / 3.0) * t2 * h_t
    e_z = ec_z * one_ec + phi_d * h_phi
    dn = dn_x + e_n + e_z * minus
    ds_c = total * h_t * tfac
    return dn, ds_x + ds_c, 2.0 * ds_c


def kernel(
    orb_hbm, bands_hbm, core_hbm, out_ref,
    orb, dmat_ref, bands_ref, part, core, x_in, x_out, summed, z_in, zf_in, zf_sum, xf_in,
    dens, grad, grad_o, flux, turned, x_line, x_res, x_back, y_line, y_res, y_back, base, final, x_fin, y_fin,
    orb_sem, core_sem, bands_sem, hop_sem, xs_sem, xr_sem, zs_sem, zr_sem, fs_sem, fr_sem,
    ps_sem, pr_sem, ys_sem, yr_sem, gs_sem, gr_sem, bs_sem, br_sem,
):
    spin = lax.axis_index("spin")
    band = lax.axis_index("band")
    grid = lax.axis_index("grid")
    bx, bz = band // NZ4, lax.rem(band, NZ4)
    gz, gy = grid // GY, lax.rem(grid, GY)

    def half_of(z):
        q = z // 2
        return 3 * q + z * (1 - 2 * q)

    q, h, e = bz // 2, half_of(bz), lax.rem(bz, 2)
    member = 2 * bx + q
    partner = (1 - spin, band, grid)

    def at_band(x, z, core=spin):
        return (core, lax.rem(x, NX4) * NZ4 + lax.rem(z, NZ4), grid)

    def copy(src, dst, send_sem, recv_sem, device):
        return pltpu.make_async_remote_copy(
            src_ref=src, dst_ref=dst, send_sem=send_sem, recv_sem=recv_sem,
            device_id=device, device_id_type=MESH,
        )

    def send(*args):
        copy(*args).start()

    def sent(like, send_sem):
        copy(like, like, send_sem, send_sem, (spin, band, grid)).wait_send()

    def arrived(like, recv_sem):
        copy(like, like, recv_sem, recv_sem, (spin, band, grid)).wait_recv()

    def rows_at(start, count):
        return pl.ds(pl.multiple_of(start, 8), count)

    bands_copy = pltpu.make_async_copy(bands_hbm, bands_ref, bands_sem)
    bands_copy.start()
    z_all = 2 * bz + gz
    near = [at_band(bx + 1, bz), at_band(bx + 3, bz)]
    near += [(spin, band, gz * GY + lax.rem(gy + d, GY)) for d in (1, 3)]
    for d in (1, 7):
        z = lax.rem(z_all + d, 8)
        near += [(spin, bx * NZ4 + z // 2, lax.rem(z, 2) * GY + gy)]
    barrier = pltpu.get_barrier_semaphore()
    across = [(1 - spin, *peer[1:]) for peer in near]
    for peer in (*near, *across, partner):
        pl.semaphore_signal(barrier, inc=1, device_id=peer, device_id_type=MESH)

    def y_of(r):
        return pl.multiple_of(lax.rem(bx + r, NX4) * YQ, YQ)

    def y_at(r):
        return pl.ds(r * YQ, YQ)

    def load(k, cs, r):
        for c in cs:
            for half in range(2):
                pltpu.make_async_copy(
                    orb_hbm.at[0, :, pl.ds(8 * half + 2 * c, 2), pl.ds(y_of(r), YQ), :],
                    orb.at[:, c, half, :, y_at(r), :],
                    orb_sem.at[k],
                ).start()

    def loaded(k, window):
        pltpu.make_async_copy(window, window, orb_sem.at[k]).wait()

    load(0, (0,), 2)
    load(1, (1, 2), 2)
    for r in range(NX4):
        load(2, (3,), r)
    for k, r in ((3, 1), (4, 3), (5, 0)):
        load(k, (0, 1, 2), r)
    core_copy = pltpu.make_async_copy(
        core_hbm.at[rows_at(8 * h, 8), rows_at(YQ * bx + 16 * q, 16), :], core, core_sem
    )
    core_copy.start()

    with jax.named_scope("first_piece"):
        bands_copy.wait()
        first = bands_ref[0, 0]
        last = first + bands_ref[0, 1]
        weights = []
        for b in range(8):
            ident = band * 8 + b
            weights.append(jnp.where((ident >= first) & (ident < last), 0.5, 1.0).astype(F32))

    def density(c, r):
        acc = None
        for b in range(8):
            v = orb[b, c, :, :, r * YQ : (r + 1) * YQ, :].astype(F32)
            term = weights[b] * (v * v)
            acc = term if acc is None else acc + term
        part[r, c] = acc

    plus, minus = at_band(bx + 1, bz), at_band(bx + 3, bz)

    def x_send(stream, c, src):
        target = minus if stream % 2 else plus
        send(src, x_in.at[c, stream], xs_sem, xr_sem.at[c, int(stream > 1)], target)

    def far(c):
        x_send(0, c, part.at[2, c, 0])
        x_send(1, c, part.at[2, c, 1])

    def direct(c):
        x_send(2, c, part.at[1, c, 1])
        x_send(3, c, part.at[3, c, 0])

    def relay(c):
        arrived(x_in.at[c, 0:2], xr_sem.at[c, 0])
        for side, r in ((0, 1), (1, 3)):
            x_out[side, c] = part[r, c, side] + x_in[c, side]
            x_send(4 + side, c, x_out.at[side, c])

    def z_targets(ds, core):
        for d in ds:
            z = lax.rem(bz + d, NZ4)
            yield d, half_of(z), rows_at(16 * (z // 2), 16), at_band(bx, z, core)

    def finish(c):
        arrived(x_in.at[c, 2:6], xr_sem.at[c, 1])
        summed[c, 0] = part[0, c, 0] + x_in[c, 4] + x_in[c, 3]
        summed[c, 1] = part[0, c, 1] + x_in[c, 5] + x_in[c, 2]
        for slot, half, ys, device in z_targets((2, 1, 3, 0), 1 - spin):
            send(summed.at[c, half, :, ys, :], z_in.at[slot, c], zs_sem, zr_sem, device)

    def z_first(ds):
        for slot, half, ys, device in z_targets(ds, spin):
            send(part.at[:, 3, half, :, ys, :], zf_in.at[slot - 1], fs_sem.at[0], fr_sem.at[0], device)

    def tell(k):
        for peer in near:
            pl.semaphore_signal(hop_sem.at[k - 1], inc=1, device_id=peer, device_id_type=MESH)

    def hear(k):
        pl.semaphore_wait(hop_sem.at[k - 1], len(near))
        if k < HOPS:
            tell(k + 1)

    loaded(0, orb.at[:, 0, :, :, y_at(2), :])
    density(0, 2)
    with jax.named_scope("barrier"):
        pl.semaphore_wait(barrier, 2 * len(near) + 1)
    with jax.named_scope("rs_head"):
        far(0)
        tell(1)
        loaded(1, orb.at[:, 1:3, :, :, y_at(2), :])
        density(1, 2)
        far(1)
        density(2, 2)
        far(2)
        loaded(2, orb.at[:, 3])
        for r in range(NX4):
            density(3, r)
        loaded(3, orb.at[:, 0:3, :, :, y_at(1), :])
        loaded(4, orb.at[:, 0:3, :, :, y_at(3), :])
        density(0, 1)
        density(0, 3)
        direct(0)
    with jax.named_scope("hear1"):
        hear(1)
        for d in (1, 3):
            pl.semaphore_signal(
                hop_sem.at[HOPS], inc=1, device_id=at_band(bx, bz + d), device_id_type=MESH
            )
        z_first((1, 3))
    with jax.named_scope("rs_rest"):
        loaded(5, orb.at[:, 0:3, :, :, y_at(0), :])
        for c, r in ((1, 1), (1, 3), (2, 1), (2, 3), (0, 0), (1, 0), (2, 0)):
            density(c, r)
        dmat_ref[...] = derivative_matrix()
    with jax.named_scope("hear_z"):
        pl.semaphore_wait(hop_sem.at[HOPS], 2)
        z_first((2,))
    for c in range(CH):
        with jax.named_scope(f"relay{c}"):
            relay(c)
        if c + 1 < CH:
            direct(c + 1)
    core_copy.wait()
    with jax.named_scope("hear2"):
        hear(2)
    with jax.named_scope("finish0"):
        finish(0)
    with jax.named_scope("hear3"):
        hear(3)
    for c in range(1, CH):
        with jax.named_scope(f"finish{c}"):
            finish(c)

    y_mine = rows_at(16 * q, 16)
    with jax.named_scope("zf_wait"):
        arrived(zf_in, fr_sem.at[0])
        zf_sum[...] = part[:, 3, h, :, y_mine, :] + zf_in[0] + zf_in[1] + zf_in[2]
        for r in (2, 1, 3, 0):
            send(
                zf_sum.at[r], xf_in.at[r], fs_sem.at[1], fr_sem.at[1],
                at_band(bx + r, bz, 1 - spin),
            )
    with jax.named_scope("hear4"):
        hear(4)
    with jax.named_scope("z_wait"):
        arrived(z_in, zr_sem)
    for c in range(CH):
        block = 0.5 * core[2 * c : 2 * c + 2] + z_in[0, c] + z_in[1, c] + z_in[2, c] + z_in[3, c]
        dens[32 * c : 32 * c + 32, :] = block.reshape(32, N)
    with jax.named_scope("hear5"):
        hear(5)
    with jax.named_scope("xf_wait"):
        arrived(xf_in, fr_sem.at[1])
    block = 0.5 * core[2 * CH : 2 * CH + 2] + xf_in[0] + xf_in[1] + xf_in[2] + xf_in[3]
    dens[32 * CH : 32 * CH + 32, :] = block.reshape(32, N)

    def dot(a, b):
        return jnp.dot(a, b, precision=lax.Precision.HIGHEST, preferred_element_type=F32)

    holder = 1 - spin

    def y_exchange(src, dst, k):
        for dx, dq in ((2, 1), (1, 1), (3, 1), (0, 1), (2, 0), (1, 0), (3, 0)):
            x, place = lax.rem(bx + dx, NX4), lax.rem(q + dq, 2)
            z = h + place * (3 - 2 * h)
            send(
                src.at[rows_at(16 * (2 * x + place), 16), :], dst.at[rows_at(16 * member, 16), :],
                ys_sem.at[k], yr_sem.at[k], (holder, x * NZ4 + z, grid),
            )
        mine = rows_at(16 * member, 16)
        send(src.at[mine, :], dst.at[mine, :], ys_sem.at[k], yr_sem.at[k], partner)

    def y_wait(dst, k):
        arrived(dst, yr_sem.at[k])

    def x_exchange(src, dst, k):
        for de in (1, 0):
            for dz in (1, 0):
                for dy in (2, 1, 3, 0):
                    if (de, dz, dy) == (0, 0, 0):
                        continue
                    e2 = lax.rem(e + de, 2)
                    g2 = lax.rem(gz + dz, 2) * GY + lax.rem(gy + dy, GY)
                    z = 2 * q + e2
                    there, here = 8 * e2 + g2, 2 * grid + h
                    if k == 1:
                        there, here = 2 * g2 + half_of(z), 8 * e + grid
                    send(
                        src.at[rows_at(8 * there, 8), :], dst.at[rows_at(8 * here, 8), :],
                        gs_sem.at[k], gr_sem.at[k], (holder, bx * NZ4 + z, g2),
                    )
        mine = (2 * grid + h, 8 * e + grid)
        there, here = mine if k == 1 else mine[::-1]
        there, here = rows_at(8 * there, 8), rows_at(8 * here, 8)
        send(src.at[there, :], dst.at[here, :], gs_sem.at[k], gr_sem.at[k], partner)

    def x_wait(dst, k):
        arrived(dst, gr_sem.at[k])

    def out_y():
        xr = 8 * h + member
        for dx in (2, 1, 3, 0):
            for dz in (2, 1, 3, 0):
                b2 = lax.rem(bx + dx, NX4) * NZ4 + lax.rem(bz + dz, NZ4)
                send(
                    y_res.at[1, rows_at(8 * b2, 8), :], y_fin.at[rows_at(8 * xr, 8), :],
                    ys_sem.at[3], yr_sem.at[3], (holder, b2, grid),
                )

    def out_x():
        for dz, dy in ((1, 2), (1, 1), (1, 3), (0, 2), (1, 0), (0, 1), (0, 3), (0, 0)):
            g2 = lax.rem(gz + dz, 2) * GY + lax.rem(gy + dy, GY)
            send(
                x_res.at[1, rows_at(XR * g2, XR), :], x_fin.at[rows_at(XR * grid, XR), :],
                gs_sem.at[3], gr_sem.at[3], (holder, band, g2),
            )

    def pencils(y_src, x_src, k):
        y_exchange(y_src, y_line.at[k], 2 * k)
        for t in range(16):
            turned[k, 8 * t : 8 * t + 8, :] = x_src[pl.ds(t, 8, stride=16), :]
        x_exchange(turned.at[k], x_line.at[k], 2 * k)

    dmat = dmat_ref[...]

    with jax.named_scope("fwd0"):
        pencils(dens, dens, 0)
        send(dens, grad_o.at[3], ps_sem, pr_sem, partner)
        grad[2] = -dot(dens[...], dmat)
        send(grad.at[2], grad_o.at[2], ps_sem, pr_sem, partner)
    with jax.named_scope("drain0"):
        sent(part.at[0:3, 0:CH], xs_sem)
        sent(z_in, zs_sem)
        sent(zf_in, fs_sem.at[0])
        sent(xf_in, fs_sem.at[1])
    with jax.named_scope("y_wait0"):
        y_wait(y_line.at[0], 0)
    with jax.named_scope("y_lines0"):
        y_res[0] = dot(dmat, y_line[0])
        y_exchange(y_res.at[0], y_back, 1)
    with jax.named_scope("x_wait0"):
        x_wait(x_line.at[0], 0)
    with jax.named_scope("x_lines0"):
        x_res[0] = dot(dmat, x_line[0])
        x_exchange(x_res.at[0], x_back, 1)
    with jax.named_scope("y_back0"):
        y_wait(y_back, 1)
        send(y_back, grad_o.at[1], ps_sem, pr_sem, partner)
    with jax.named_scope("x_back0"):
        x_wait(x_back, 1)
        for i in range(8):
            grad[0, 16 * i : 16 * i + 16, :] = x_back[pl.ds(i, 16, stride=8), :]
    with jax.named_scope("swap"):
        send(grad.at[0], grad_o.at[0], ps_sem, pr_sem, partner)
        arrived(grad_o, pr_sem)

    with jax.named_scope("xc"):
        step = 16
        for i in range(0, N, step):
            rows = slice(i, i + step)
            o = (grad[0, rows, :], y_back[rows, :], grad[2, rows, :])
            g = (grad_o[0, rows, :], grad_o[1, rows, :], grad_o[2, rows, :])
            s_own = g[0] * g[0] + g[1] * g[1] + g[2] * g[2]
            s_mix = g[0] * o[0] + g[1] * o[1] + g[2] * o[2]
            s_other = o[0] * o[0] + o[1] * o[1] + o[2] * o[2]
            dn, ds, dm = xc_derivs(grad_o[3, rows, :], dens[rows, :], s_own, s_mix, s_other)
            for a in range(3):
                flux[a, rows, :] = 2.0 * ds * g[a] + dm * o[a]
            flux[3, rows, :] = dn

    with jax.named_scope("fwd1"):
        pencils(flux.at[1], flux.at[0], 1)
        base[...] = (flux[3] + dot(flux[2], dmat)).reshape(8, 16, N)
        there = lax.rem(e + 1, 2)
        send(
            base.at[:, rows_at(8 * there, 8), :], final.at[h],
            bs_sem, br_sem, (spin, bx * NZ4 + 2 * q + there, grid),
        )
        final[h] = base[:, rows_at(8 * e, 8), :]
    with jax.named_scope("drain1"):
        for k in (0, 1):
            sent(y_line.at[k], ys_sem.at[k])
            sent(x_line.at[k], gs_sem.at[k])
        sent(grad_o, ps_sem)
    with jax.named_scope("y_wait1"):
        y_wait(y_line.at[1], 2)
    with jax.named_scope("y_lines1"):
        y_res[1] = dot(dmat, y_line[1])
        out_y()
    with jax.named_scope("x_wait1"):
        x_wait(x_line.at[1], 2)
    with jax.named_scope("x_lines1"):
        x_res[1] = dot(dmat, x_line[1])
        out_x()
    with jax.named_scope("drain2"):
        for k in (2, 3):
            sent(y_line.at[0], ys_sem.at[k])
            sent(x_line.at[0], gs_sem.at[k])
        sent(final.at[0], bs_sem)
        arrived(final.at[0], br_sem)
    with jax.named_scope("x_back1"):
        arrived(x_fin, gr_sem.at[3])
        for i in range(XR):
            out_ref[0, i] = final[i // 8, i % 8] - x_fin[pl.ds(i, YB, stride=XR), :]
    with jax.named_scope("y_back1"):
        arrived(y_fin, yr_sem.at[3])
    with jax.named_scope("tail"):
        out_ref[0] = out_ref[0] - y_fin[...].reshape(XR, YB, N)


def per_device(orbitals, partial_bands, core_density):
    vm = pltpu.VMEM
    sem = pltpu.SemaphoreType.DMA
    anyspace = pl.BlockSpec(memory_space=pltpu.HBM)
    return pl.pallas_call(
        kernel,
        out_shape=jax.ShapeDtypeStruct((1, XR, YB, N), F32),
        in_specs=[anyspace] * 3,
        out_specs=pl.BlockSpec(memory_space=pltpu.VMEM),
        scratch_shapes=[
            vm((8, CH + 1, 2, 2, N, N), jnp.bfloat16),
            vm((N, N), F32),
            pltpu.SMEM((1, 2), jnp.int32),
            vm((NX4, CH + 1, 2, 2, YQ, N), F32),
            vm((8, 16, N), F32),
            vm((CH, 6, 2, YQ, N), F32),
            vm((2, CH, 2, YQ, N), F32),
            vm((CH, 2, 2, YQ, N), F32),
            vm((NZ4, CH, 2, 16, N), F32),
            vm((NZ4 - 1, NX4, 2, 16, N), F32),
            vm((NX4, 2, 16, N), F32),
            vm((NX4, 2, 16, N), F32),
            vm((N, N), F32),
            vm((3, N, N), F32),
            vm((4, N, N), F32),
            vm((4, N, N), F32),
            vm((2, N, N), F32),
            vm((2, N, N), F32),
            vm((2, N, N), F32),
            vm((N, N), F32),
            vm((2, N, N), F32),
            vm((2, N, N), F32),
            vm((N, N), F32),
            vm((8, 16, N), F32),
            vm((2, 8, YB, N), F32),
            vm((N, N), F32),
            vm((N, N), F32),
            sem((6,)),
            sem,
            sem,
            pltpu.SemaphoreType.REGULAR((HOPS + 1,)),
            sem,
            sem((CH, 2)),
            sem,
            sem,
            sem((2,)),
            sem((2,)),
            sem,
            sem,
            sem((4,)),
            sem((4,)),
            sem((4,)),
            sem((4,)),
            sem,
            sem,
        ],
        compiler_params=pltpu.CompilerParams(
            collective_id=0, has_side_effects=True, vmem_limit_bytes=54400 * 1024
        ),
    )(orbitals, partial_bands, core_density)


def solution(mesh):
    in_specs = (P("spin", "band", "grid", None, None), P("spin", None), P("grid", None, None))
    out_specs = P("spin", "grid", "band", None)

    return jax.shard_map(
        per_device, mesh=mesh, in_specs=in_specs, out_specs=out_specs, check_vma=False
    )
```

```python
import math

import jax
import jax.numpy as jnp
from jax import lax
from jax.experimental import pallas as pl
from jax.experimental.pallas import tpu as pltpu
from jax.sharding import PartitionSpec as P

KAPPA = 0.804
MU_X = 0.2195149727645171
BETA = 0.06672455060314922
GAMMA = (1.0 - math.log(2.0)) / math.pi**2
FZ_NORM = 2.0 ** (4.0 / 3.0) - 2.0
FPP_ZERO = 1.709921

MESH = pl.DeviceIdType.MESH
F32 = jnp.float32
N = 128
XR = 16
NX4 = 4
NZ4 = 4
GY = 4
GRID = 2 * GY
BAND = NX4 * NZ4
YB = N // BAND
YQ = N // NX4
CH = 3
HOPS = 5


def derivative_matrix():
    k = lax.broadcasted_iota(jnp.int32, (N, N), 0) - lax.broadcasted_iota(jnp.int32, (N, N), 1)
    far = jnp.abs(k)
    near = jnp.minimum(far, N - far)
    angle = (math.pi / N) * jnp.maximum(near, 1).astype(F32)
    size = (math.pi / N) * jnp.cos(angle) / jnp.sin(angle)
    flips = (k < 0).astype(jnp.int32) + (far > N // 2).astype(jnp.int32) + (far & 1)
    signed = jnp.where((flips & 1) == 1, -size, size)
    return jnp.where(k == 0, 0.0, signed)


def pw_fit(r, root, amp, alpha, b1, b2, b3, b4):
    denom = (2.0 * amp) * (root * (b1 + root * (b2 + root * (b3 + root * b4))))
    slope = (2.0 * amp) * (0.5 * b1 / root + (b2 + root * (1.5 * b3 + root * (2.0 * b4))))
    log = jnp.log(1.0 + 1.0 / denom)
    front = (-2.0 * amp) * (1.0 + alpha * r)
    value = front * log
    deriv = (-2.0 * amp * alpha) * log - front * slope / (denom * (denom + 1.0))
    return value, deriv


def cbrt(x):
    return jnp.exp(jnp.log(x) * (1.0 / 3.0))


def xc_derivs(own, other, s_own, s_mix, s_other):
    total = own + other
    inv_n = 1.0 / total
    c_own = cbrt(own)
    c_other = cbrt(other)
    c_tot = cbrt(total)
    inv_c = 1.0 / c_tot
    double = 2.0 * own
    kf = (6.0 * math.pi**2) ** (1.0 / 3.0) * c_own
    inv_kn = 1.0 / (kf * double)
    s2 = s_own * inv_kn * inv_kn
    inv_den = 1.0 / (1.0 + (MU_X / KAPPA) * s2)
    enh = (1.0 + KAPPA) - KAPPA * inv_den
    enh_d = MU_X * inv_den * inv_den
    dn_x = (-1.0 / math.pi) * kf * (enh - 2.0 * s2 * enh_d)
    ds_x = (-3.0 / (8.0 * math.pi)) * enh_d * inv_kn
    two13 = 2.0 ** (1.0 / 3.0)
    plus = double * inv_n
    minus = 2.0 * other * inv_n
    zeta = (own - other) * inv_n
    plus13 = two13 * c_own * inv_c
    minus13 = two13 * c_other * inv_c
    radius = (3.0 / (4.0 * math.pi)) ** (1.0 / 3.0) * inv_c
    root = jnp.sqrt(radius)
    ec0, ec0_r = pw_fit(radius, root, 0.031091, 0.2137, 7.5957, 3.5876, 1.6382, 0.49294)
    ec1, ec1_r = pw_fit(radius, root, 0.015545, 0.20548, 14.1189, 6.1977, 3.3662, 0.62517)
    ac, ac_r = pw_fit(radius, root, 0.016887, 0.11125, 10.357, 3.6231, 0.88026, 0.49671)
    fz = (plus * plus13 + minus * minus13 - 2.0) * (1.0 / FZ_NORM)
    fz_d = (4.0 / 3.0 / FZ_NORM) * (plus13 - minus13)
    z2 = zeta * zeta
    z3 = z2 * zeta
    z4 = z2 * z2
    w1 = (-1.0 / FPP_ZERO) * (1.0 - z4)
    diff = ec1 - ec0
    mix = ac * w1 + diff * z4
    ec = ec0 + fz * mix
    ec_r = ec0_r + fz * (ac_r * w1 + (ec1_r - ec0_r) * z4)
    ec_z = fz_d * mix + 4.0 * z3 * fz * (ac * (1.0 / FPP_ZERO) + diff)
    phi = 0.5 * (plus13 * plus13 + minus13 * minus13)
    phi_d = (1.0 / 3.0) * (1.0 / plus13 - 1.0 / minus13)
    inv_phi = 1.0 / phi
    phi3 = phi * phi * phi
    kf_tot = (3.0 * math.pi**2) ** (1.0 / 3.0)
    tfac = (math.pi / (16.0 * kf_tot)) * inv_phi * inv_phi * inv_c * inv_n * inv_n
    sigma = s_own + 2.0 * s_mix + s_other
    t2 = sigma * tfac
    inv_gp3 = (1.0 / GAMMA) * inv_phi * inv_phi * inv_phi
    ex = jnp.exp(-ec * inv_gp3)
    amp = (BETA / GAMMA) / (ex - 1.0)
    y = amp * t2
    den = 1.0 + y + y * y
    inv_d = 1.0 / den
    ct = (BETA / GAMMA) * t2
    q = ct * (1.0 + y) * inv_d
    grad_h = GAMMA * phi3 * jnp.log(1.0 + q)
    scale = GAMMA * phi3 / (1.0 + q) * inv_d * inv_d
    h_t = scale * ((BETA / GAMMA) * (1.0 + 2.0 * y))
    h_a = -scale * (ct * t2) * (y * (2.0 + y))
    h_ec = h_a * (amp * amp * ex * (GAMMA / BETA) * inv_gp3)
    h_phi = inv_phi * (3.0 * (grad_h - ec * h_ec) - 2.0 * t2 * h_t)
    one_ec = 1.0 + h_ec
    e_n = ec + grad_h - (1.0 / 3.0) * radius * ec_r * one_ec - (7.0 / 3.0) * t2 * h_t
    e_z = ec_z * one_ec + phi_d * h_phi
    dn = dn_x + e_n + e_z * minus
    ds_c = total * h_t * tfac
    return dn, ds_x + ds_c, 2.0 * ds_c


def kernel(
    orb_hbm, bands_hbm, core_hbm, out_ref,
    orb, dmat_ref, lane_ref, bands_ref, part, core, x_in, x_out, summed, z_in, zf_in, zf_sum, xf_in,
    dens, grad, grad_o, flux, turned, x_line, x_res, x_back, y_line, y_res, y_back, base, final, x_fin, y_fin,
    orb_sem, core_sem, bands_sem, hop_sem, xs_sem, xr_sem, zs_sem, zr_sem, fs_sem, fr_sem,
    ps_sem, pr_sem, ys_sem, yr_sem, gs_sem, gr_sem, bs_sem, br_sem,
):
    spin = lax.axis_index("spin")
    band = lax.axis_index("band")
    grid = lax.axis_index("grid")
    bx, bz = band // NZ4, lax.rem(band, NZ4)
    gz, gy = grid // GY, lax.rem(grid, GY)

    def half_of(z):
        q = z // 2
        return 3 * q + z * (1 - 2 * q)

    q, h, e = bz // 2, half_of(bz), lax.rem(bz, 2)
    member = 2 * bx + q
    partner = (1 - spin, band, grid)

    def at_band(x, z, core=spin):
        return (core, lax.rem(x, NX4) * NZ4 + lax.rem(z, NZ4), grid)

    def copy(src, dst, send_sem, recv_sem, device):
        return pltpu.make_async_remote_copy(
            src_ref=src, dst_ref=dst, send_sem=send_sem, recv_sem=recv_sem,
            device_id=device, device_id_type=MESH,
        )

    def send(*args):
        copy(*args).start()

    def sent(like, send_sem):
        copy(like, like, send_sem, send_sem, (spin, band, grid)).wait_send()

    def arrived(like, recv_sem):
        copy(like, like, recv_sem, recv_sem, (spin, band, grid)).wait_recv()

    def rows_at(start, count):
        return pl.ds(pl.multiple_of(start, 8), count)

    bands_copy = pltpu.make_async_copy(bands_hbm, bands_ref, bands_sem)
    bands_copy.start()
    z_all = 2 * bz + gz
    near = [at_band(bx + 1, bz), at_band(bx + 3, bz)]
    near += [(spin, band, gz * GY + lax.rem(gy + d, GY)) for d in (1, 3)]
    for d in (1, 7):
        z = lax.rem(z_all + d, 8)
        near += [(spin, bx * NZ4 + z // 2, lax.rem(z, 2) * GY + gy)]
    barrier = pltpu.get_barrier_semaphore()
    across = [(1 - spin, *peer[1:]) for peer in near]
    aside = [at_band(bx, bz + d) for d in (1, 3)]
    entry = (*near, *across, partner, *aside)
    for peer in entry:
        pl.semaphore_signal(barrier, inc=1, device_id=peer, device_id_type=MESH)

    def y_of(r):
        return pl.multiple_of(lax.rem(bx + r, NX4) * YQ, YQ)

    def y_at(r):
        return pl.ds(r * YQ, YQ)

    def load(k, cs, r):
        for c in cs:
            for half in range(2):
                pltpu.make_async_copy(
                    orb_hbm.at[0, :, pl.ds(8 * half + 2 * c, 2), pl.ds(y_of(r), YQ), :],
                    orb.at[:, c, half, :, y_at(r), :],
                    orb_sem.at[k],
                ).start()

    def loaded(k, window):
        pltpu.make_async_copy(window, window, orb_sem.at[k]).wait()

    load(0, (0,), 2)
    for r in range(NX4):
        load(2, (3,), r)
    load(1, (1, 2), 2)
    for k, r in ((3, 1), (4, 3), (5, 0)):
        load(k, (0, 1, 2), r)
    core_copy = pltpu.make_async_copy(
        core_hbm.at[rows_at(8 * h, 8), rows_at(YQ * bx + 16 * q, 16), :], core, core_sem
    )
    core_copy.start()

    with jax.named_scope("first_piece"):
        bands_copy.wait()
        first = bands_ref[0, 0]
        last = first + bands_ref[0, 1]
        weights = []
        for b in range(8):
            ident = band * 8 + b
            weights.append(jnp.where((ident >= first) & (ident < last), 0.5, 1.0).astype(F32))

    def density(c, r):
        acc = None
        for b in range(8):
            v = orb[b, c, :, :, r * YQ : (r + 1) * YQ, :].astype(F32)
            term = weights[b] * (v * v)
            acc = term if acc is None else acc + term
        part[r, c] = acc

    plus, minus = at_band(bx + 1, bz), at_band(bx + 3, bz)

    def x_send(stream, c, src):
        target = minus if stream % 2 else plus
        send(src, x_in.at[c, stream], xs_sem, xr_sem.at[c, int(stream > 1)], target)

    def far(c):
        x_send(0, c, part.at[2, c, 0])
        x_send(1, c, part.at[2, c, 1])

    def direct(c):
        x_send(2, c, part.at[1, c, 1])
        x_send(3, c, part.at[3, c, 0])

    def relay(c):
        arrived(x_in.at[c, 0:2], xr_sem.at[c, 0])
        for side, r in ((0, 1), (1, 3)):
            x_out[side, c] = part[r, c, side] + x_in[c, side]
            x_send(4 + side, c, x_out.at[side, c])

    def z_targets(ds, core):
        for d in ds:
            z = lax.rem(bz + d, NZ4)
            yield d, half_of(z), rows_at(16 * (z // 2), 16), at_band(bx, z, core)

    def finish(c):
        arrived(x_in.at[c, 2:6], xr_sem.at[c, 1])
        if c == 0:
            hear(3)
        summed[c, 0] = part[0, c, 0] + x_in[c, 4] + x_in[c, 3]
        summed[c, 1] = part[0, c, 1] + x_in[c, 5] + x_in[c, 2]
        for slot, half, ys, device in z_targets((2, 1, 3, 0), 1 - spin):
            send(summed.at[c, half, :, ys, :], z_in.at[slot, c], zs_sem, zr_sem, device)

    def z_first(ds):
        for slot, half, ys, device in z_targets(ds, spin):
            send(part.at[:, 3, half, :, ys, :], zf_in.at[slot - 1], fs_sem.at[0], fr_sem.at[0], device)

    def dmat_table():
        table = derivative_matrix()
        hi = table.astype(jnp.bfloat16)
        lo = (table - hi.astype(F32)).astype(jnp.bfloat16)
        dmat_ref[...] = jnp.concatenate([hi, hi, lo], 1)
        lane_ref[...] = jnp.concatenate([hi, lo, hi], 0)

    def tell(k):
        for peer in near:
            pl.semaphore_signal(hop_sem.at[k - 1], inc=1, device_id=peer, device_id_type=MESH)

    def hear(k):
        pl.semaphore_wait(hop_sem.at[k - 1], len(near))
        if k < HOPS:
            tell(k + 1)

    loaded(0, orb.at[:, 0, :, :, y_at(2), :])
    density(0, 2)
    with jax.named_scope("barrier"):
        pl.semaphore_wait(barrier, len(entry))
    with jax.named_scope("rs_head"):
        far(0)
        for peer in aside:
            pl.semaphore_signal(hop_sem.at[HOPS], inc=1, device_id=peer, device_id_type=MESH)
        tell(1)
        loaded(2, orb.at[:, 3])
        for r in range(NX4):
            density(3, r)
        z_first((1, 3))
        loaded(1, orb.at[:, 1:3, :, :, y_at(2), :])
        density(1, 2)
        far(1)
        density(2, 2)
        far(2)
        loaded(3, orb.at[:, 0:3, :, :, y_at(1), :])
        loaded(4, orb.at[:, 0:3, :, :, y_at(3), :])
        density(0, 1)
        density(0, 3)
        direct(0)
        for c, r in ((1, 1), (1, 3), (2, 1), (2, 3)):
            density(c, r)
    with jax.named_scope("hear_z"):
        pl.semaphore_wait(hop_sem.at[HOPS], 2)
        z_first((2,))
    with jax.named_scope("rs_rest"):
        hear(1)
        loaded(5, orb.at[:, 0:3, :, :, y_at(0), :])
        for c in range(CH):
            density(c, 0)
        dmat_table()
    for c in range(CH):
        with jax.named_scope(f"relay{c}"):
            relay(c)
        if c + 1 < CH:
            direct(c + 1)
    core_copy.wait()
    with jax.named_scope("hear2"):
        hear(2)
    for c in range(CH):
        with jax.named_scope(f"finish{c}"):
            finish(c)

    y_mine = rows_at(16 * q, 16)
    with jax.named_scope("zf_wait"):
        arrived(zf_in, fr_sem.at[0])
        zf_sum[...] = part[:, 3, h, :, y_mine, :] + zf_in[0] + zf_in[1] + zf_in[2]
        for r in (2, 1, 3, 0):
            send(
                zf_sum.at[r], xf_in.at[r], fs_sem.at[1], fr_sem.at[1],
                at_band(bx + r, bz, 1 - spin),
            )
    with jax.named_scope("hear4"):
        hear(4)
    with jax.named_scope("z_wait"):
        arrived(z_in, zr_sem)
    for c in range(CH):
        block = 0.5 * core[2 * c : 2 * c + 2] + z_in[0, c] + z_in[1, c] + z_in[2, c] + z_in[3, c]
        dens[32 * c : 32 * c + 32, :] = block.reshape(32, N)
    with jax.named_scope("hear5"):
        hear(5)
    with jax.named_scope("xf_wait"):
        arrived(xf_in, fr_sem.at[1])
    block = 0.5 * core[2 * CH : 2 * CH + 2] + xf_in[0] + xf_in[1] + xf_in[2] + xf_in[3]
    dens[32 * CH : 32 * CH + 32, :] = block.reshape(32, N)

    def halves(x):
        hi = x.astype(jnp.bfloat16)
        return hi, (x - hi.astype(F32)).astype(jnp.bfloat16)

    def along_rows(x):
        hi, lo = halves(x)
        return jnp.dot(dmat_ref[...], jnp.concatenate([hi, lo, hi], 0), preferred_element_type=F32)

    def along_lanes(x):
        hi, lo = halves(x)
        return jnp.dot(jnp.concatenate([hi, hi, lo], 1), lane_ref[...], preferred_element_type=F32)

    holder = 1 - spin

    def y_exchange(src, dst, k):
        for dx, dq in ((2, 1), (1, 1), (3, 1), (0, 1), (2, 0), (1, 0), (3, 0)):
            x, place = lax.rem(bx + dx, NX4), lax.rem(q + dq, 2)
            z = h + place * (3 - 2 * h)
            send(
                src.at[rows_at(16 * (2 * x + place), 16), :], dst.at[rows_at(16 * member, 16), :],
                ys_sem.at[k], yr_sem.at[k], (holder, x * NZ4 + z, grid),
            )
        mine = rows_at(16 * member, 16)
        send(src.at[mine, :], dst.at[mine, :], ys_sem.at[k], yr_sem.at[k], partner)

    def y_wait(dst, k):
        arrived(dst, yr_sem.at[k])

    def x_exchange(src, dst, k):
        for de in (1, 0):
            for dz in (1, 0):
                for dy in (2, 1, 3, 0):
                    if (de, dz, dy) == (0, 0, 0):
                        continue
                    e2 = lax.rem(e + de, 2)
                    g2 = lax.rem(gz + dz, 2) * GY + lax.rem(gy + dy, GY)
                    z = 2 * q + e2
                    there, here = 8 * e2 + g2, 2 * grid + h
                    if k == 1:
                        there, here = 2 * g2 + half_of(z), 8 * e + grid
                    send(
                        src.at[rows_at(8 * there, 8), :], dst.at[rows_at(8 * here, 8), :],
                        gs_sem.at[k], gr_sem.at[k], (holder, bx * NZ4 + z, g2),
                    )
        mine = (2 * grid + h, 8 * e + grid)
        there, here = mine if k == 1 else mine[::-1]
        there, here = rows_at(8 * there, 8), rows_at(8 * here, 8)
        send(src.at[there, :], dst.at[here, :], gs_sem.at[k], gr_sem.at[k], partner)

    def x_wait(dst, k):
        arrived(dst, gr_sem.at[k])

    def out_y():
        xr = 8 * h + member
        for dx in (2, 1, 3, 0):
            for dz in (2, 1, 3, 0):
                b2 = lax.rem(bx + dx, NX4) * NZ4 + lax.rem(bz + dz, NZ4)
                send(
                    y_res.at[1, rows_at(8 * b2, 8), :], y_fin.at[rows_at(8 * xr, 8), :],
                    ys_sem.at[3], yr_sem.at[3], (holder, b2, grid),
                )

    def out_x():
        for dz, dy in ((1, 2), (1, 1), (1, 3), (0, 2), (1, 0), (0, 1), (0, 3), (0, 0)):
            g2 = lax.rem(gz + dz, 2) * GY + lax.rem(gy + dy, GY)
            send(
                x_res.at[1, rows_at(XR * g2, XR), :], x_fin.at[rows_at(XR * grid, XR), :],
                gs_sem.at[3], gr_sem.at[3], (holder, band, g2),
            )

    def pencils(y_src, x_src, k):
        y_exchange(y_src, y_line.at[k], 2 * k)
        for t in range(16):
            turned[k, 8 * t : 8 * t + 8, :] = x_src[pl.ds(t, 8, stride=16), :]
        x_exchange(turned.at[k], x_line.at[k], 2 * k)

    with jax.named_scope("fwd0"):
        pencils(dens, dens, 0)
        send(dens, grad_o.at[3], ps_sem, pr_sem, partner)
        grad[2] = -along_lanes(dens[...])
        send(grad.at[2], grad_o.at[2], ps_sem, pr_sem, partner)
    with jax.named_scope("drain0"):
        sent(part.at[0:3, 0:CH], xs_sem)
        sent(z_in, zs_sem)
        sent(zf_in, fs_sem.at[0])
        sent(xf_in, fs_sem.at[1])
    with jax.named_scope("y_wait0"):
        y_wait(y_line.at[0], 0)
    with jax.named_scope("y_lines0"):
        y_res[0] = along_rows(y_line[0])
        y_exchange(y_res.at[0], y_back, 1)
    with jax.named_scope("x_wait0"):
        x_wait(x_line.at[0], 0)
    with jax.named_scope("x_lines0"):
        x_res[0] = along_rows(x_line[0])
        x_exchange(x_res.at[0], x_back, 1)
    with jax.named_scope("y_back0"):
        y_wait(y_back, 1)
        send(y_back, grad_o.at[1], ps_sem, pr_sem, partner)
    with jax.named_scope("x_back0"):
        x_wait(x_back, 1)
        for i in range(8):
            grad[0, 16 * i : 16 * i + 16, :] = x_back[pl.ds(i, 16, stride=8), :]
    with jax.named_scope("swap"):
        send(grad.at[0], grad_o.at[0], ps_sem, pr_sem, partner)
        arrived(grad_o, pr_sem)

    with jax.named_scope("xc"):
        step = 16
        for i in range(0, N, step):
            rows = slice(i, i + step)
            o = (grad[0, rows, :], y_back[rows, :], grad[2, rows, :])
            g = (grad_o[0, rows, :], grad_o[1, rows, :], grad_o[2, rows, :])
            s_own = g[0] * g[0] + g[1] * g[1] + g[2] * g[2]
            s_mix = g[0] * o[0] + g[1] * o[1] + g[2] * o[2]
            s_other = o[0] * o[0] + o[1] * o[1] + o[2] * o[2]
            dn, ds, dm = xc_derivs(grad_o[3, rows, :], dens[rows, :], s_own, s_mix, s_other)
            for a in range(3):
                flux[a, rows, :] = 2.0 * ds * g[a] + dm * o[a]
            flux[3, rows, :] = dn

    with jax.named_scope("fwd1"):
        pencils(flux.at[1], flux.at[0], 1)
        base[...] = (flux[3] + along_lanes(flux[2])).reshape(8, 16, N)
        there = lax.rem(e + 1, 2)
        send(
            base.at[:, rows_at(8 * there, 8), :], final.at[h],
            bs_sem, br_sem, (spin, bx * NZ4 + 2 * q + there, grid),
        )
        final[h] = base[:, rows_at(8 * e, 8), :]
    with jax.named_scope("drain1"):
        for k in (0, 1):
            sent(y_line.at[k], ys_sem.at[k])
            sent(x_line.at[k], gs_sem.at[k])
        sent(grad_o, ps_sem)
    with jax.named_scope("y_wait1"):
        y_wait(y_line.at[1], 2)
    with jax.named_scope("y_lines1"):
        y_res[1] = along_rows(y_line[1])
        out_y()
    with jax.named_scope("x_wait1"):
        x_wait(x_line.at[1], 2)
    with jax.named_scope("x_lines1"):
        x_res[1] = along_rows(x_line[1])
        out_x()
    with jax.named_scope("drain2"):
        for k in (2, 3):
            sent(y_line.at[0], ys_sem.at[k])
            sent(x_line.at[0], gs_sem.at[k])
        sent(final.at[0], bs_sem)
        arrived(final.at[0], br_sem)
    with jax.named_scope("x_back1"):
        arrived(x_fin, gr_sem.at[3])
        for i in range(XR):
            out_ref[0, i] = final[i // 8, i % 8] - x_fin[pl.ds(i, YB, stride=XR), :]
    with jax.named_scope("y_back1"):
        arrived(y_fin, yr_sem.at[3])
    with jax.named_scope("tail"):
        out_ref[0] = out_ref[0] - y_fin[...].reshape(XR, YB, N)


def per_device(orbitals, partial_bands, core_density):
    vm = pltpu.VMEM
    sem = pltpu.SemaphoreType.DMA
    anyspace = pl.BlockSpec(memory_space=pltpu.HBM)
    return pl.pallas_call(
        kernel,
        out_shape=jax.ShapeDtypeStruct((1, XR, YB, N), F32),
        in_specs=[anyspace] * 3,
        out_specs=pl.BlockSpec(memory_space=pltpu.VMEM),
        scratch_shapes=[
            vm((8, CH + 1, 2, 2, N, N), jnp.bfloat16),
            vm((N, 3 * N), jnp.bfloat16),
            vm((3 * N, N), jnp.bfloat16),
            pltpu.SMEM((1, 2), jnp.int32),
            vm((NX4, CH + 1, 2, 2, YQ, N), F32),
            vm((8, 16, N), F32),
            vm((CH, 6, 2, YQ, N), F32),
            vm((2, CH, 2, YQ, N), F32),
            vm((CH, 2, 2, YQ, N), F32),
            vm((NZ4, CH, 2, 16, N), F32),
            vm((NZ4 - 1, NX4, 2, 16, N), F32),
            vm((NX4, 2, 16, N), F32),
            vm((NX4, 2, 16, N), F32),
            vm((N, N), F32),
            vm((3, N, N), F32),
            vm((4, N, N), F32),
            vm((4, N, N), F32),
            vm((2, N, N), F32),
            vm((2, N, N), F32),
            vm((2, N, N), F32),
            vm((N, N), F32),
            vm((2, N, N), F32),
            vm((2, N, N), F32),
            vm((N, N), F32),
            vm((8, 16, N), F32),
            vm((2, 8, YB, N), F32),
            vm((N, N), F32),
            vm((N, N), F32),
            sem((6,)),
            sem,
            sem,
            pltpu.SemaphoreType.REGULAR((HOPS + 1,)),
            sem,
            sem((CH, 2)),
            sem,
            sem,
            sem((2,)),
            sem((2,)),
            sem,
            sem,
            sem((4,)),
            sem((4,)),
            sem((4,)),
            sem((4,)),
            sem,
            sem,
        ],
        compiler_params=pltpu.CompilerParams(
            collective_id=0, has_side_effects=True, vmem_limit_bytes=54400 * 1024
        ),
    )(orbitals, partial_bands, core_density)


def solution(mesh):
    in_specs = (P("spin", "band", "grid", None, None), P("spin", None), P("grid", None, None))
    out_specs = P("spin", "grid", "band", None)

    return jax.shard_map(
        per_device, mesh=mesh, in_specs=in_specs, out_specs=out_specs, check_vma=False
    )
```

```python
import math

import jax
import jax.numpy as jnp
from jax import lax
from jax.experimental import pallas as pl
from jax.experimental.pallas import tpu as pltpu
from jax.sharding import PartitionSpec as P

KAPPA = 0.804
MU_X = 0.2195149727645171
BETA = 0.06672455060314922
GAMMA = (1.0 - math.log(2.0)) / math.pi**2
FZ_NORM = 2.0 ** (4.0 / 3.0) - 2.0
FPP_ZERO = 1.709921

MESH = pl.DeviceIdType.MESH
F32 = jnp.float32
N = 128
XR = 16
NX4 = 4
NZ4 = 4
GY = 4
GRID = 2 * GY
BAND = NX4 * NZ4
YB = N // BAND
YQ = N // NX4
CH = 3
HOPS = 5


def derivative_matrix():
    k = lax.broadcasted_iota(jnp.int32, (N, N), 0) - lax.broadcasted_iota(jnp.int32, (N, N), 1)
    far = jnp.abs(k)
    near = jnp.minimum(far, N - far)
    angle = (math.pi / N) * jnp.maximum(near, 1).astype(F32)
    size = (math.pi / N) * jnp.cos(angle) / jnp.sin(angle)
    flips = (k < 0).astype(jnp.int32) + (far > N // 2).astype(jnp.int32) + (far & 1)
    signed = jnp.where((flips & 1) == 1, -size, size)
    return jnp.where(k == 0, 0.0, signed)


def pw_fit(r, root, amp, alpha, b1, b2, b3, b4):
    denom = (2.0 * amp) * (root * (b1 + root * (b2 + root * (b3 + root * b4))))
    slope = (2.0 * amp) * (0.5 * b1 / root + (b2 + root * (1.5 * b3 + root * (2.0 * b4))))
    log = jnp.log(1.0 + 1.0 / denom)
    front = (-2.0 * amp) * (1.0 + alpha * r)
    value = front * log
    deriv = (-2.0 * amp * alpha) * log - front * slope / (denom * (denom + 1.0))
    return value, deriv


def cbrt(x):
    return jnp.exp(jnp.log(x) * (1.0 / 3.0))


def xc_derivs(own, other, s_own, s_mix, s_other):
    total = own + other
    inv_n = 1.0 / total
    c_own = cbrt(own)
    c_other = cbrt(other)
    c_tot = cbrt(total)
    inv_c = 1.0 / c_tot
    double = 2.0 * own
    kf = (6.0 * math.pi**2) ** (1.0 / 3.0) * c_own
    inv_kn = 1.0 / (kf * double)
    s2 = s_own * inv_kn * inv_kn
    inv_den = 1.0 / (1.0 + (MU_X / KAPPA) * s2)
    enh = (1.0 + KAPPA) - KAPPA * inv_den
    enh_d = MU_X * inv_den * inv_den
    dn_x = (-1.0 / math.pi) * kf * (enh - 2.0 * s2 * enh_d)
    ds_x = (-3.0 / (8.0 * math.pi)) * enh_d * inv_kn
    two13 = 2.0 ** (1.0 / 3.0)
    plus = double * inv_n
    minus = 2.0 * other * inv_n
    zeta = (own - other) * inv_n
    plus13 = two13 * c_own * inv_c
    minus13 = two13 * c_other * inv_c
    radius = (3.0 / (4.0 * math.pi)) ** (1.0 / 3.0) * inv_c
    root = jnp.sqrt(radius)
    ec0, ec0_r = pw_fit(radius, root, 0.031091, 0.2137, 7.5957, 3.5876, 1.6382, 0.49294)
    ec1, ec1_r = pw_fit(radius, root, 0.015545, 0.20548, 14.1189, 6.1977, 3.3662, 0.62517)
    ac, ac_r = pw_fit(radius, root, 0.016887, 0.11125, 10.357, 3.6231, 0.88026, 0.49671)
    fz = (plus * plus13 + minus * minus13 - 2.0) * (1.0 / FZ_NORM)
    fz_d = (4.0 / 3.0 / FZ_NORM) * (plus13 - minus13)
    z2 = zeta * zeta
    z3 = z2 * zeta
    z4 = z2 * z2
    w1 = (-1.0 / FPP_ZERO) * (1.0 - z4)
    diff = ec1 - ec0
    mix = ac * w1 + diff * z4
    ec = ec0 + fz * mix
    ec_r = ec0_r + fz * (ac_r * w1 + (ec1_r - ec0_r) * z4)
    ec_z = fz_d * mix + 4.0 * z3 * fz * (ac * (1.0 / FPP_ZERO) + diff)
    phi = 0.5 * (plus13 * plus13 + minus13 * minus13)
    phi_d = (1.0 / 3.0) * (1.0 / plus13 - 1.0 / minus13)
    inv_phi = 1.0 / phi
    phi3 = phi * phi * phi
    kf_tot = (3.0 * math.pi**2) ** (1.0 / 3.0)
    tfac = (math.pi / (16.0 * kf_tot)) * inv_phi * inv_phi * inv_c * inv_n * inv_n
    sigma = s_own + 2.0 * s_mix + s_other
    t2 = sigma * tfac
    inv_gp3 = (1.0 / GAMMA) * inv_phi * inv_phi * inv_phi
    ex = jnp.exp(-ec * inv_gp3)
    amp = (BETA / GAMMA) / (ex - 1.0)
    y = amp * t2
    den = 1.0 + y + y * y
    inv_d = 1.0 / den
    ct = (BETA / GAMMA) * t2
    q = ct * (1.0 + y) * inv_d
    grad_h = GAMMA * phi3 * jnp.log(1.0 + q)
    scale = GAMMA * phi3 / (1.0 + q) * inv_d * inv_d
    h_t = scale * ((BETA / GAMMA) * (1.0 + 2.0 * y))
    h_a = -scale * (ct * t2) * (y * (2.0 + y))
    h_ec = h_a * (amp * amp * ex * (GAMMA / BETA) * inv_gp3)
    h_phi = inv_phi * (3.0 * (grad_h - ec * h_ec) - 2.0 * t2 * h_t)
    one_ec = 1.0 + h_ec
    e_n = ec + grad_h - (1.0 / 3.0) * radius * ec_r * one_ec - (7.0 / 3.0) * t2 * h_t
    e_z = ec_z * one_ec + phi_d * h_phi
    dn = dn_x + e_n + e_z * minus
    ds_c = total * h_t * tfac
    return dn, ds_x + ds_c, 2.0 * ds_c


def kernel(
    orb_hbm, bands_hbm, core_hbm, out_ref,
    orb, dmat_ref, lane_ref, bands_ref, part, core, x_in, x_out, summed, z_in, zf_in, zf_sum, xf_in,
    dens, grad, grad_o, flux, turned, x_line, x_res, x_back, y_line, y_res, y_back, base, final, x_fin, y_fin,
    orb_sem, core_sem, bands_sem, hop_sem, xs_sem, xr_sem, zs_sem, zr_sem, fs_sem, fr_sem,
    ps_sem, pr_sem, ys_sem, yr_sem, gs_sem, gr_sem, bs_sem, br_sem,
):
    spin = lax.axis_index("spin")
    band = lax.axis_index("band")
    grid = lax.axis_index("grid")
    bx, bz = band // NZ4, lax.rem(band, NZ4)
    gz, gy = grid // GY, lax.rem(grid, GY)

    def half_of(z):
        q = z // 2
        return 3 * q + z * (1 - 2 * q)

    q, h, e = bz // 2, half_of(bz), lax.rem(bz, 2)
    member = 2 * bx + q
    partner = (1 - spin, band, grid)

    def at_band(x, z, core=spin):
        return (core, lax.rem(x, NX4) * NZ4 + lax.rem(z, NZ4), grid)

    def copy(src, dst, send_sem, recv_sem, device):
        return pltpu.make_async_remote_copy(
            src_ref=src, dst_ref=dst, send_sem=send_sem, recv_sem=recv_sem,
            device_id=device, device_id_type=MESH,
        )

    def send(*args):
        copy(*args).start()

    def sent(like, send_sem):
        copy(like, like, send_sem, send_sem, (spin, band, grid)).wait_send()

    def arrived(like, recv_sem):
        copy(like, like, recv_sem, recv_sem, (spin, band, grid)).wait_recv()

    def rows_at(start, count):
        return pl.ds(pl.multiple_of(start, 8), count)

    bands_copy = pltpu.make_async_copy(bands_hbm, bands_ref, bands_sem)
    bands_copy.start()
    z_all = 2 * bz + gz
    near = [at_band(bx + 1, bz), at_band(bx + 3, bz)]
    near += [(spin, band, gz * GY + lax.rem(gy + d, GY)) for d in (1, 3)]
    for d in (1, 7):
        z = lax.rem(z_all + d, 8)
        near += [(spin, bx * NZ4 + z // 2, lax.rem(z, 2) * GY + gy)]
    barrier = pltpu.get_barrier_semaphore()
    across = [(1 - spin, *peer[1:]) for peer in near]
    aside = [at_band(bx, bz + d) for d in (1, 3)]
    entry = (*near, *across, partner, *aside)
    for peer in entry:
        pl.semaphore_signal(barrier, inc=1, device_id=peer, device_id_type=MESH)

    def y_of(r):
        return pl.multiple_of(lax.rem(bx + r, NX4) * YQ, YQ)

    def y_at(r):
        return pl.ds(r * YQ, YQ)

    def load(k, cs, r):
        for c in cs:
            for half in range(2):
                pltpu.make_async_copy(
                    orb_hbm.at[0, :, pl.ds(8 * half + 2 * c, 2), pl.ds(y_of(r), YQ), :],
                    orb.at[:, c, half, :, y_at(r), :],
                    orb_sem.at[k],
                ).start()

    def loaded(k, window):
        pltpu.make_async_copy(window, window, orb_sem.at[k]).wait()

    load(0, (0,), 2)
    for r in range(NX4):
        load(2, (3,), r)
    load(1, (1, 2), 2)
    for k, r in ((3, 1), (4, 3), (5, 0)):
        load(k, (0, 1, 2), r)
    core_copy = pltpu.make_async_copy(
        core_hbm.at[rows_at(8 * h, 8), rows_at(YQ * bx + 16 * q, 16), :], core, core_sem
    )
    core_copy.start()

    with jax.named_scope("first_piece"):
        bands_copy.wait()
        first = bands_ref[0, 0]
        last = first + bands_ref[0, 1]
        weights = []
        for b in range(8):
            ident = band * 8 + b
            weights.append(jnp.where((ident >= first) & (ident < last), 0.5, 1.0).astype(F32))

    def density(c, r):
        acc = None
        for b in range(8):
            v = orb[b, c, :, :, r * YQ : (r + 1) * YQ, :].astype(F32)
            term = weights[b] * (v * v)
            acc = term if acc is None else acc + term
        part[r, c] = acc

    plus, minus = at_band(bx + 1, bz), at_band(bx + 3, bz)

    def x_send(stream, c, src):
        target = minus if stream % 2 else plus
        send(src, x_in.at[c, stream], xs_sem, xr_sem.at[c, int(stream > 1)], target)

    def far(c):
        x_send(0, c, part.at[2, c, 0])
        x_send(1, c, part.at[2, c, 1])

    def direct(c):
        x_send(2, c, part.at[1, c, 1])
        x_send(3, c, part.at[3, c, 0])

    def relay(c):
        arrived(x_in.at[c, 0:2], xr_sem.at[c, 0])
        for side, r in ((0, 1), (1, 3)):
            x_out[side, c] = part[r, c, side] + x_in[c, side]
            x_send(4 + side, c, x_out.at[side, c])

    def z_targets(ds, core):
        for d in ds:
            z = lax.rem(bz + d, NZ4)
            yield d, half_of(z), rows_at(16 * (z // 2), 16), at_band(bx, z, core)

    def finish(c):
        arrived(x_in.at[c, 2:6], xr_sem.at[c, 1])
        if c == 0:
            hear(3)
        summed[c, 0] = part[0, c, 0] + x_in[c, 4] + x_in[c, 3]
        summed[c, 1] = part[0, c, 1] + x_in[c, 5] + x_in[c, 2]
        for slot, half, ys, device in z_targets((2, 1, 3, 0), 1 - spin):
            send(summed.at[c, half, :, ys, :], z_in.at[slot, c], zs_sem, zr_sem, device)

    def z_first(ds):
        for slot, half, ys, device in z_targets(ds, spin):
            send(part.at[:, 3, half, :, ys, :], zf_in.at[slot - 1], fs_sem.at[0], fr_sem.at[0], device)

    def dmat_table():
        table = derivative_matrix()
        hi = table.astype(jnp.bfloat16)
        lo = (table - hi.astype(F32)).astype(jnp.bfloat16)
        dmat_ref[...] = jnp.concatenate([hi, hi, lo], 1)
        lane_ref[...] = jnp.concatenate([hi, lo, hi], 0)

    def tell(k):
        for peer in near:
            pl.semaphore_signal(hop_sem.at[k - 1], inc=1, device_id=peer, device_id_type=MESH)

    def hear(k):
        pl.semaphore_wait(hop_sem.at[k - 1], len(near))
        if k < HOPS:
            tell(k + 1)

    loaded(0, orb.at[:, 0, :, :, y_at(2), :])
    density(0, 2)
    with jax.named_scope("barrier"):
        pl.semaphore_wait(barrier, len(entry))
    with jax.named_scope("rs_head"):
        far(0)
        for peer in aside:
            pl.semaphore_signal(hop_sem.at[HOPS], inc=1, device_id=peer, device_id_type=MESH)
        tell(1)
        loaded(2, orb.at[:, 3])
        for r in range(NX4):
            density(3, r)
        z_first((1, 3))
        loaded(1, orb.at[:, 1:3, :, :, y_at(2), :])
        density(1, 2)
        far(1)
        density(2, 2)
        far(2)
        loaded(3, orb.at[:, 0:3, :, :, y_at(1), :])
        loaded(4, orb.at[:, 0:3, :, :, y_at(3), :])
        density(0, 1)
        density(0, 3)
        direct(0)
        for c, r in ((1, 1), (1, 3), (2, 1), (2, 3)):
            density(c, r)
    with jax.named_scope("hear_z"):
        pl.semaphore_wait(hop_sem.at[HOPS], 2)
        z_first((2,))
    with jax.named_scope("rs_rest"):
        hear(1)
        loaded(5, orb.at[:, 0:3, :, :, y_at(0), :])
        for c in range(CH):
            density(c, 0)
        dmat_table()
    for c in range(CH):
        with jax.named_scope(f"relay{c}"):
            relay(c)
        if c + 1 < CH:
            direct(c + 1)
    core_copy.wait()
    with jax.named_scope("hear2"):
        hear(2)
    for c in range(CH):
        with jax.named_scope(f"finish{c}"):
            finish(c)

    y_mine = rows_at(16 * q, 16)
    with jax.named_scope("zf_wait"):
        arrived(zf_in, fr_sem.at[0])
        zf_sum[...] = part[:, 3, h, :, y_mine, :] + zf_in[0] + zf_in[1] + zf_in[2]
        for r in (2, 1, 3, 0):
            send(
                zf_sum.at[r], xf_in.at[r], fs_sem.at[1], fr_sem.at[1],
                at_band(bx + r, bz, 1 - spin),
            )
    with jax.named_scope("hear4"):
        hear(4)
    with jax.named_scope("z_wait"):
        arrived(z_in, zr_sem)
    for c in range(CH):
        block = 0.5 * core[2 * c : 2 * c + 2] + z_in[0, c] + z_in[1, c] + z_in[2, c] + z_in[3, c]
        dens[32 * c : 32 * c + 32, :] = block.reshape(32, N)
    with jax.named_scope("hear5"):
        hear(5)
    with jax.named_scope("xf_wait"):
        arrived(xf_in, fr_sem.at[1])
    block = 0.5 * core[2 * CH : 2 * CH + 2] + xf_in[0] + xf_in[1] + xf_in[2] + xf_in[3]
    dens[32 * CH : 32 * CH + 32, :] = block.reshape(32, N)

    def halves(x):
        hi = x.astype(jnp.bfloat16)
        return hi, (x - hi.astype(F32)).astype(jnp.bfloat16)

    def along_rows(x):
        hi, lo = halves(x)
        return jnp.dot(dmat_ref[...], jnp.concatenate([hi, lo, hi], 0), preferred_element_type=F32)

    def along_lanes(x):
        hi, lo = halves(x)
        return jnp.dot(jnp.concatenate([hi, hi, lo], 1), lane_ref[...], preferred_element_type=F32)

    holder = 1 - spin

    def y_exchange(src, dst, k):
        for dx, dq in ((2, 1), (1, 1), (3, 1), (0, 1), (2, 0), (1, 0), (3, 0)):
            x, place = lax.rem(bx + dx, NX4), lax.rem(q + dq, 2)
            z = h + place * (3 - 2 * h)
            send(
                src.at[rows_at(16 * (2 * x + place), 16), :], dst.at[rows_at(16 * member, 16), :],
                ys_sem.at[k], yr_sem.at[k], (holder, x * NZ4 + z, grid),
            )
        mine = rows_at(16 * member, 16)
        send(src.at[mine, :], dst.at[mine, :], ys_sem.at[k], yr_sem.at[k], partner)

    def y_wait(dst, k):
        arrived(dst, yr_sem.at[k])

    def x_exchange(src, dst, k):
        for de in (1, 0):
            for dz in (1, 0):
                for dy in (2, 1, 3, 0):
                    if (de, dz, dy) == (0, 0, 0):
                        continue
                    e2 = lax.rem(e + de, 2)
                    g2 = lax.rem(gz + dz, 2) * GY + lax.rem(gy + dy, GY)
                    z = 2 * q + e2
                    there, here = 8 * e2 + g2, 2 * grid + h
                    if k == 1:
                        there, here = 2 * g2 + half_of(z), 8 * e + grid
                    send(
                        src.at[rows_at(8 * there, 8), :], dst.at[rows_at(8 * here, 8), :],
                        gs_sem.at[k], gr_sem.at[k], (holder, bx * NZ4 + z, g2),
                    )
        mine = (2 * grid + h, 8 * e + grid)
        there, here = mine if k == 1 else mine[::-1]
        there, here = rows_at(8 * there, 8), rows_at(8 * here, 8)
        send(src.at[there, :], dst.at[here, :], gs_sem.at[k], gr_sem.at[k], partner)

    def x_wait(dst, k):
        arrived(dst, gr_sem.at[k])

    def out_y():
        xr = 8 * h + member
        for dx in (2, 1, 3, 0):
            for dz in (2, 1, 3, 0):
                b2 = lax.rem(bx + dx, NX4) * NZ4 + lax.rem(bz + dz, NZ4)
                send(
                    y_res.at[1, rows_at(8 * b2, 8), :], y_fin.at[rows_at(8 * xr, 8), :],
                    ys_sem.at[3], yr_sem.at[3], (holder, b2, grid),
                )

    def out_x():
        for dz, dy in ((1, 2), (1, 1), (1, 3), (0, 2), (1, 0), (0, 1), (0, 3), (0, 0)):
            g2 = lax.rem(gz + dz, 2) * GY + lax.rem(gy + dy, GY)
            send(
                x_res.at[1, rows_at(XR * g2, XR), :], x_fin.at[rows_at(XR * grid, XR), :],
                gs_sem.at[3], gr_sem.at[3], (holder, band, g2),
            )

    def pencils(y_src, x_src, k):
        y_exchange(y_src, y_line.at[k], 2 * k)
        for t in range(16):
            turned[k, 8 * t : 8 * t + 8, :] = x_src[pl.ds(t, 8, stride=16), :]
        x_exchange(turned.at[k], x_line.at[k], 2 * k)

    with jax.named_scope("fwd0"):
        pencils(dens, dens, 0)
        send(dens, grad_o.at[3], ps_sem, pr_sem, partner)
        grad[2] = -along_lanes(dens[...])
        send(grad.at[2], grad_o.at[2], ps_sem, pr_sem, partner)
    with jax.named_scope("drain0"):
        sent(part.at[0:3, 0:CH], xs_sem)
        sent(z_in, zs_sem)
        sent(zf_in, fs_sem.at[0])
        sent(xf_in, fs_sem.at[1])
    with jax.named_scope("y_wait0"):
        y_wait(y_line.at[0], 0)
    with jax.named_scope("y_lines0"):
        y_res[0] = along_rows(y_line[0])
        y_exchange(y_res.at[0], y_back, 1)
    with jax.named_scope("x_wait0"):
        x_wait(x_line.at[0], 0)
    with jax.named_scope("x_lines0"):
        x_res[0] = along_rows(x_line[0])
        x_exchange(x_res.at[0], x_back, 1)
    with jax.named_scope("y_back0"):
        y_wait(y_back, 1)
        send(y_back, grad_o.at[1], ps_sem, pr_sem, partner)
    with jax.named_scope("x_back0"):
        x_wait(x_back, 1)
        for i in range(8):
            grad[0, 16 * i : 16 * i + 16, :] = x_back[pl.ds(i, 16, stride=8), :]
    with jax.named_scope("swap"):
        send(grad.at[0], grad_o.at[0], ps_sem, pr_sem, partner)
        arrived(grad_o, pr_sem)

    with jax.named_scope("xc"):
        step = 16
        for i in range(0, N, step):
            rows = slice(i, i + step)
            o = (grad[0, rows, :], y_back[rows, :], grad[2, rows, :])
            g = (grad_o[0, rows, :], grad_o[1, rows, :], grad_o[2, rows, :])
            s_own = g[0] * g[0] + g[1] * g[1] + g[2] * g[2]
            s_mix = g[0] * o[0] + g[1] * o[1] + g[2] * o[2]
            s_other = o[0] * o[0] + o[1] * o[1] + o[2] * o[2]
            dn, ds, dm = xc_derivs(grad_o[3, rows, :], dens[rows, :], s_own, s_mix, s_other)
            for a in range(3):
                flux[a, rows, :] = 2.0 * ds * g[a] + dm * o[a]
            flux[3, rows, :] = dn

    with jax.named_scope("fwd1"):
        pencils(flux.at[1], flux.at[0], 1)
        base[...] = (flux[3] + along_lanes(flux[2])).reshape(8, 16, N)
        there = lax.rem(e + 1, 2)
        send(
            base.at[:, rows_at(8 * there, 8), :], final.at[h],
            bs_sem, br_sem, (spin, bx * NZ4 + 2 * q + there, grid),
        )
        final[h] = base[:, rows_at(8 * e, 8), :]
    with jax.named_scope("drain1"):
        for k in (0, 1):
            sent(y_line.at[k], ys_sem.at[k])
            sent(x_line.at[k], gs_sem.at[k])
        sent(grad_o, ps_sem)
    with jax.named_scope("y_wait1"):
        y_wait(y_line.at[1], 2)
    with jax.named_scope("y_lines1"):
        y_res[1] = along_rows(y_line[1])
        out_y()
    with jax.named_scope("x_wait1"):
        x_wait(x_line.at[1], 2)
    with jax.named_scope("x_lines1"):
        x_res[1] = along_rows(x_line[1])
        out_x()
    with jax.named_scope("drain2"):
        for k in (2, 3):
            sent(y_line.at[0], ys_sem.at[k])
            sent(x_line.at[0], gs_sem.at[k])
        sent(final.at[0], bs_sem)
        arrived(final.at[0], br_sem)
    with jax.named_scope("x_back1"):
        arrived(x_fin, gr_sem.at[3])
        for i in range(XR):
            out_ref[0, i] = final[i // 8, i % 8] - x_fin[pl.ds(i, YB, stride=XR), :]
    with jax.named_scope("y_back1"):
        arrived(y_fin, yr_sem.at[3])
    with jax.named_scope("tail"):
        out_ref[0] = out_ref[0] - y_fin[...].reshape(XR, YB, N)


def per_device(orbitals, partial_bands, core_density):
    vm = pltpu.VMEM
    sem = pltpu.SemaphoreType.DMA
    anyspace = pl.BlockSpec(memory_space=pltpu.HBM)
    return pl.pallas_call(
        kernel,
        out_shape=jax.ShapeDtypeStruct((1, XR, YB, N), F32),
        in_specs=[anyspace] * 3,
        out_specs=pl.BlockSpec(memory_space=pltpu.VMEM),
        scratch_shapes=[
            vm((8, CH + 1, 2, 2, N, N), jnp.bfloat16),
            vm((N, 3 * N), jnp.bfloat16),
            vm((3 * N, N), jnp.bfloat16),
            pltpu.SMEM((1, 2), jnp.int32),
            vm((NX4, CH + 1, 2, 2, YQ, N), F32),
            vm((8, 16, N), F32),
            vm((CH, 6, 2, YQ, N), F32),
            vm((2, CH, 2, YQ, N), F32),
            vm((CH, 2, 2, YQ, N), F32),
            vm((NZ4, CH, 2, 16, N), F32),
            vm((NZ4 - 1, NX4, 2, 16, N), F32),
            vm((NX4, 2, 16, N), F32),
            vm((NX4, 2, 16, N), F32),
            vm((N, N), F32),
            vm((3, N, N), F32),
            vm((4, N, N), F32),
            vm((4, N, N), F32),
            vm((2, N, N), F32),
            vm((2, N, N), F32),
            vm((2, N, N), F32),
            vm((N, N), F32),
            vm((2, N, N), F32),
            vm((2, N, N), F32),
            vm((N, N), F32),
            vm((8, 16, N), F32),
            vm((2, 8, YB, N), F32),
            vm((N, N), F32),
            vm((N, N), F32),
            sem((6,)),
            sem,
            sem,
            pltpu.SemaphoreType.REGULAR((HOPS + 1,)),
            sem,
            sem((CH, 2)),
            sem,
            sem,
            sem((2,)),
            sem((2,)),
            sem,
            sem,
            sem((4,)),
            sem((4,)),
            sem((4,)),
            sem((4,)),
            sem,
            sem,
        ],
        compiler_params=pltpu.CompilerParams(
            collective_id=0, has_side_effects=True, vmem_limit_bytes=54400 * 1024
        ),
    )(*[pltpu.with_memory_space_constraint(a, pltpu.HBM) for a in (orbitals, partial_bands, core_density)])


def solution(mesh):
    in_specs = (P("spin", "band", "grid", None, None), P("spin", None), P("grid", None, None))
    out_specs = P("spin", "grid", "band", None)

    return jax.shard_map(
        per_device, mesh=mesh, in_specs=in_specs, out_specs=out_specs, check_vma=False
    )
```

```python
import math

import jax
import jax.numpy as jnp
from jax import lax
from jax.experimental import pallas as pl
from jax.experimental.pallas import tpu as pltpu
from jax.sharding import PartitionSpec as P

KAPPA = 0.804
MU_X = 0.2195149727645171
BETA = 0.06672455060314922
GAMMA = (1.0 - math.log(2.0)) / math.pi**2
FZ_NORM = 2.0 ** (4.0 / 3.0) - 2.0
FPP_ZERO = 1.709921

MESH = pl.DeviceIdType.MESH
F32 = jnp.float32
N = 128
XR = 16
NX4 = 4
NZ4 = 4
GY = 4
GRID = 2 * GY
BAND = NX4 * NZ4
YB = N // BAND
YQ = N // NX4
CH = 3
HOPS = 5


def derivative_matrix():
    k = lax.broadcasted_iota(jnp.int32, (N, N), 0) - lax.broadcasted_iota(jnp.int32, (N, N), 1)
    far = jnp.abs(k)
    near = jnp.minimum(far, N - far)
    angle = (math.pi / N) * jnp.maximum(near, 1).astype(F32)
    size = (math.pi / N) * jnp.cos(angle) / jnp.sin(angle)
    flips = (k < 0).astype(jnp.int32) + (far > N // 2).astype(jnp.int32) + (far & 1)
    signed = jnp.where((flips & 1) == 1, -size, size)
    return jnp.where(k == 0, 0.0, signed)


def pw_fit(r, root, amp, alpha, b1, b2, b3, b4):
    denom = (2.0 * amp) * (root * (b1 + root * (b2 + root * (b3 + root * b4))))
    slope = (2.0 * amp) * (0.5 * b1 / root + (b2 + root * (1.5 * b3 + root * (2.0 * b4))))
    log = jnp.log(1.0 + 1.0 / denom)
    front = (-2.0 * amp) * (1.0 + alpha * r)
    value = front * log
    deriv = (-2.0 * amp * alpha) * log - front * slope / (denom * (denom + 1.0))
    return value, deriv


def cbrt(x):
    return jnp.exp(jnp.log(x) * (1.0 / 3.0))


def xc_prepare(own, other):
    total = own + other
    inv_n = 1.0 / total
    c_own = cbrt(own)
    c_other = cbrt(other)
    c_tot = cbrt(total)
    inv_c = 1.0 / c_tot
    double = 2.0 * own
    kf = (6.0 * math.pi**2) ** (1.0 / 3.0) * c_own
    inv_kn = 1.0 / (kf * double)
    two13 = 2.0 ** (1.0 / 3.0)
    plus = double * inv_n
    minus = 2.0 * other * inv_n
    zeta = (own - other) * inv_n
    plus13 = two13 * c_own * inv_c
    minus13 = two13 * c_other * inv_c
    radius = (3.0 / (4.0 * math.pi)) ** (1.0 / 3.0) * inv_c
    root = jnp.sqrt(radius)
    ec0, ec0_r = pw_fit(radius, root, 0.031091, 0.2137, 7.5957, 3.5876, 1.6382, 0.49294)
    ec1, ec1_r = pw_fit(radius, root, 0.015545, 0.20548, 14.1189, 6.1977, 3.3662, 0.62517)
    ac, ac_r = pw_fit(radius, root, 0.016887, 0.11125, 10.357, 3.6231, 0.88026, 0.49671)
    fz = (plus * plus13 + minus * minus13 - 2.0) * (1.0 / FZ_NORM)
    fz_d = (4.0 / 3.0 / FZ_NORM) * (plus13 - minus13)
    z2 = zeta * zeta
    z3 = z2 * zeta
    z4 = z2 * z2
    w1 = (-1.0 / FPP_ZERO) * (1.0 - z4)
    diff = ec1 - ec0
    mix = ac * w1 + diff * z4
    ec = ec0 + fz * mix
    ec_r = ec0_r + fz * (ac_r * w1 + (ec1_r - ec0_r) * z4)
    ec_z = fz_d * mix + 4.0 * z3 * fz * (ac * (1.0 / FPP_ZERO) + diff)
    phi = 0.5 * (plus13 * plus13 + minus13 * minus13)
    phi_d = (1.0 / 3.0) * (1.0 / plus13 - 1.0 / minus13)
    inv_phi = 1.0 / phi
    gp3 = GAMMA * phi * phi * phi
    kf_tot = (3.0 * math.pi**2) ** (1.0 / 3.0)
    tfac = (math.pi / (16.0 * kf_tot)) * inv_phi * inv_phi * inv_c * inv_n * inv_n
    inv_gp3 = (1.0 / GAMMA) * inv_phi * inv_phi * inv_phi
    ex = jnp.exp(-ec * inv_gp3)
    amp = (BETA / GAMMA) / (ex - 1.0)
    amp_ec = amp * amp * ex * (GAMMA / BETA) * inv_gp3
    drift = (1.0 / 3.0) * radius * ec_r
    return kf, inv_kn, ec, drift, ec_z, minus, gp3, tfac, amp, amp_ec, phi_d * inv_phi, total


PREPARED = 12


def xc_derivs(prepared, s_own, s_mix, s_other):
    kf, inv_kn, ec, drift, ec_z, minus, gp3, tfac, amp, amp_ec, phi_r, total = prepared
    s2 = s_own * inv_kn * inv_kn
    inv_den = 1.0 / (1.0 + (MU_X / KAPPA) * s2)
    enh = (1.0 + KAPPA) - KAPPA * inv_den
    enh_d = MU_X * inv_den * inv_den
    dn_x = (-1.0 / math.pi) * kf * (enh - 2.0 * s2 * enh_d)
    ds_x = (-3.0 / (8.0 * math.pi)) * enh_d * inv_kn
    sigma = s_own + 2.0 * s_mix + s_other
    t2 = sigma * tfac
    y = amp * t2
    den = 1.0 + y + y * y
    inv_d = 1.0 / den
    ct = (BETA / GAMMA) * t2
    q = ct * (1.0 + y) * inv_d
    grad_h = gp3 * jnp.log(1.0 + q)
    scale = gp3 / (1.0 + q) * inv_d * inv_d
    h_t = scale * ((BETA / GAMMA) * (1.0 + 2.0 * y))
    h_a = -scale * (ct * t2) * (y * (2.0 + y))
    h_ec = h_a * amp_ec
    one_ec = 1.0 + h_ec
    e_n = ec + grad_h - drift * one_ec - (7.0 / 3.0) * t2 * h_t
    e_z = ec_z * one_ec + phi_r * (3.0 * (grad_h - ec * h_ec) - 2.0 * t2 * h_t)
    dn = dn_x + e_n + e_z * minus
    ds_c = total * h_t * tfac
    return dn, ds_x + ds_c, 2.0 * ds_c


def kernel(
    orb_hbm, bands_hbm, core_hbm, out_ref,
    orb, dmat_ref, lane_ref, bands_ref, part, core, x_in, x_out, summed, z_in, zf_in, zf_sum, xf_in,
    dens, dens_o, prepared, grad, grad_o, flux, turned, x_line, x_res, x_back, y_line, y_res, y_back, base, final, x_fin, y_fin,
    orb_sem, core_sem, bands_sem, hop_sem, xs_sem, xr_sem, zs_sem, zr_sem, fs_sem, fr_sem,
    ps_sem, pr_sem, ys_sem, yr_sem, gs_sem, gr_sem, bs_sem, br_sem,
):
    spin = lax.axis_index("spin")
    band = lax.axis_index("band")
    grid = lax.axis_index("grid")
    bx, bz = band // NZ4, lax.rem(band, NZ4)
    gz, gy = grid // GY, lax.rem(grid, GY)

    def half_of(z):
        q = z // 2
        return 3 * q + z * (1 - 2 * q)

    q, h, e = bz // 2, half_of(bz), lax.rem(bz, 2)
    member = 2 * bx + q
    partner = (1 - spin, band, grid)

    def at_band(x, z, core=spin):
        return (core, lax.rem(x, NX4) * NZ4 + lax.rem(z, NZ4), grid)

    def copy(src, dst, send_sem, recv_sem, device):
        return pltpu.make_async_remote_copy(
            src_ref=src, dst_ref=dst, send_sem=send_sem, recv_sem=recv_sem,
            device_id=device, device_id_type=MESH,
        )

    def send(*args):
        copy(*args).start()

    def sent(like, send_sem):
        copy(like, like, send_sem, send_sem, (spin, band, grid)).wait_send()

    def arrived(like, recv_sem):
        copy(like, like, recv_sem, recv_sem, (spin, band, grid)).wait_recv()

    def rows_at(start, count):
        return pl.ds(pl.multiple_of(start, 8), count)

    bands_copy = pltpu.make_async_copy(bands_hbm, bands_ref, bands_sem)
    bands_copy.start()
    z_all = 2 * bz + gz
    near = [at_band(bx + 1, bz), at_band(bx + 3, bz)]
    near += [(spin, band, gz * GY + lax.rem(gy + d, GY)) for d in (1, 3)]
    for d in (1, 7):
        z = lax.rem(z_all + d, 8)
        near += [(spin, bx * NZ4 + z // 2, lax.rem(z, 2) * GY + gy)]
    barrier = pltpu.get_barrier_semaphore()
    across = [(1 - spin, *peer[1:]) for peer in near]
    aside = [at_band(bx, bz + d) for d in (1, 3)]
    entry = (*near, *across, partner, *aside)
    for peer in entry:
        pl.semaphore_signal(barrier, inc=1, device_id=peer, device_id_type=MESH)

    def y_of(r):
        return pl.multiple_of(lax.rem(bx + r, NX4) * YQ, YQ)

    def y_at(r):
        return pl.ds(r * YQ, YQ)

    def load(k, cs, r):
        for c in cs:
            for half in range(2):
                pltpu.make_async_copy(
                    orb_hbm.at[0, :, pl.ds(8 * half + 2 * c, 2), pl.ds(y_of(r), YQ), :],
                    orb.at[:, c, half, :, y_at(r), :],
                    orb_sem.at[k],
                ).start()

    def loaded(k, window):
        pltpu.make_async_copy(window, window, orb_sem.at[k]).wait()

    load(0, (0,), 2)
    for r in range(NX4):
        load(2, (3,), r)
    load(1, (1, 2), 2)
    for k, r in ((3, 1), (4, 3), (5, 0)):
        load(k, (0, 1, 2), r)
    core_copy = pltpu.make_async_copy(
        core_hbm.at[rows_at(8 * h, 8), rows_at(YQ * bx + 16 * q, 16), :], core, core_sem
    )
    core_copy.start()

    with jax.named_scope("first_piece"):
        bands_copy.wait()
        first = bands_ref[0, 0]
        last = first + bands_ref[0, 1]
        weights = []
        for b in range(8):
            ident = band * 8 + b
            weights.append(jnp.where((ident >= first) & (ident < last), 0.5, 1.0).astype(F32))

    def density(c, r):
        acc = None
        for b in range(8):
            v = orb[b, c, :, :, r * YQ : (r + 1) * YQ, :].astype(F32)
            term = weights[b] * (v * v)
            acc = term if acc is None else acc + term
        part[r, c] = acc

    plus, minus = at_band(bx + 1, bz), at_band(bx + 3, bz)

    def x_send(stream, c, src):
        target = minus if stream % 2 else plus
        send(src, x_in.at[c, stream], xs_sem, xr_sem.at[c, int(stream > 1)], target)

    def far(c):
        x_send(0, c, part.at[2, c, 0])
        x_send(1, c, part.at[2, c, 1])

    def direct(c):
        x_send(2, c, part.at[1, c, 1])
        x_send(3, c, part.at[3, c, 0])

    def relay(c):
        arrived(x_in.at[c, 0:2], xr_sem.at[c, 0])
        for side, r in ((0, 1), (1, 3)):
            x_out[side, c] = part[r, c, side] + x_in[c, side]
            x_send(4 + side, c, x_out.at[side, c])

    def z_targets(ds, core):
        for d in ds:
            z = lax.rem(bz + d, NZ4)
            yield d, half_of(z), rows_at(16 * (z // 2), 16), at_band(bx, z, core)

    def finish(c):
        arrived(x_in.at[c, 2:6], xr_sem.at[c, 1])
        if c == 0:
            hear(3)
        summed[c, 0] = part[0, c, 0] + x_in[c, 4] + x_in[c, 3]
        summed[c, 1] = part[0, c, 1] + x_in[c, 5] + x_in[c, 2]
        for slot, half, ys, device in z_targets((2, 1, 3, 0), 1 - spin):
            send(summed.at[c, half, :, ys, :], z_in.at[slot, c], zs_sem, zr_sem, device)

    def z_first(ds):
        for slot, half, ys, device in z_targets(ds, spin):
            send(part.at[:, 3, half, :, ys, :], zf_in.at[slot - 1], fs_sem.at[0], fr_sem.at[0], device)

    def dmat_table():
        table = derivative_matrix()
        hi = table.astype(jnp.bfloat16)
        lo = (table - hi.astype(F32)).astype(jnp.bfloat16)
        dmat_ref[...] = jnp.concatenate([hi, hi, lo], 1)
        lane_ref[...] = jnp.concatenate([hi, lo, hi], 0)

    def tell(k):
        for peer in near:
            pl.semaphore_signal(hop_sem.at[k - 1], inc=1, device_id=peer, device_id_type=MESH)

    def hear(k):
        pl.semaphore_wait(hop_sem.at[k - 1], len(near))
        if k < HOPS:
            tell(k + 1)

    loaded(0, orb.at[:, 0, :, :, y_at(2), :])
    density(0, 2)
    with jax.named_scope("barrier"):
        pl.semaphore_wait(barrier, len(entry))
    with jax.named_scope("rs_head"):
        far(0)
        for peer in aside:
            pl.semaphore_signal(hop_sem.at[HOPS], inc=1, device_id=peer, device_id_type=MESH)
        tell(1)
        loaded(2, orb.at[:, 3])
        for r in range(NX4):
            density(3, r)
        z_first((1, 3))
        loaded(1, orb.at[:, 1:3, :, :, y_at(2), :])
        density(1, 2)
        far(1)
        density(2, 2)
        far(2)
        loaded(3, orb.at[:, 0:3, :, :, y_at(1), :])
        loaded(4, orb.at[:, 0:3, :, :, y_at(3), :])
        density(0, 1)
        density(0, 3)
        direct(0)
        for c, r in ((1, 1), (1, 3), (2, 1), (2, 3)):
            density(c, r)
    with jax.named_scope("hear_z"):
        pl.semaphore_wait(hop_sem.at[HOPS], 2)
        z_first((2,))
    with jax.named_scope("rs_rest"):
        hear(1)
        loaded(5, orb.at[:, 0:3, :, :, y_at(0), :])
        for c in range(CH):
            density(c, 0)
        dmat_table()
    for c in range(CH):
        with jax.named_scope(f"relay{c}"):
            relay(c)
        if c + 1 < CH:
            direct(c + 1)
    core_copy.wait()
    with jax.named_scope("hear2"):
        hear(2)
    for c in range(CH):
        with jax.named_scope(f"finish{c}"):
            finish(c)

    y_mine = rows_at(16 * q, 16)
    with jax.named_scope("zf_wait"):
        arrived(zf_in, fr_sem.at[0])
        zf_sum[...] = part[:, 3, h, :, y_mine, :] + zf_in[0] + zf_in[1] + zf_in[2]
        for r in (2, 1, 3, 0):
            send(
                zf_sum.at[r], xf_in.at[r], fs_sem.at[1], fr_sem.at[1],
                at_band(bx + r, bz, 1 - spin),
            )
    with jax.named_scope("hear4"):
        hear(4)
    with jax.named_scope("z_wait"):
        arrived(z_in, zr_sem)
    for c in range(CH):
        block = 0.5 * core[2 * c : 2 * c + 2] + z_in[0, c] + z_in[1, c] + z_in[2, c] + z_in[3, c]
        dens[32 * c : 32 * c + 32, :] = block.reshape(32, N)
    with jax.named_scope("hear5"):
        hear(5)
    with jax.named_scope("xf_wait"):
        arrived(xf_in, fr_sem.at[1])
    block = 0.5 * core[2 * CH : 2 * CH + 2] + xf_in[0] + xf_in[1] + xf_in[2] + xf_in[3]
    dens[32 * CH : 32 * CH + 32, :] = block.reshape(32, N)

    def halves(x):
        hi = x.astype(jnp.bfloat16)
        return hi, (x - hi.astype(F32)).astype(jnp.bfloat16)

    def along_rows(x):
        hi, lo = halves(x)
        return jnp.dot(dmat_ref[...], jnp.concatenate([hi, lo, hi], 0), preferred_element_type=F32)

    def along_lanes(x):
        hi, lo = halves(x)
        return jnp.dot(jnp.concatenate([hi, hi, lo], 1), lane_ref[...], preferred_element_type=F32)

    holder = 1 - spin

    def y_exchange(src, dst, k):
        for dx, dq in ((2, 1), (1, 1), (3, 1), (0, 1), (2, 0), (1, 0), (3, 0)):
            x, place = lax.rem(bx + dx, NX4), lax.rem(q + dq, 2)
            z = h + place * (3 - 2 * h)
            send(
                src.at[rows_at(16 * (2 * x + place), 16), :], dst.at[rows_at(16 * member, 16), :],
                ys_sem.at[k], yr_sem.at[k], (holder, x * NZ4 + z, grid),
            )
        mine = rows_at(16 * member, 16)
        send(src.at[mine, :], dst.at[mine, :], ys_sem.at[k], yr_sem.at[k], partner)

    def y_wait(dst, k):
        arrived(dst, yr_sem.at[k])

    def x_exchange(src, dst, k):
        for de in (1, 0):
            for dz in (1, 0):
                for dy in (2, 1, 3, 0):
                    if (de, dz, dy) == (0, 0, 0):
                        continue
                    e2 = lax.rem(e + de, 2)
                    g2 = lax.rem(gz + dz, 2) * GY + lax.rem(gy + dy, GY)
                    z = 2 * q + e2
                    there, here = 8 * e2 + g2, 2 * grid + h
                    if k == 1:
                        there, here = 2 * g2 + half_of(z), 8 * e + grid
                    send(
                        src.at[rows_at(8 * there, 8), :], dst.at[rows_at(8 * here, 8), :],
                        gs_sem.at[k], gr_sem.at[k], (holder, bx * NZ4 + z, g2),
                    )
        mine = (2 * grid + h, 8 * e + grid)
        there, here = mine if k == 1 else mine[::-1]
        there, here = rows_at(8 * there, 8), rows_at(8 * here, 8)
        send(src.at[there, :], dst.at[here, :], gs_sem.at[k], gr_sem.at[k], partner)

    def x_wait(dst, k):
        arrived(dst, gr_sem.at[k])

    def out_y():
        xr = 8 * h + member
        for dx in (2, 1, 3, 0):
            for dz in (2, 1, 3, 0):
                b2 = lax.rem(bx + dx, NX4) * NZ4 + lax.rem(bz + dz, NZ4)
                send(
                    y_res.at[1, rows_at(8 * b2, 8), :], y_fin.at[rows_at(8 * xr, 8), :],
                    ys_sem.at[3], yr_sem.at[3], (holder, b2, grid),
                )

    def out_x():
        for dz, dy in ((1, 2), (1, 1), (1, 3), (0, 2), (1, 0), (0, 1), (0, 3), (0, 0)):
            g2 = lax.rem(gz + dz, 2) * GY + lax.rem(gy + dy, GY)
            send(
                x_res.at[1, rows_at(XR * g2, XR), :], x_fin.at[rows_at(XR * grid, XR), :],
                gs_sem.at[3], gr_sem.at[3], (holder, band, g2),
            )

    def pencils(y_src, x_src, k):
        y_exchange(y_src, y_line.at[k], 2 * k)
        for t in range(16):
            turned[k, 8 * t : 8 * t + 8, :] = x_src[pl.ds(t, 8, stride=16), :]
        x_exchange(turned.at[k], x_line.at[k], 2 * k)

    with jax.named_scope("fwd0"):
        pencils(dens, dens, 0)
        send(dens, dens_o, ps_sem, pr_sem.at[0], partner)
        grad[2] = -along_lanes(dens[...])
        send(grad.at[2], grad_o.at[2], ps_sem, pr_sem.at[1], partner)
    with jax.named_scope("drain0"):
        sent(part.at[0:3, 0:CH], xs_sem)
        sent(z_in, zs_sem)
        sent(zf_in, fs_sem.at[0])
        sent(xf_in, fs_sem.at[1])
    with jax.named_scope("y_wait0"):
        y_wait(y_line.at[0], 0)
    with jax.named_scope("y_lines0"):
        y_res[0] = along_rows(y_line[0])
        y_exchange(y_res.at[0], y_back, 1)
    with jax.named_scope("x_wait0"):
        x_wait(x_line.at[0], 0)
    with jax.named_scope("x_lines0"):
        x_res[0] = along_rows(x_line[0])
        x_exchange(x_res.at[0], x_back, 1)
    with jax.named_scope("prepare"):
        arrived(dens_o, pr_sem.at[0])
        step = 16
        for i in range(0, N, step):
            rows = slice(i, i + step)
            for k, known in enumerate(xc_prepare(dens_o[rows, :], dens[rows, :])):
                prepared[k, rows, :] = known
    with jax.named_scope("y_back0"):
        y_wait(y_back, 1)
        send(y_back, grad_o.at[1], ps_sem, pr_sem.at[1], partner)
    with jax.named_scope("x_back0"):
        x_wait(x_back, 1)
        for i in range(8):
            grad[0, 16 * i : 16 * i + 16, :] = x_back[pl.ds(i, 16, stride=8), :]
    with jax.named_scope("swap"):
        send(grad.at[0], grad_o.at[0], ps_sem, pr_sem.at[1], partner)
        arrived(grad_o, pr_sem.at[1])

    with jax.named_scope("xc"):
        for i in range(0, N, step):
            rows = slice(i, i + step)
            o = (grad[0, rows, :], y_back[rows, :], grad[2, rows, :])
            g = (grad_o[0, rows, :], grad_o[1, rows, :], grad_o[2, rows, :])
            s_own = g[0] * g[0] + g[1] * g[1] + g[2] * g[2]
            s_mix = g[0] * o[0] + g[1] * o[1] + g[2] * o[2]
            s_other = o[0] * o[0] + o[1] * o[1] + o[2] * o[2]
            known = [prepared[k, rows, :] for k in range(PREPARED)]
            dn, ds, dm = xc_derivs(known, s_own, s_mix, s_other)
            for a in range(3):
                flux[a, rows, :] = 2.0 * ds * g[a] + dm * o[a]
            flux[3, rows, :] = dn

    with jax.named_scope("fwd1"):
        pencils(flux.at[1], flux.at[0], 1)
        base[...] = (flux[3] + along_lanes(flux[2])).reshape(8, 16, N)
        there = lax.rem(e + 1, 2)
        send(
            base.at[:, rows_at(8 * there, 8), :], final.at[h],
            bs_sem, br_sem, (spin, bx * NZ4 + 2 * q + there, grid),
        )
        final[h] = base[:, rows_at(8 * e, 8), :]
    with jax.named_scope("drain1"):
        for k in (0, 1):
            sent(y_line.at[k], ys_sem.at[k])
            sent(x_line.at[k], gs_sem.at[k])
        sent(grad_o, ps_sem)
        sent(dens_o, ps_sem)
    with jax.named_scope("y_wait1"):
        y_wait(y_line.at[1], 2)
    with jax.named_scope("y_lines1"):
        y_res[1] = along_rows(y_line[1])
        out_y()
    with jax.named_scope("x_wait1"):
        x_wait(x_line.at[1], 2)
    with jax.named_scope("x_lines1"):
        x_res[1] = along_rows(x_line[1])
        out_x()
    with jax.named_scope("drain2"):
        for k in (2, 3):
            sent(y_line.at[0], ys_sem.at[k])
            sent(x_line.at[0], gs_sem.at[k])
        sent(final.at[0], bs_sem)
        arrived(final.at[0], br_sem)
    with jax.named_scope("x_back1"):
        arrived(x_fin, gr_sem.at[3])
        for i in range(XR):
            out_ref[0, i] = final[i // 8, i % 8] - x_fin[pl.ds(i, YB, stride=XR), :]
    with jax.named_scope("y_back1"):
        arrived(y_fin, yr_sem.at[3])
    with jax.named_scope("tail"):
        out_ref[0] = out_ref[0] - y_fin[...].reshape(XR, YB, N)


def per_device(orbitals, partial_bands, core_density):
    vm = pltpu.VMEM
    sem = pltpu.SemaphoreType.DMA
    anyspace = pl.BlockSpec(memory_space=pltpu.HBM)
    return pl.pallas_call(
        kernel,
        out_shape=jax.ShapeDtypeStruct((1, XR, YB, N), F32),
        in_specs=[anyspace] * 3,
        out_specs=pl.BlockSpec(memory_space=pltpu.VMEM),
        scratch_shapes=[
            vm((8, CH + 1, 2, 2, N, N), jnp.bfloat16),
            vm((N, 3 * N), jnp.bfloat16),
            vm((3 * N, N), jnp.bfloat16),
            pltpu.SMEM((1, 2), jnp.int32),
            vm((NX4, CH + 1, 2, 2, YQ, N), F32),
            vm((8, 16, N), F32),
            vm((CH, 6, 2, YQ, N), F32),
            vm((2, CH, 2, YQ, N), F32),
            vm((CH, 2, 2, YQ, N), F32),
            vm((NZ4, CH, 2, 16, N), F32),
            vm((NZ4 - 1, NX4, 2, 16, N), F32),
            vm((NX4, 2, 16, N), F32),
            vm((NX4, 2, 16, N), F32),
            vm((N, N), F32),
            vm((N, N), F32),
            vm((PREPARED, N, N), F32),
            vm((3, N, N), F32),
            vm((3, N, N), F32),
            vm((4, N, N), F32),
            vm((2, N, N), F32),
            vm((2, N, N), F32),
            vm((2, N, N), F32),
            vm((N, N), F32),
            vm((2, N, N), F32),
            vm((2, N, N), F32),
            vm((N, N), F32),
            vm((8, 16, N), F32),
            vm((2, 8, YB, N), F32),
            vm((N, N), F32),
            vm((N, N), F32),
            sem((6,)),
            sem,
            sem,
            pltpu.SemaphoreType.REGULAR((HOPS + 1,)),
            sem,
            sem((CH, 2)),
            sem,
            sem,
            sem((2,)),
            sem((2,)),
            sem,
            sem((2,)),
            sem((4,)),
            sem((4,)),
            sem((4,)),
            sem((4,)),
            sem,
            sem,
        ],
        compiler_params=pltpu.CompilerParams(
            collective_id=0, has_side_effects=True, vmem_limit_bytes=54400 * 1024
        ),
    )(*[pltpu.with_memory_space_constraint(a, pltpu.HBM) for a in (orbitals, partial_bands, core_density)])


def solution(mesh):
    in_specs = (P("spin", "band", "grid", None, None), P("spin", None), P("grid", None, None))
    out_specs = P("spin", "grid", "band", None)

    return jax.shard_map(
        per_device, mesh=mesh, in_specs=in_specs, out_specs=out_specs, check_vma=False
    )
```

```python
import math

import jax
import jax.numpy as jnp
from jax import lax
from jax.experimental import pallas as pl
from jax.experimental.pallas import tpu as pltpu
from jax.sharding import PartitionSpec as P

KAPPA = 0.804
MU_X = 0.2195149727645171
BETA = 0.06672455060314922
GAMMA = (1.0 - math.log(2.0)) / math.pi**2
FZ_NORM = 2.0 ** (4.0 / 3.0) - 2.0
FPP_ZERO = 1.709921

MESH = pl.DeviceIdType.MESH
F32 = jnp.float32
N = 128
XR = 16
NX4 = 4
NZ4 = 4
GY = 4
GRID = 2 * GY
BAND = NX4 * NZ4
YB = N // BAND
YQ = N // NX4
CH = 3
HOPS = 5


def derivative_matrix():
    k = lax.broadcasted_iota(jnp.int32, (N, N), 0) - lax.broadcasted_iota(jnp.int32, (N, N), 1)
    far = jnp.abs(k)
    near = jnp.minimum(far, N - far)
    angle = (math.pi / N) * jnp.maximum(near, 1).astype(F32)
    size = (math.pi / N) * jnp.cos(angle) / jnp.sin(angle)
    flips = (k < 0).astype(jnp.int32) + (far > N // 2).astype(jnp.int32) + (far & 1)
    signed = jnp.where((flips & 1) == 1, -size, size)
    return jnp.where(k == 0, 0.0, signed)


def pw_fit(r, root, amp, alpha, b1, b2, b3, b4):
    denom = (2.0 * amp) * (root * (b1 + root * (b2 + root * (b3 + root * b4))))
    slope = (2.0 * amp) * (0.5 * b1 / root + (b2 + root * (1.5 * b3 + root * (2.0 * b4))))
    log = jnp.log(1.0 + 1.0 / denom)
    front = (-2.0 * amp) * (1.0 + alpha * r)
    value = front * log
    deriv = (-2.0 * amp * alpha) * log - front * slope / (denom * (denom + 1.0))
    return value, deriv


def cbrt(x):
    return jnp.exp(jnp.log(x) * (1.0 / 3.0))


def xc_prepare(own, other):
    total = own + other
    inv_n = 1.0 / total
    c_own = cbrt(own)
    c_other = cbrt(other)
    c_tot = cbrt(total)
    inv_c = 1.0 / c_tot
    double = 2.0 * own
    kf = (6.0 * math.pi**2) ** (1.0 / 3.0) * c_own
    inv_kn = 1.0 / (kf * double)
    two13 = 2.0 ** (1.0 / 3.0)
    plus = double * inv_n
    minus = 2.0 * other * inv_n
    zeta = (own - other) * inv_n
    plus13 = two13 * c_own * inv_c
    minus13 = two13 * c_other * inv_c
    radius = (3.0 / (4.0 * math.pi)) ** (1.0 / 3.0) * inv_c
    root = jnp.sqrt(radius)
    ec0, ec0_r = pw_fit(radius, root, 0.031091, 0.2137, 7.5957, 3.5876, 1.6382, 0.49294)
    ec1, ec1_r = pw_fit(radius, root, 0.015545, 0.20548, 14.1189, 6.1977, 3.3662, 0.62517)
    ac, ac_r = pw_fit(radius, root, 0.016887, 0.11125, 10.357, 3.6231, 0.88026, 0.49671)
    fz = (plus * plus13 + minus * minus13 - 2.0) * (1.0 / FZ_NORM)
    fz_d = (4.0 / 3.0 / FZ_NORM) * (plus13 - minus13)
    z2 = zeta * zeta
    z3 = z2 * zeta
    z4 = z2 * z2
    w1 = (-1.0 / FPP_ZERO) * (1.0 - z4)
    diff = ec1 - ec0
    mix = ac * w1 + diff * z4
    ec = ec0 + fz * mix
    ec_r = ec0_r + fz * (ac_r * w1 + (ec1_r - ec0_r) * z4)
    ec_z = fz_d * mix + 4.0 * z3 * fz * (ac * (1.0 / FPP_ZERO) + diff)
    phi = 0.5 * (plus13 * plus13 + minus13 * minus13)
    phi_d = (1.0 / 3.0) * (1.0 / plus13 - 1.0 / minus13)
    inv_phi = 1.0 / phi
    gp3 = GAMMA * phi * phi * phi
    kf_tot = (3.0 * math.pi**2) ** (1.0 / 3.0)
    tfac = (math.pi / (16.0 * kf_tot)) * inv_phi * inv_phi * inv_c * inv_n * inv_n
    inv_gp3 = (1.0 / GAMMA) * inv_phi * inv_phi * inv_phi
    ex = jnp.exp(-ec * inv_gp3)
    amp = (BETA / GAMMA) / (ex - 1.0)
    amp_ec = amp * amp * ex * (GAMMA / BETA) * inv_gp3
    drift = (1.0 / 3.0) * radius * ec_r
    return kf, inv_kn, ec, drift, ec_z, minus, gp3, tfac, amp, amp_ec, phi_d * inv_phi, total


PREPARED = 12


def xc_derivs(prepared, s_own, s_mix, s_other):
    kf, inv_kn, ec, drift, ec_z, minus, gp3, tfac, amp, amp_ec, phi_r, total = prepared
    s2 = s_own * inv_kn * inv_kn
    inv_den = 1.0 / (1.0 + (MU_X / KAPPA) * s2)
    enh = (1.0 + KAPPA) - KAPPA * inv_den
    enh_d = MU_X * inv_den * inv_den
    dn_x = (-1.0 / math.pi) * kf * (enh - 2.0 * s2 * enh_d)
    ds_x = (-3.0 / (8.0 * math.pi)) * enh_d * inv_kn
    sigma = s_own + 2.0 * s_mix + s_other
    t2 = sigma * tfac
    y = amp * t2
    den = 1.0 + y + y * y
    inv_d = 1.0 / den
    ct = (BETA / GAMMA) * t2
    q = ct * (1.0 + y) * inv_d
    grad_h = gp3 * jnp.log(1.0 + q)
    scale = gp3 / (1.0 + q) * inv_d * inv_d
    h_t = scale * ((BETA / GAMMA) * (1.0 + 2.0 * y))
    h_a = -scale * (ct * t2) * (y * (2.0 + y))
    h_ec = h_a * amp_ec
    one_ec = 1.0 + h_ec
    e_n = ec + grad_h - drift * one_ec - (7.0 / 3.0) * t2 * h_t
    e_z = ec_z * one_ec + phi_r * (3.0 * (grad_h - ec * h_ec) - 2.0 * t2 * h_t)
    dn = dn_x + e_n + e_z * minus
    ds_c = total * h_t * tfac
    return dn, ds_x + ds_c, 2.0 * ds_c


def kernel(
    orb_hbm, bands_hbm, core_hbm, out_ref,
    orb, dmat_ref, lane_ref, bands_ref, part, core, x_in, x_out, summed, z_in, zf_in, zf_sum, xf_in,
    dens, dens_o, prepared, grad, grad_o, flux, turned, x_line, x_line_n, x_res, x_res_n, x_back, y_line, y_line_n, y_res, y_res_n, y_back, base, final, x_fin, y_fin,
    orb_sem, core_sem, bands_sem, hop_sem, xs_sem, xr_sem, zs_sem, zr_sem, fs_sem, fr_sem,
    ps_sem, pr_sem, ys_sem, yr_sem, gs_sem, gr_sem, bs_sem, br_sem,
):
    spin = lax.axis_index("spin")
    band = lax.axis_index("band")
    grid = lax.axis_index("grid")
    bx, bz = band // NZ4, lax.rem(band, NZ4)
    gz, gy = grid // GY, lax.rem(grid, GY)

    def half_of(z):
        q = z // 2
        return 3 * q + z * (1 - 2 * q)

    q, h, e = bz // 2, half_of(bz), lax.rem(bz, 2)
    member = 2 * bx + q
    partner = (1 - spin, band, grid)

    def at_band(x, z, core=spin):
        return (core, lax.rem(x, NX4) * NZ4 + lax.rem(z, NZ4), grid)

    def copy(src, dst, send_sem, recv_sem, device):
        return pltpu.make_async_remote_copy(
            src_ref=src, dst_ref=dst, send_sem=send_sem, recv_sem=recv_sem,
            device_id=device, device_id_type=MESH,
        )

    def send(*args):
        copy(*args).start()

    def sent(like, send_sem):
        copy(like, like, send_sem, send_sem, (spin, band, grid)).wait_send()

    def arrived(like, recv_sem):
        copy(like, like, recv_sem, recv_sem, (spin, band, grid)).wait_recv()

    def rows_at(start, count):
        return pl.ds(pl.multiple_of(start, 8), count)

    bands_copy = pltpu.make_async_copy(bands_hbm, bands_ref, bands_sem)
    bands_copy.start()
    z_all = 2 * bz + gz
    near = [at_band(bx + 1, bz), at_band(bx + 3, bz)]
    near += [(spin, band, gz * GY + lax.rem(gy + d, GY)) for d in (1, 3)]
    for d in (1, 7):
        z = lax.rem(z_all + d, 8)
        near += [(spin, bx * NZ4 + z // 2, lax.rem(z, 2) * GY + gy)]
    barrier = pltpu.get_barrier_semaphore()
    across = [(1 - spin, *peer[1:]) for peer in near]
    aside = [at_band(bx, bz + d) for d in (1, 3)]
    entry = (*near, *across, partner, *aside)
    for peer in entry:
        pl.semaphore_signal(barrier, inc=1, device_id=peer, device_id_type=MESH)

    def y_of(r):
        return pl.multiple_of(lax.rem(bx + r, NX4) * YQ, YQ)

    def y_at(r):
        return pl.ds(r * YQ, YQ)

    def load(k, cs, r):
        for c in cs:
            for half in range(2):
                pltpu.make_async_copy(
                    orb_hbm.at[0, :, pl.ds(8 * half + 2 * c, 2), pl.ds(y_of(r), YQ), :],
                    orb.at[:, c, half, :, y_at(r), :],
                    orb_sem.at[k],
                ).start()

    def loaded(k, window):
        pltpu.make_async_copy(window, window, orb_sem.at[k]).wait()

    load(0, (0,), 2)
    for r in range(NX4):
        load(2, (3,), r)
    load(1, (1, 2), 2)
    for k, r in ((3, 1), (4, 3), (5, 0)):
        load(k, (0, 1, 2), r)
    core_copy = pltpu.make_async_copy(
        core_hbm.at[rows_at(8 * h, 8), rows_at(YQ * bx + 16 * q, 16), :], core, core_sem
    )
    core_copy.start()

    with jax.named_scope("first_piece"):
        bands_copy.wait()
        first = bands_ref[0, 0]
        last = first + bands_ref[0, 1]
        weights = []
        for b in range(8):
            ident = band * 8 + b
            weights.append(jnp.where((ident >= first) & (ident < last), 0.5, 1.0).astype(F32))

    def density(c, r):
        acc = None
        for b in range(8):
            v = orb[b, c, :, :, r * YQ : (r + 1) * YQ, :].astype(F32)
            term = weights[b] * (v * v)
            acc = term if acc is None else acc + term
        part[r, c] = acc

    plus, minus = at_band(bx + 1, bz), at_band(bx + 3, bz)

    def x_send(stream, c, src):
        target = minus if stream % 2 else plus
        send(src, x_in.at[c, stream], xs_sem, xr_sem.at[c, int(stream > 1)], target)

    def far(c):
        x_send(0, c, part.at[2, c, 0])
        x_send(1, c, part.at[2, c, 1])

    def direct(c):
        x_send(2, c, part.at[1, c, 1])
        x_send(3, c, part.at[3, c, 0])

    def relay(c):
        arrived(x_in.at[c, 0:2], xr_sem.at[c, 0])
        for side, r in ((0, 1), (1, 3)):
            x_out[side, c] = part[r, c, side] + x_in[c, side]
            x_send(4 + side, c, x_out.at[side, c])

    def z_targets(ds, core):
        for d in ds:
            z = lax.rem(bz + d, NZ4)
            yield d, half_of(z), rows_at(16 * (z // 2), 16), at_band(bx, z, core)

    def finish(c):
        arrived(x_in.at[c, 2:6], xr_sem.at[c, 1])
        if c == 0:
            hear(3)
        summed[c, 0] = part[0, c, 0] + x_in[c, 4] + x_in[c, 3]
        summed[c, 1] = part[0, c, 1] + x_in[c, 5] + x_in[c, 2]
        for slot, half, ys, device in z_targets((2, 1, 3, 0), 1 - spin):
            send(summed.at[c, half, :, ys, :], z_in.at[slot, c], zs_sem, zr_sem, device)

    def z_first(ds):
        for slot, half, ys, device in z_targets(ds, spin):
            send(part.at[:, 3, half, :, ys, :], zf_in.at[slot - 1], fs_sem.at[0], fr_sem.at[0], device)

    def dmat_table():
        table = derivative_matrix()
        hi = table.astype(jnp.bfloat16)
        lo = (table - hi.astype(F32)).astype(jnp.bfloat16)
        dmat_ref[...] = jnp.concatenate([hi, hi, lo], 1)
        lane_ref[...] = jnp.concatenate([hi, lo, hi], 0)

    def tell(k):
        for peer in near:
            pl.semaphore_signal(hop_sem.at[k - 1], inc=1, device_id=peer, device_id_type=MESH)

    def hear(k):
        pl.semaphore_wait(hop_sem.at[k - 1], len(near))
        if k < HOPS:
            tell(k + 1)

    loaded(0, orb.at[:, 0, :, :, y_at(2), :])
    density(0, 2)
    with jax.named_scope("barrier"):
        pl.semaphore_wait(barrier, len(entry))
    with jax.named_scope("rs_head"):
        far(0)
        for peer in aside:
            pl.semaphore_signal(hop_sem.at[HOPS], inc=1, device_id=peer, device_id_type=MESH)
        tell(1)
        loaded(2, orb.at[:, 3])
        for r in range(NX4):
            density(3, r)
        z_first((1, 3))
        loaded(1, orb.at[:, 1:3, :, :, y_at(2), :])
        density(1, 2)
        far(1)
        density(2, 2)
        far(2)
        loaded(3, orb.at[:, 0:3, :, :, y_at(1), :])
        loaded(4, orb.at[:, 0:3, :, :, y_at(3), :])
        density(0, 1)
        density(0, 3)
        direct(0)
        for c, r in ((1, 1), (1, 3), (2, 1), (2, 3)):
            density(c, r)
    with jax.named_scope("hear_z"):
        pl.semaphore_wait(hop_sem.at[HOPS], 2)
        z_first((2,))
    with jax.named_scope("rs_rest"):
        hear(1)
        loaded(5, orb.at[:, 0:3, :, :, y_at(0), :])
        for c in range(CH):
            density(c, 0)
        dmat_table()
    for c in range(CH):
        with jax.named_scope(f"relay{c}"):
            relay(c)
        if c + 1 < CH:
            direct(c + 1)
    core_copy.wait()
    with jax.named_scope("hear2"):
        hear(2)
    for c in range(CH):
        with jax.named_scope(f"finish{c}"):
            finish(c)

    y_mine = rows_at(16 * q, 16)
    with jax.named_scope("zf_wait"):
        arrived(zf_in, fr_sem.at[0])
        zf_sum[...] = part[:, 3, h, :, y_mine, :] + zf_in[0] + zf_in[1] + zf_in[2]
        for r in (2, 1, 3, 0):
            send(
                zf_sum.at[r], xf_in.at[r], fs_sem.at[1], fr_sem.at[1],
                at_band(bx + r, bz, 1 - spin),
            )
    with jax.named_scope("hear4"):
        hear(4)
    with jax.named_scope("z_wait"):
        arrived(z_in, zr_sem)
    for c in range(CH):
        block = 0.5 * core[2 * c : 2 * c + 2] + z_in[0, c] + z_in[1, c] + z_in[2, c] + z_in[3, c]
        dens[32 * c : 32 * c + 32, :] = block.reshape(32, N)
    with jax.named_scope("hear5"):
        hear(5)
    with jax.named_scope("xf_wait"):
        arrived(xf_in, fr_sem.at[1])
    block = 0.5 * core[2 * CH : 2 * CH + 2] + xf_in[0] + xf_in[1] + xf_in[2] + xf_in[3]
    dens[32 * CH : 32 * CH + 32, :] = block.reshape(32, N)

    def halves(x):
        hi = x.astype(jnp.bfloat16)
        return hi, (x - hi.astype(F32)).astype(jnp.bfloat16)

    def along_rows(x):
        hi, lo = halves(x)
        return jnp.dot(dmat_ref[...], jnp.concatenate([hi, lo, hi], 0), preferred_element_type=F32)

    def along_lanes(x):
        hi, lo = halves(x)
        return jnp.dot(jnp.concatenate([hi, hi, lo], 1), lane_ref[...], preferred_element_type=F32)

    holder = 1 - spin

    def pass_on(src, dst, send_sem, recv_sem, local):
        if local:
            dst[...] = src[...]
        else:
            send(src, dst, send_sem, recv_sem, partner)

    def y_exchange(src, dst, ks, kr, core, local=False):
        for dx, dq in ((2, 1), (1, 1), (3, 1), (0, 1), (2, 0), (1, 0), (3, 0)):
            x, place = lax.rem(bx + dx, NX4), lax.rem(q + dq, 2)
            z = h + place * (3 - 2 * h)
            send(
                src.at[rows_at(16 * (2 * x + place), 16), :], dst.at[rows_at(16 * member, 16), :],
                ys_sem.at[ks], yr_sem.at[kr], (core, x * NZ4 + z, grid),
            )
        mine = rows_at(16 * member, 16)
        pass_on(src.at[mine, :], dst.at[mine, :], ys_sem.at[ks], yr_sem.at[kr], local)

    def x_exchange(src, dst, ks, kr, core, local=False, back=False):
        for de in (1, 0):
            for dz in (1, 0):
                for dy in (2, 1, 3, 0):
                    if (de, dz, dy) == (0, 0, 0):
                        continue
                    e2 = lax.rem(e + de, 2)
                    g2 = lax.rem(gz + dz, 2) * GY + lax.rem(gy + dy, GY)
                    z = 2 * q + e2
                    there, here = 8 * e2 + g2, 2 * grid + h
                    if back:
                        there, here = 2 * g2 + half_of(z), 8 * e + grid
                    send(
                        src.at[rows_at(8 * there, 8), :], dst.at[rows_at(8 * here, 8), :],
                        gs_sem.at[ks], gr_sem.at[kr], (core, bx * NZ4 + z, g2),
                    )
        mine = (2 * grid + h, 8 * e + grid)
        there, here = mine if back else mine[::-1]
        there, here = rows_at(8 * there, 8), rows_at(8 * here, 8)
        pass_on(src.at[there, :], dst.at[here, :], gs_sem.at[ks], gr_sem.at[kr], local)

    def y_wait(dst, k, local=False):
        arrived(dst.at[0 : N - 16, :] if local else dst, yr_sem.at[k])

    def x_wait(dst, k, local=False):
        arrived(dst.at[0 : N - 8, :] if local else dst, gr_sem.at[k])

    def out_y():
        xr = 8 * h + member
        for dx in (2, 1, 3, 0):
            for dz in (2, 1, 3, 0):
                b2 = lax.rem(bx + dx, NX4) * NZ4 + lax.rem(bz + dz, NZ4)
                send(
                    y_res.at[1, rows_at(8 * b2, 8), :], y_fin.at[rows_at(8 * xr, 8), :],
                    ys_sem.at[3], yr_sem.at[3], (holder, b2, grid),
                )

    def out_x():
        for dz, dy in ((1, 2), (1, 1), (1, 3), (0, 2), (1, 0), (0, 1), (0, 3), (0, 0)):
            g2 = lax.rem(gz + dz, 2) * GY + lax.rem(gy + dy, GY)
            send(
                x_res.at[1, rows_at(XR * g2, XR), :], x_fin.at[rows_at(XR * grid, XR), :],
                gs_sem.at[3], gr_sem.at[3], (holder, band, g2),
            )

    def turn(src, dst):
        for t in range(16):
            dst[8 * t : 8 * t + 8, :] = src[pl.ds(t, 8, stride=16), :]

    with jax.named_scope("fwd0"):

        @pl.when(spin == 0)
        def _():
            y_exchange(dens, y_line.at[0], 0, 0, 1)
            turn(dens, turned.at[0])
            x_exchange(turned.at[0], x_line.at[0], 0, 0, 1)

        @pl.when(spin == 1)
        def _():
            y_exchange(dens, y_line_n, 4, 4, 1, local=True)
            turn(dens, turned.at[0])
            x_exchange(turned.at[0], x_line_n, 4, 4, 1, local=True)

        send(dens, dens_o, ps_sem, pr_sem.at[0], partner)
        grad[2] = -along_lanes(dens[...])
        send(grad.at[2], grad_o.at[2], ps_sem, pr_sem.at[1], partner)
    with jax.named_scope("drain0"):
        sent(part.at[0:3, 0:CH], xs_sem)
        sent(z_in, zs_sem)
        sent(zf_in, fs_sem.at[0])
        sent(xf_in, fs_sem.at[1])
    with jax.named_scope("prepare"):
        arrived(dens_o, pr_sem.at[0])
        step = 16
        for i in range(0, N, step):
            rows = slice(i, i + step)
            for k, known in enumerate(xc_prepare(dens_o[rows, :], dens[rows, :])):
                prepared[k, rows, :] = known
    with jax.named_scope("lines0"):

        @pl.when(spin == 1)
        def _():
            y_wait(y_line.at[0], 0)
            y_res[0] = along_rows(y_line[0])
            y_exchange(y_res.at[0], y_back, 1, 1, 0)
            x_wait(x_line.at[0], 0)
            x_res[0] = along_rows(x_line[0])
            x_exchange(x_res.at[0], x_back, 1, 1, 0, back=True)
            y_wait(y_line_n, 4, local=True)
            y_res_n[...] = along_rows(y_line_n[...])
            y_exchange(y_res_n, y_back, 1, 1, 1, local=True)
            x_wait(x_line_n, 4, local=True)
            x_res_n[...] = along_rows(x_line_n[...])
            x_exchange(x_res_n, x_back, 1, 1, 1, local=True, back=True)

    with jax.named_scope("y_back0"):
        pl.when(spin == 0)(lambda: y_wait(y_back, 1))
        pl.when(spin == 1)(lambda: y_wait(y_back, 1, local=True))
        send(y_back, grad_o.at[1], ps_sem, pr_sem.at[1], partner)
    with jax.named_scope("x_back0"):
        pl.when(spin == 0)(lambda: x_wait(x_back, 1))
        pl.when(spin == 1)(lambda: x_wait(x_back, 1, local=True))
        for i in range(8):
            grad[0, 16 * i : 16 * i + 16, :] = x_back[pl.ds(i, 16, stride=8), :]
    with jax.named_scope("swap"):
        send(grad.at[0], grad_o.at[0], ps_sem, pr_sem.at[1], partner)
        arrived(grad_o, pr_sem.at[1])

    with jax.named_scope("xc"):
        for i in range(0, N, step):
            rows = slice(i, i + step)
            o = (grad[0, rows, :], y_back[rows, :], grad[2, rows, :])
            g = (grad_o[0, rows, :], grad_o[1, rows, :], grad_o[2, rows, :])
            s_own = g[0] * g[0] + g[1] * g[1] + g[2] * g[2]
            s_mix = g[0] * o[0] + g[1] * o[1] + g[2] * o[2]
            s_other = o[0] * o[0] + o[1] * o[1] + o[2] * o[2]
            known = [prepared[k, rows, :] for k in range(PREPARED)]
            dn, ds, dm = xc_derivs(known, s_own, s_mix, s_other)
            for a in range(3):
                flux[a, rows, :] = 2.0 * ds * g[a] + dm * o[a]
            flux[3, rows, :] = dn

    with jax.named_scope("fwd1"):
        y_exchange(flux.at[1], y_line.at[1], 2, 2, holder)
        turn(flux.at[0], turned.at[1])
        x_exchange(turned.at[1], x_line.at[1], 2, 2, holder)
        base[...] = (flux[3] + along_lanes(flux[2])).reshape(8, 16, N)
        there = lax.rem(e + 1, 2)
        send(
            base.at[:, rows_at(8 * there, 8), :], final.at[h],
            bs_sem, br_sem, (spin, bx * NZ4 + 2 * q + there, grid),
        )
        final[h] = base[:, rows_at(8 * e, 8), :]
    with jax.named_scope("drain1"):

        @pl.when(spin == 0)
        def _():
            sent(y_line.at[0], ys_sem.at[0])
            sent(x_line.at[0], gs_sem.at[0])

        @pl.when(spin == 1)
        def _():
            for k in (1, 4):
                sent(y_line.at[0, 0 : N - 16, :], ys_sem.at[k])
                sent(x_line.at[0, 0 : N - 8, :], gs_sem.at[k])
            sent(y_line.at[0], ys_sem.at[1])
            sent(x_line.at[0], gs_sem.at[1])

        sent(grad_o, ps_sem)
        sent(dens_o, ps_sem)
    with jax.named_scope("y_wait1"):
        y_wait(y_line.at[1], 2)
    with jax.named_scope("y_lines1"):
        y_res[1] = along_rows(y_line[1])
        out_y()
    with jax.named_scope("x_wait1"):
        x_wait(x_line.at[1], 2)
    with jax.named_scope("x_lines1"):
        x_res[1] = along_rows(x_line[1])
        out_x()
    with jax.named_scope("drain2"):
        for k in (2, 3):
            sent(y_line.at[0], ys_sem.at[k])
            sent(x_line.at[0], gs_sem.at[k])
        sent(final.at[0], bs_sem)
        arrived(final.at[0], br_sem)
    with jax.named_scope("x_back1"):
        arrived(x_fin, gr_sem.at[3])
        for i in range(XR):
            out_ref[0, i] = final[i // 8, i % 8] - x_fin[pl.ds(i, YB, stride=XR), :]
    with jax.named_scope("y_back1"):
        arrived(y_fin, yr_sem.at[3])
    with jax.named_scope("tail"):
        out_ref[0] = out_ref[0] - y_fin[...].reshape(XR, YB, N)


def per_device(orbitals, partial_bands, core_density):
    vm = pltpu.VMEM
    sem = pltpu.SemaphoreType.DMA
    anyspace = pl.BlockSpec(memory_space=pltpu.HBM)
    return pl.pallas_call(
        kernel,
        out_shape=jax.ShapeDtypeStruct((1, XR, YB, N), F32),
        in_specs=[anyspace] * 3,
        out_specs=pl.BlockSpec(memory_space=pltpu.VMEM),
        scratch_shapes=[
            vm((8, CH + 1, 2, 2, N, N), jnp.bfloat16),
            vm((N, 3 * N), jnp.bfloat16),
            vm((3 * N, N), jnp.bfloat16),
            pltpu.SMEM((1, 2), jnp.int32),
            vm((NX4, CH + 1, 2, 2, YQ, N), F32),
            vm((8, 16, N), F32),
            vm((CH, 6, 2, YQ, N), F32),
            vm((2, CH, 2, YQ, N), F32),
            vm((CH, 2, 2, YQ, N), F32),
            vm((NZ4, CH, 2, 16, N), F32),
            vm((NZ4 - 1, NX4, 2, 16, N), F32),
            vm((NX4, 2, 16, N), F32),
            vm((NX4, 2, 16, N), F32),
            vm((N, N), F32),
            vm((N, N), F32),
            vm((PREPARED, N, N), F32),
            vm((3, N, N), F32),
            vm((3, N, N), F32),
            vm((4, N, N), F32),
            vm((2, N, N), F32),
            vm((2, N, N), F32),
            vm((N, N), F32),
            vm((2, N, N), F32),
            vm((N, N), F32),
            vm((N, N), F32),
            vm((2, N, N), F32),
            vm((N, N), F32),
            vm((2, N, N), F32),
            vm((N, N), F32),
            vm((N, N), F32),
            vm((8, 16, N), F32),
            vm((2, 8, YB, N), F32),
            vm((N, N), F32),
            vm((N, N), F32),
            sem((6,)),
            sem,
            sem,
            pltpu.SemaphoreType.REGULAR((HOPS + 1,)),
            sem,
            sem((CH, 2)),
            sem,
            sem,
            sem((2,)),
            sem((2,)),
            sem,
            sem((2,)),
            sem((5,)),
            sem((5,)),
            sem((5,)),
            sem((5,)),
            sem,
            sem,
        ],
        compiler_params=pltpu.CompilerParams(
            collective_id=0, has_side_effects=True, vmem_limit_bytes=54400 * 1024
        ),
    )(*[pltpu.with_memory_space_constraint(a, pltpu.HBM) for a in (orbitals, partial_bands, core_density)])


def solution(mesh):
    in_specs = (P("spin", "band", "grid", None, None), P("spin", None), P("grid", None, None))
    out_specs = P("spin", "grid", "band", None)

    return jax.shard_map(
        per_device, mesh=mesh, in_specs=in_specs, out_specs=out_specs, check_vma=False
    )
```

```python
import math

import jax
import jax.numpy as jnp
from jax import lax
from jax.experimental import pallas as pl
from jax.experimental.pallas import tpu as pltpu
from jax.sharding import PartitionSpec as P

KAPPA = 0.804
MU_X = 0.2195149727645171
BETA = 0.06672455060314922
GAMMA = (1.0 - math.log(2.0)) / math.pi**2
FZ_NORM = 2.0 ** (4.0 / 3.0) - 2.0
FPP_ZERO = 1.709921

MESH = pl.DeviceIdType.MESH
F32 = jnp.float32
N = 128
XR = 16
NX4 = 4
NZ4 = 4
GY = 4
GRID = 2 * GY
BAND = NX4 * NZ4
YB = N // BAND
YQ = N // NX4
CH = 3
HOPS = 5


def derivative_matrix():
    k = lax.broadcasted_iota(jnp.int32, (N, N), 0) - lax.broadcasted_iota(jnp.int32, (N, N), 1)
    far = jnp.abs(k)
    near = jnp.minimum(far, N - far)
    angle = (math.pi / N) * jnp.maximum(near, 1).astype(F32)
    size = (math.pi / N) * jnp.cos(angle) / jnp.sin(angle)
    flips = (k < 0).astype(jnp.int32) + (far > N // 2).astype(jnp.int32) + (far & 1)
    signed = jnp.where((flips & 1) == 1, -size, size)
    return jnp.where(k == 0, 0.0, signed)


def pw_fit(r, root, amp, alpha, b1, b2, b3, b4):
    denom = (2.0 * amp) * (root * (b1 + root * (b2 + root * (b3 + root * b4))))
    slope = (2.0 * amp) * (0.5 * b1 / root + (b2 + root * (1.5 * b3 + root * (2.0 * b4))))
    log = jnp.log(1.0 + 1.0 / denom)
    front = (-2.0 * amp) * (1.0 + alpha * r)
    value = front * log
    deriv = (-2.0 * amp * alpha) * log - front * slope / (denom * (denom + 1.0))
    return value, deriv


def cbrt(x):
    return jnp.exp(jnp.log(x) * (1.0 / 3.0))


def xc_prepare(own, other):
    total = own + other
    inv_n = 1.0 / total
    c_own = cbrt(own)
    c_other = cbrt(other)
    c_tot = cbrt(total)
    inv_c = 1.0 / c_tot
    double = 2.0 * own
    kf = (6.0 * math.pi**2) ** (1.0 / 3.0) * c_own
    inv_kn = 1.0 / (kf * double)
    two13 = 2.0 ** (1.0 / 3.0)
    plus = double * inv_n
    minus = 2.0 * other * inv_n
    zeta = (own - other) * inv_n
    plus13 = two13 * c_own * inv_c
    minus13 = two13 * c_other * inv_c
    radius = (3.0 / (4.0 * math.pi)) ** (1.0 / 3.0) * inv_c
    root = jnp.sqrt(radius)
    ec0, ec0_r = pw_fit(radius, root, 0.031091, 0.2137, 7.5957, 3.5876, 1.6382, 0.49294)
    ec1, ec1_r = pw_fit(radius, root, 0.015545, 0.20548, 14.1189, 6.1977, 3.3662, 0.62517)
    ac, ac_r = pw_fit(radius, root, 0.016887, 0.11125, 10.357, 3.6231, 0.88026, 0.49671)
    fz = (plus * plus13 + minus * minus13 - 2.0) * (1.0 / FZ_NORM)
    fz_d = (4.0 / 3.0 / FZ_NORM) * (plus13 - minus13)
    z2 = zeta * zeta
    z3 = z2 * zeta
    z4 = z2 * z2
    w1 = (-1.0 / FPP_ZERO) * (1.0 - z4)
    diff = ec1 - ec0
    mix = ac * w1 + diff * z4
    ec = ec0 + fz * mix
    ec_r = ec0_r + fz * (ac_r * w1 + (ec1_r - ec0_r) * z4)
    ec_z = fz_d * mix + 4.0 * z3 * fz * (ac * (1.0 / FPP_ZERO) + diff)
    phi = 0.5 * (plus13 * plus13 + minus13 * minus13)
    phi_d = (1.0 / 3.0) * (1.0 / plus13 - 1.0 / minus13)
    inv_phi = 1.0 / phi
    gp3 = GAMMA * phi * phi * phi
    kf_tot = (3.0 * math.pi**2) ** (1.0 / 3.0)
    tfac = (math.pi / (16.0 * kf_tot)) * inv_phi * inv_phi * inv_c * inv_n * inv_n
    inv_gp3 = (1.0 / GAMMA) * inv_phi * inv_phi * inv_phi
    ex = jnp.exp(-ec * inv_gp3)
    amp = (BETA / GAMMA) / (ex - 1.0)
    amp_ec = amp * amp * ex * (GAMMA / BETA) * inv_gp3
    drift = (1.0 / 3.0) * radius * ec_r
    return kf, inv_kn, ec, drift, ec_z, minus, gp3, tfac, amp, amp_ec, phi_d * inv_phi, total


PREPARED = 12


def xc_derivs(prepared, s_own, s_mix, s_other):
    kf, inv_kn, ec, drift, ec_z, minus, gp3, tfac, amp, amp_ec, phi_r, total = prepared
    s2 = s_own * inv_kn * inv_kn
    inv_den = 1.0 / (1.0 + (MU_X / KAPPA) * s2)
    enh = (1.0 + KAPPA) - KAPPA * inv_den
    enh_d = MU_X * inv_den * inv_den
    dn_x = (-1.0 / math.pi) * kf * (enh - 2.0 * s2 * enh_d)
    ds_x = (-3.0 / (8.0 * math.pi)) * enh_d * inv_kn
    sigma = s_own + 2.0 * s_mix + s_other
    t2 = sigma * tfac
    y = amp * t2
    den = 1.0 + y + y * y
    inv_d = 1.0 / den
    ct = (BETA / GAMMA) * t2
    q = ct * (1.0 + y) * inv_d
    grad_h = gp3 * jnp.log(1.0 + q)
    scale = gp3 / (1.0 + q) * inv_d * inv_d
    h_t = scale * ((BETA / GAMMA) * (1.0 + 2.0 * y))
    h_a = -scale * (ct * t2) * (y * (2.0 + y))
    h_ec = h_a * amp_ec
    one_ec = 1.0 + h_ec
    e_n = ec + grad_h - drift * one_ec - (7.0 / 3.0) * t2 * h_t
    e_z = ec_z * one_ec + phi_r * (3.0 * (grad_h - ec * h_ec) - 2.0 * t2 * h_t)
    dn = dn_x + e_n + e_z * minus
    ds_c = total * h_t * tfac
    return dn, ds_x + ds_c, 2.0 * ds_c


def kernel(
    orb_hbm, bands_hbm, core_hbm, out_ref,
    orb, dmat_ref, lane_ref, bands_ref, part, core, x_in, x_out, summed, z_in, zf_in, zf_sum, xf_in,
    dens, dens_o, prepared, grad, grad_o, flux, turned, x_line, x_line_n, x_res, x_res_n, x_back, y_line, y_line_n, y_res, y_res_n, y_back, base, final, x_fin, y_fin,
    orb_sem, core_sem, bands_sem, hop_sem, xs_sem, xr_sem, zs_sem, zr_sem, fs_sem, fr_sem,
    ps_sem, pr_sem, ys_sem, yr_sem, gs_sem, gr_sem, bs_sem, br_sem,
):
    spin = lax.axis_index("spin")
    band = lax.axis_index("band")
    grid = lax.axis_index("grid")
    bx, bz = band // NZ4, lax.rem(band, NZ4)
    gz, gy = grid // GY, lax.rem(grid, GY)

    def half_of(z):
        q = z // 2
        return 3 * q + z * (1 - 2 * q)

    q, h, e = bz // 2, half_of(bz), lax.rem(bz, 2)
    member = 2 * bx + q
    partner = (1 - spin, band, grid)

    def at_band(x, z, core=spin):
        return (core, lax.rem(x, NX4) * NZ4 + lax.rem(z, NZ4), grid)

    def copy(src, dst, send_sem, recv_sem, device):
        return pltpu.make_async_remote_copy(
            src_ref=src, dst_ref=dst, send_sem=send_sem, recv_sem=recv_sem,
            device_id=device, device_id_type=MESH,
        )

    def send(*args):
        copy(*args).start()

    def sent(like, send_sem):
        copy(like, like, send_sem, send_sem, (spin, band, grid)).wait_send()

    def arrived(like, recv_sem):
        copy(like, like, recv_sem, recv_sem, (spin, band, grid)).wait_recv()

    def rows_at(start, count):
        return pl.ds(pl.multiple_of(start, 8), count)

    bands_copy = pltpu.make_async_copy(bands_hbm, bands_ref, bands_sem)
    bands_copy.start()
    z_all = 2 * bz + gz
    near = [at_band(bx + 1, bz), at_band(bx + 3, bz)]
    near += [(spin, band, gz * GY + lax.rem(gy + d, GY)) for d in (1, 3)]
    for d in (1, 7):
        z = lax.rem(z_all + d, 8)
        near += [(spin, bx * NZ4 + z // 2, lax.rem(z, 2) * GY + gy)]
    barrier = pltpu.get_barrier_semaphore()
    across = [(1 - spin, *peer[1:]) for peer in near]
    aside = [at_band(bx, bz + d) for d in (1, 3)]
    entry = (*near, *across, partner, *aside)
    for peer in entry:
        pl.semaphore_signal(barrier, inc=1, device_id=peer, device_id_type=MESH)

    def y_of(r):
        return pl.multiple_of(lax.rem(bx + r, NX4) * YQ, YQ)

    def y_at(r):
        return pl.ds(r * YQ, YQ)

    def load(k, cs, r):
        for c in cs:
            for half in range(2):
                pltpu.make_async_copy(
                    orb_hbm.at[0, :, pl.ds(8 * half + 2 * c, 2), pl.ds(y_of(r), YQ), :],
                    orb.at[:, c, half, :, y_at(r), :],
                    orb_sem.at[k],
                ).start()

    def loaded(k, window):
        pltpu.make_async_copy(window, window, orb_sem.at[k]).wait()

    load(0, (0,), 2)
    for r in range(NX4):
        load(2, (3,), r)
    load(1, (1, 2), 2)
    for k, r in ((3, 1), (4, 3), (5, 0)):
        load(k, (0, 1, 2), r)
    core_copy = pltpu.make_async_copy(
        core_hbm.at[rows_at(8 * h, 8), rows_at(YQ * bx + 16 * q, 16), :], core, core_sem
    )
    core_copy.start()

    with jax.named_scope("first_piece"):
        bands_copy.wait()
        first = bands_ref[0, 0]
        last = first + bands_ref[0, 1]
        weights = []
        for b in range(8):
            ident = band * 8 + b
            weights.append(jnp.where((ident >= first) & (ident < last), 0.5, 1.0).astype(F32))

    def density(c, r):
        acc = None
        for b in range(8):
            v = orb[b, c, :, :, r * YQ : (r + 1) * YQ, :].astype(F32)
            term = weights[b] * (v * v)
            acc = term if acc is None else acc + term
        part[r, c] = acc

    plus, minus = at_band(bx + 1, bz), at_band(bx + 3, bz)

    def x_send(stream, c, src):
        target = minus if stream % 2 else plus
        send(src, x_in.at[c, stream], xs_sem, xr_sem.at[c, int(stream > 1)], target)

    def far(c):
        x_send(0, c, part.at[2, c, 0])
        x_send(1, c, part.at[2, c, 1])

    def direct(c):
        x_send(2, c, part.at[1, c, 1])
        x_send(3, c, part.at[3, c, 0])

    def relay(c):
        arrived(x_in.at[c, 0:2], xr_sem.at[c, 0])
        for side, r in ((0, 1), (1, 3)):
            x_out[side, c] = part[r, c, side] + x_in[c, side]
            x_send(4 + side, c, x_out.at[side, c])

    def z_targets(ds, core):
        for d in ds:
            z = lax.rem(bz + d, NZ4)
            yield d, half_of(z), rows_at(16 * (z // 2), 16), at_band(bx, z, core)

    def finish(c):
        arrived(x_in.at[c, 2:6], xr_sem.at[c, 1])
        if c == 0:
            hear(3)
        summed[c, 0] = part[0, c, 0] + x_in[c, 4] + x_in[c, 3]
        summed[c, 1] = part[0, c, 1] + x_in[c, 5] + x_in[c, 2]
        for slot, half, ys, device in z_targets((2, 1, 3, 0), 1 - spin):
            send(summed.at[c, half, :, ys, :], z_in.at[slot, c], zs_sem, zr_sem, device)

    def z_first(ds):
        for slot, half, ys, device in z_targets(ds, spin):
            send(part.at[:, 3, half, :, ys, :], zf_in.at[slot - 1], fs_sem.at[0], fr_sem.at[0], device)

    def dmat_table():
        table = derivative_matrix()
        hi = table.astype(jnp.bfloat16)
        lo = (table - hi.astype(F32)).astype(jnp.bfloat16)
        dmat_ref[...] = jnp.concatenate([hi, hi, lo], 1)
        lane_ref[...] = jnp.concatenate([hi, lo, hi], 0)

    def tell(k):
        for peer in near:
            pl.semaphore_signal(hop_sem.at[k - 1], inc=1, device_id=peer, device_id_type=MESH)

    def hear(k):
        pl.semaphore_wait(hop_sem.at[k - 1], len(near))
        if k < HOPS:
            tell(k + 1)

    loaded(0, orb.at[:, 0, :, :, y_at(2), :])
    density(0, 2)
    with jax.named_scope("barrier"):
        pl.semaphore_wait(barrier, len(entry))
    with jax.named_scope("rs_head"):
        far(0)
        for peer in aside:
            pl.semaphore_signal(hop_sem.at[HOPS], inc=1, device_id=peer, device_id_type=MESH)
        tell(1)
        loaded(2, orb.at[:, 3])
        for r in range(NX4):
            density(3, r)
        z_first((1, 3))
        loaded(1, orb.at[:, 1:3, :, :, y_at(2), :])
        density(1, 2)
        far(1)
        density(2, 2)
        far(2)
        loaded(3, orb.at[:, 0:3, :, :, y_at(1), :])
        loaded(4, orb.at[:, 0:3, :, :, y_at(3), :])
        density(0, 1)
        density(0, 3)
        direct(0)
        for c, r in ((1, 1), (1, 3), (2, 1), (2, 3)):
            density(c, r)
    with jax.named_scope("hear_z"):
        pl.semaphore_wait(hop_sem.at[HOPS], 2)
        z_first((2,))
    with jax.named_scope("rs_rest"):
        hear(1)
        loaded(5, orb.at[:, 0:3, :, :, y_at(0), :])
        for c in range(CH):
            density(c, 0)
        dmat_table()
    for c in range(CH):
        with jax.named_scope(f"relay{c}"):
            relay(c)
        if c + 1 < CH:
            direct(c + 1)
    core_copy.wait()
    with jax.named_scope("hear2"):
        hear(2)
    for c in range(CH):
        with jax.named_scope(f"finish{c}"):
            finish(c)

    y_mine = rows_at(16 * q, 16)
    with jax.named_scope("zf_wait"):
        arrived(zf_in, fr_sem.at[0])
        zf_sum[...] = part[:, 3, h, :, y_mine, :] + zf_in[0] + zf_in[1] + zf_in[2]
        for r in (2, 1, 3, 0):
            send(
                zf_sum.at[r], xf_in.at[r], fs_sem.at[1], fr_sem.at[1],
                at_band(bx + r, bz, 1 - spin),
            )
    with jax.named_scope("hear4"):
        hear(4)
    with jax.named_scope("z_wait"):
        arrived(z_in, zr_sem)
    for c in range(CH):
        block = 0.5 * core[2 * c : 2 * c + 2] + z_in[0, c] + z_in[1, c] + z_in[2, c] + z_in[3, c]
        dens[32 * c : 32 * c + 32, :] = block.reshape(32, N)
    with jax.named_scope("hear5"):
        hear(5)
    with jax.named_scope("xf_wait"):
        arrived(xf_in, fr_sem.at[1])
    block = 0.5 * core[2 * CH : 2 * CH + 2] + xf_in[0] + xf_in[1] + xf_in[2] + xf_in[3]
    dens[32 * CH : 32 * CH + 32, :] = block.reshape(32, N)

    def halves(x):
        hi = x.astype(jnp.bfloat16)
        return hi, (x - hi.astype(F32)).astype(jnp.bfloat16)

    def along_rows(x):
        hi, lo = halves(x)
        return jnp.dot(dmat_ref[...], jnp.concatenate([hi, lo, hi], 0), preferred_element_type=F32)

    def along_lanes(x):
        hi, lo = halves(x)
        return jnp.dot(jnp.concatenate([hi, hi, lo], 1), lane_ref[...], preferred_element_type=F32)

    def pass_on(src, dst, send_sem, recv_sem, local):
        if local:
            dst[...] = src[...]
        else:
            send(src, dst, send_sem, recv_sem, partner)

    def y_exchange(src, dst, ks, kr, core, local=False):
        for dx, dq in ((2, 1), (1, 1), (3, 1), (0, 1), (2, 0), (1, 0), (3, 0)):
            x, place = lax.rem(bx + dx, NX4), lax.rem(q + dq, 2)
            z = h + place * (3 - 2 * h)
            send(
                src.at[rows_at(16 * (2 * x + place), 16), :], dst.at[rows_at(16 * member, 16), :],
                ys_sem.at[ks], yr_sem.at[kr], (core, x * NZ4 + z, grid),
            )
        mine = rows_at(16 * member, 16)
        pass_on(src.at[mine, :], dst.at[mine, :], ys_sem.at[ks], yr_sem.at[kr], local)

    def x_exchange(src, dst, ks, kr, core, local=False, back=False):
        for de in (1, 0):
            for dz in (1, 0):
                for dy in (2, 1, 3, 0):
                    if (de, dz, dy) == (0, 0, 0):
                        continue
                    e2 = lax.rem(e + de, 2)
                    g2 = lax.rem(gz + dz, 2) * GY + lax.rem(gy + dy, GY)
                    z = 2 * q + e2
                    there, here = 8 * e2 + g2, 2 * grid + h
                    if back:
                        there, here = 2 * g2 + half_of(z), 8 * e + grid
                    send(
                        src.at[rows_at(8 * there, 8), :], dst.at[rows_at(8 * here, 8), :],
                        gs_sem.at[ks], gr_sem.at[kr], (core, bx * NZ4 + z, g2),
                    )
        mine = (2 * grid + h, 8 * e + grid)
        there, here = mine if back else mine[::-1]
        there, here = rows_at(8 * there, 8), rows_at(8 * here, 8)
        pass_on(src.at[there, :], dst.at[here, :], gs_sem.at[ks], gr_sem.at[kr], local)

    def y_wait(dst, k, local=False):
        arrived(dst.at[0 : N - 16, :] if local else dst, yr_sem.at[k])

    def x_wait(dst, k, local=False):
        arrived(dst.at[0 : N - 8, :] if local else dst, gr_sem.at[k])

    def out_y(src, core, local=False):
        xr = rows_at(8 * (8 * h + member), 8)
        for dx in (2, 1, 3, 0):
            for dz in (2, 1, 3, 0):
                if (dx, dz) != (0, 0):
                    b2 = lax.rem(bx + dx, NX4) * NZ4 + lax.rem(bz + dz, NZ4)
                    send(
                        src.at[rows_at(8 * b2, 8), :], y_fin.at[xr, :],
                        ys_sem.at[3], yr_sem.at[3], (core, b2, grid),
                    )
        pass_on(src.at[rows_at(8 * band, 8), :], y_fin.at[xr, :], ys_sem.at[3], yr_sem.at[3], local)

    def out_x(src, core, local=False):
        mine = rows_at(XR * grid, XR)
        for dz, dy in ((1, 2), (1, 1), (1, 3), (0, 2), (1, 0), (0, 1), (0, 3)):
            g2 = lax.rem(gz + dz, 2) * GY + lax.rem(gy + dy, GY)
            send(
                src.at[rows_at(XR * g2, XR), :], x_fin.at[mine, :],
                gs_sem.at[3], gr_sem.at[3], (core, band, g2),
            )
        pass_on(src.at[mine, :], x_fin.at[mine, :], gs_sem.at[3], gr_sem.at[3], local)

    def turn(src, dst):
        for t in range(16):
            dst[8 * t : 8 * t + 8, :] = src[pl.ds(t, 8, stride=16), :]

    with jax.named_scope("fwd0"):

        @pl.when(spin == 0)
        def _():
            y_exchange(dens, y_line.at[0], 0, 0, 1)
            turn(dens, turned.at[0])
            x_exchange(turned.at[0], x_line.at[0], 0, 0, 1)

        @pl.when(spin == 1)
        def _():
            y_exchange(dens, y_line_n.at[0], 4, 4, 1, local=True)
            turn(dens, turned.at[0])
            x_exchange(turned.at[0], x_line_n.at[0], 4, 4, 1, local=True)

        send(dens, dens_o, ps_sem, pr_sem.at[0], partner)
        grad[2] = -along_lanes(dens[...])
        send(grad.at[2], grad_o.at[2], ps_sem, pr_sem.at[1], partner)
    with jax.named_scope("drain0"):
        sent(part.at[0:3, 0:CH], xs_sem)
        sent(z_in, zs_sem)
        sent(zf_in, fs_sem.at[0])
        sent(xf_in, fs_sem.at[1])
    with jax.named_scope("prepare"):
        arrived(dens_o, pr_sem.at[0])
        step = 16
        for i in range(0, N, step):
            rows = slice(i, i + step)
            for k, known in enumerate(xc_prepare(dens_o[rows, :], dens[rows, :])):
                prepared[k, rows, :] = known
    with jax.named_scope("lines0"):

        @pl.when(spin == 1)
        def _():
            y_wait(y_line.at[0], 0)
            y_res[0] = along_rows(y_line[0])
            y_exchange(y_res.at[0], y_back, 1, 1, 0)
            x_wait(x_line.at[0], 0)
            x_res[0] = along_rows(x_line[0])
            x_exchange(x_res.at[0], x_back, 1, 1, 0, back=True)
            y_wait(y_line_n.at[0], 4, local=True)
            y_res_n[0] = along_rows(y_line_n[0])
            y_exchange(y_res_n.at[0], y_back, 1, 1, 1, local=True)
            x_wait(x_line_n.at[0], 4, local=True)
            x_res_n[0] = along_rows(x_line_n[0])
            x_exchange(x_res_n.at[0], x_back, 1, 1, 1, local=True, back=True)

    with jax.named_scope("y_back0"):
        pl.when(spin == 0)(lambda: y_wait(y_back, 1))
        pl.when(spin == 1)(lambda: y_wait(y_back, 1, local=True))
        send(y_back, grad_o.at[1], ps_sem, pr_sem.at[1], partner)
    with jax.named_scope("x_back0"):
        pl.when(spin == 0)(lambda: x_wait(x_back, 1))
        pl.when(spin == 1)(lambda: x_wait(x_back, 1, local=True))
        for i in range(8):
            grad[0, 16 * i : 16 * i + 16, :] = x_back[pl.ds(i, 16, stride=8), :]
    with jax.named_scope("swap"):
        send(grad.at[0], grad_o.at[0], ps_sem, pr_sem.at[1], partner)
        arrived(grad_o, pr_sem.at[1])

    with jax.named_scope("xc"):
        for i in range(0, N, step):
            rows = slice(i, i + step)
            o = (grad[0, rows, :], y_back[rows, :], grad[2, rows, :])
            g = (grad_o[0, rows, :], grad_o[1, rows, :], grad_o[2, rows, :])
            s_own = g[0] * g[0] + g[1] * g[1] + g[2] * g[2]
            s_mix = g[0] * o[0] + g[1] * o[1] + g[2] * o[2]
            s_other = o[0] * o[0] + o[1] * o[1] + o[2] * o[2]
            known = [prepared[k, rows, :] for k in range(PREPARED)]
            dn, ds, dm = xc_derivs(known, s_own, s_mix, s_other)
            for a in range(3):
                flux[a, rows, :] = 2.0 * ds * g[a] + dm * o[a]
            flux[3, rows, :] = dn

    with jax.named_scope("fwd1"):

        @pl.when(spin == 0)
        def _():
            y_exchange(flux.at[1], y_line.at[1], 2, 2, 1)
            turn(flux.at[0], turned.at[1])
            x_exchange(turned.at[1], x_line.at[1], 2, 2, 1)

        @pl.when(spin == 1)
        def _():
            y_exchange(flux.at[1], y_line_n.at[1], 5, 5, 1, local=True)
            turn(flux.at[0], turned.at[1])
            x_exchange(turned.at[1], x_line_n.at[1], 5, 5, 1, local=True)

        base[...] = (flux[3] + along_lanes(flux[2])).reshape(8, 16, N)
        there = lax.rem(e + 1, 2)
        send(
            base.at[:, rows_at(8 * there, 8), :], final.at[h],
            bs_sem, br_sem, (spin, bx * NZ4 + 2 * q + there, grid),
        )
        final[h] = base[:, rows_at(8 * e, 8), :]
    with jax.named_scope("drain1"):

        @pl.when(spin == 0)
        def _():
            sent(y_line.at[0], ys_sem.at[0])
            sent(x_line.at[0], gs_sem.at[0])

        @pl.when(spin == 1)
        def _():
            for k in (1, 4):
                sent(y_line.at[0, 0 : N - 16, :], ys_sem.at[k])
                sent(x_line.at[0, 0 : N - 8, :], gs_sem.at[k])
            sent(y_line.at[0], ys_sem.at[1])
            sent(x_line.at[0], gs_sem.at[1])

        sent(grad_o, ps_sem)
        sent(dens_o, ps_sem)
    with jax.named_scope("lines1"):

        @pl.when(spin == 1)
        def _():
            y_wait(y_line_n.at[1], 5, local=True)
            y_res_n[1] = along_rows(y_line_n[1])
            out_y(y_res_n.at[1], 1, local=True)
            x_wait(x_line_n.at[1], 5, local=True)
            x_res_n[1] = along_rows(x_line_n[1])
            out_x(x_res_n.at[1], 1, local=True)
            y_wait(y_line.at[1], 2)
            y_res[1] = along_rows(y_line[1])
            out_y(y_res.at[1], 0)
            x_wait(x_line.at[1], 2)
            x_res[1] = along_rows(x_line[1])
            out_x(x_res.at[1], 0)

    with jax.named_scope("drain2"):

        @pl.when(spin == 0)
        def _():
            sent(y_line.at[0], ys_sem.at[2])
            sent(x_line.at[0], gs_sem.at[2])

        @pl.when(spin == 1)
        def _():
            sent(y_line.at[0, 0 : N - 16, :], ys_sem.at[5])
            sent(x_line.at[0, 0 : N - 8, :], gs_sem.at[5])
            sent(y_line.at[0, 0 : N - YB, :], ys_sem.at[3])
            sent(x_line.at[0, 0 : N - XR, :], gs_sem.at[3])
            sent(y_line.at[0], ys_sem.at[3])
            sent(x_line.at[0], gs_sem.at[3])

        sent(final.at[0], bs_sem)
        arrived(final.at[0], br_sem)
    with jax.named_scope("x_back1"):
        pl.when(spin == 0)(lambda: arrived(x_fin, gr_sem.at[3]))
        pl.when(spin == 1)(lambda: arrived(x_fin.at[0 : N - XR, :], gr_sem.at[3]))
        for i in range(XR):
            out_ref[0, i] = final[i // 8, i % 8] - x_fin[pl.ds(i, YB, stride=XR), :]
    with jax.named_scope("y_back1"):
        pl.when(spin == 0)(lambda: arrived(y_fin, yr_sem.at[3]))
        pl.when(spin == 1)(lambda: arrived(y_fin.at[0 : N - YB, :], yr_sem.at[3]))
    with jax.named_scope("tail"):
        out_ref[0] = out_ref[0] - y_fin[...].reshape(XR, YB, N)


def per_device(orbitals, partial_bands, core_density):
    vm = pltpu.VMEM
    sem = pltpu.SemaphoreType.DMA
    anyspace = pl.BlockSpec(memory_space=pltpu.HBM)
    return pl.pallas_call(
        kernel,
        out_shape=jax.ShapeDtypeStruct((1, XR, YB, N), F32),
        in_specs=[anyspace] * 3,
        out_specs=pl.BlockSpec(memory_space=pltpu.VMEM),
        scratch_shapes=[
            vm((8, CH + 1, 2, 2, N, N), jnp.bfloat16),
            vm((N, 3 * N), jnp.bfloat16),
            vm((3 * N, N), jnp.bfloat16),
            pltpu.SMEM((1, 2), jnp.int32),
            vm((NX4, CH + 1, 2, 2, YQ, N), F32),
            vm((8, 16, N), F32),
            vm((CH, 6, 2, YQ, N), F32),
            vm((2, CH, 2, YQ, N), F32),
            vm((CH, 2, 2, YQ, N), F32),
            vm((NZ4, CH, 2, 16, N), F32),
            vm((NZ4 - 1, NX4, 2, 16, N), F32),
            vm((NX4, 2, 16, N), F32),
            vm((NX4, 2, 16, N), F32),
            vm((N, N), F32),
            vm((N, N), F32),
            vm((PREPARED, N, N), F32),
            vm((3, N, N), F32),
            vm((3, N, N), F32),
            vm((4, N, N), F32),
            vm((2, N, N), F32),
            vm((2, N, N), F32),
            vm((2, N, N), F32),
            vm((2, N, N), F32),
            vm((2, N, N), F32),
            vm((N, N), F32),
            vm((2, N, N), F32),
            vm((2, N, N), F32),
            vm((2, N, N), F32),
            vm((2, N, N), F32),
            vm((N, N), F32),
            vm((8, 16, N), F32),
            vm((2, 8, YB, N), F32),
            vm((N, N), F32),
            vm((N, N), F32),
            sem((6,)),
            sem,
            sem,
            pltpu.SemaphoreType.REGULAR((HOPS + 1,)),
            sem,
            sem((CH, 2)),
            sem,
            sem,
            sem((2,)),
            sem((2,)),
            sem,
            sem((2,)),
            sem((6,)),
            sem((6,)),
            sem((6,)),
            sem((6,)),
            sem,
            sem,
        ],
        compiler_params=pltpu.CompilerParams(
            collective_id=0, has_side_effects=True, vmem_limit_bytes=54400 * 1024
        ),
    )(*[pltpu.with_memory_space_constraint(a, pltpu.HBM) for a in (orbitals, partial_bands, core_density)])


def solution(mesh):
    in_specs = (P("spin", "band", "grid", None, None), P("spin", None), P("grid", None, None))
    out_specs = P("spin", "grid", "band", None)

    return jax.shard_map(
        per_device, mesh=mesh, in_specs=in_specs, out_specs=out_specs, check_vma=False
    )
```

```python
import math

import jax
import jax.numpy as jnp
from jax import lax
from jax.experimental import pallas as pl
from jax.experimental.pallas import tpu as pltpu
from jax.sharding import PartitionSpec as P

KAPPA = 0.804
MU_X = 0.2195149727645171
BETA = 0.06672455060314922
GAMMA = (1.0 - math.log(2.0)) / math.pi**2
FZ_NORM = 2.0 ** (4.0 / 3.0) - 2.0
FPP_ZERO = 1.709921

MESH = pl.DeviceIdType.MESH
F32 = jnp.float32
N = 128
XR = 16
NX4 = 4
NZ4 = 4
GY = 4
GRID = 2 * GY
BAND = NX4 * NZ4
YB = N // BAND
YQ = N // NX4
CH = 3
HOPS = 5


def derivative_matrix():
    k = lax.broadcasted_iota(jnp.int32, (N, N), 0) - lax.broadcasted_iota(jnp.int32, (N, N), 1)
    far = jnp.abs(k)
    near = jnp.minimum(far, N - far)
    angle = (math.pi / N) * jnp.maximum(near, 1).astype(F32)
    size = (math.pi / N) * jnp.cos(angle) / jnp.sin(angle)
    flips = (k < 0).astype(jnp.int32) + (far > N // 2).astype(jnp.int32) + (far & 1)
    signed = jnp.where((flips & 1) == 1, -size, size)
    return jnp.where(k == 0, 0.0, signed)


def pw_fit(r, root, amp, alpha, b1, b2, b3, b4):
    denom = (2.0 * amp) * (root * (b1 + root * (b2 + root * (b3 + root * b4))))
    slope = (2.0 * amp) * (0.5 * b1 / root + (b2 + root * (1.5 * b3 + root * (2.0 * b4))))
    log = jnp.log(1.0 + 1.0 / denom)
    front = (-2.0 * amp) * (1.0 + alpha * r)
    value = front * log
    deriv = (-2.0 * amp * alpha) * log - front * slope / (denom * (denom + 1.0))
    return value, deriv


def cbrt(x):
    return jnp.exp(jnp.log(x) * (1.0 / 3.0))


def xc_prepare(own, other):
    total = own + other
    inv_n = 1.0 / total
    c_own = cbrt(own)
    c_other = cbrt(other)
    c_tot = cbrt(total)
    inv_c = 1.0 / c_tot
    double = 2.0 * own
    kf = (6.0 * math.pi**2) ** (1.0 / 3.0) * c_own
    inv_kn = 1.0 / (kf * double)
    two13 = 2.0 ** (1.0 / 3.0)
    plus = double * inv_n
    minus = 2.0 * other * inv_n
    zeta = (own - other) * inv_n
    plus13 = two13 * c_own * inv_c
    minus13 = two13 * c_other * inv_c
    radius = (3.0 / (4.0 * math.pi)) ** (1.0 / 3.0) * inv_c
    root = jnp.sqrt(radius)
    ec0, ec0_r = pw_fit(radius, root, 0.031091, 0.2137, 7.5957, 3.5876, 1.6382, 0.49294)
    ec1, ec1_r = pw_fit(radius, root, 0.015545, 0.20548, 14.1189, 6.1977, 3.3662, 0.62517)
    ac, ac_r = pw_fit(radius, root, 0.016887, 0.11125, 10.357, 3.6231, 0.88026, 0.49671)
    fz = (plus * plus13 + minus * minus13 - 2.0) * (1.0 / FZ_NORM)
    fz_d = (4.0 / 3.0 / FZ_NORM) * (plus13 - minus13)
    z2 = zeta * zeta
    z3 = z2 * zeta
    z4 = z2 * z2
    w1 = (-1.0 / FPP_ZERO) * (1.0 - z4)
    diff = ec1 - ec0
    mix = ac * w1 + diff * z4
    ec = ec0 + fz * mix
    ec_r = ec0_r + fz * (ac_r * w1 + (ec1_r - ec0_r) * z4)
    ec_z = fz_d * mix + 4.0 * z3 * fz * (ac * (1.0 / FPP_ZERO) + diff)
    phi = 0.5 * (plus13 * plus13 + minus13 * minus13)
    phi_d = (1.0 / 3.0) * (1.0 / plus13 - 1.0 / minus13)
    inv_phi = 1.0 / phi
    gp3 = GAMMA * phi * phi * phi
    kf_tot = (3.0 * math.pi**2) ** (1.0 / 3.0)
    tfac = (math.pi / (16.0 * kf_tot)) * inv_phi * inv_phi * inv_c * inv_n * inv_n
    inv_gp3 = (1.0 / GAMMA) * inv_phi * inv_phi * inv_phi
    ex = jnp.exp(-ec * inv_gp3)
    amp = (BETA / GAMMA) / (ex - 1.0)
    amp_ec = amp * amp * ex * (GAMMA / BETA) * inv_gp3
    drift = (1.0 / 3.0) * radius * ec_r
    return kf, inv_kn, ec, drift, ec_z, minus, gp3, tfac, amp, amp_ec, phi_d * inv_phi, total


PREPARED = 12


def xc_derivs(prepared, s_own, s_mix, s_other):
    kf, inv_kn, ec, drift, ec_z, minus, gp3, tfac, amp, amp_ec, phi_r, total = prepared
    s2 = s_own * inv_kn * inv_kn
    inv_den = 1.0 / (1.0 + (MU_X / KAPPA) * s2)
    enh = (1.0 + KAPPA) - KAPPA * inv_den
    enh_d = MU_X * inv_den * inv_den
    dn_x = (-1.0 / math.pi) * kf * (enh - 2.0 * s2 * enh_d)
    ds_x = (-3.0 / (8.0 * math.pi)) * enh_d * inv_kn
    sigma = s_own + 2.0 * s_mix + s_other
    t2 = sigma * tfac
    y = amp * t2
    den = 1.0 + y + y * y
    inv_d = 1.0 / den
    ct = (BETA / GAMMA) * t2
    q = ct * (1.0 + y) * inv_d
    grad_h = gp3 * jnp.log(1.0 + q)
    scale = gp3 / (1.0 + q) * inv_d * inv_d
    h_t = scale * ((BETA / GAMMA) * (1.0 + 2.0 * y))
    h_a = -scale * (ct * t2) * (y * (2.0 + y))
    h_ec = h_a * amp_ec
    one_ec = 1.0 + h_ec
    e_n = ec + grad_h - drift * one_ec - (7.0 / 3.0) * t2 * h_t
    e_z = ec_z * one_ec + phi_r * (3.0 * (grad_h - ec * h_ec) - 2.0 * t2 * h_t)
    dn = dn_x + e_n + e_z * minus
    ds_c = total * h_t * tfac
    return dn, ds_x + ds_c, 2.0 * ds_c


def kernel(
    orb_hbm, bands_hbm, core_hbm, out_ref,
    orb, dmat_ref, lane_ref, bands_ref, part, core, x_in, x_out, summed, z_in, zf_in, zf_sum, xf_in,
    dens, dens_o, prepared, grad, grad_o, flux, turned, x_line, x_line_n, x_res, x_res_n, x_back, y_line, y_line_n, y_res, y_res_n, y_back, base, final, x_fin, y_fin,
    orb_sem, core_sem, bands_sem, hop_sem, xs_sem, xr_sem, zs_sem, zr_sem, fs_sem, fr_sem,
    ps_sem, pr_sem, es_sem, yr_sem, gr_sem, bs_sem, br_sem,
):
    spin = lax.axis_index("spin")
    band = lax.axis_index("band")
    grid = lax.axis_index("grid")
    bx, bz = band // NZ4, lax.rem(band, NZ4)
    gz, gy = grid // GY, lax.rem(grid, GY)

    def half_of(z):
        q = z // 2
        return 3 * q + z * (1 - 2 * q)

    q, h, e = bz // 2, half_of(bz), lax.rem(bz, 2)
    member = 2 * bx + q
    partner = (1 - spin, band, grid)

    def at_band(x, z, core=spin):
        return (core, lax.rem(x, NX4) * NZ4 + lax.rem(z, NZ4), grid)

    def copy(src, dst, send_sem, recv_sem, device):
        return pltpu.make_async_remote_copy(
            src_ref=src, dst_ref=dst, send_sem=send_sem, recv_sem=recv_sem,
            device_id=device, device_id_type=MESH,
        )

    def send(*args):
        copy(*args).start()

    def sent(like, send_sem):
        copy(like, like, send_sem, send_sem, (spin, band, grid)).wait_send()

    def arrived(like, recv_sem):
        copy(like, like, recv_sem, recv_sem, (spin, band, grid)).wait_recv()

    def rows_at(start, count):
        return pl.ds(pl.multiple_of(start, 8), count)

    bands_copy = pltpu.make_async_copy(bands_hbm, bands_ref, bands_sem)
    bands_copy.start()
    z_all = 2 * bz + gz
    near = [at_band(bx + 1, bz), at_band(bx + 3, bz)]
    near += [(spin, band, gz * GY + lax.rem(gy + d, GY)) for d in (1, 3)]
    for d in (1, 7):
        z = lax.rem(z_all + d, 8)
        near += [(spin, bx * NZ4 + z // 2, lax.rem(z, 2) * GY + gy)]
    barrier = pltpu.get_barrier_semaphore()
    across = [(1 - spin, *peer[1:]) for peer in near]
    aside = [at_band(bx, bz + d) for d in (1, 3)]
    entry = (*near, *across, partner, *aside)
    for peer in entry:
        pl.semaphore_signal(barrier, inc=1, device_id=peer, device_id_type=MESH)

    def y_of(r):
        return pl.multiple_of(lax.rem(bx + r, NX4) * YQ, YQ)

    def y_at(r):
        return pl.ds(r * YQ, YQ)

    def load(k, cs, r):
        for c in cs:
            for half in range(2):
                pltpu.make_async_copy(
                    orb_hbm.at[0, :, pl.ds(8 * half + 2 * c, 2), pl.ds(y_of(r), YQ), :],
                    orb.at[:, c, half, :, y_at(r), :],
                    orb_sem.at[k],
                ).start()

    def loaded(k, window):
        pltpu.make_async_copy(window, window, orb_sem.at[k]).wait()

    load(0, (0,), 2)
    for r in range(NX4):
        load(2, (3,), r)
    load(1, (1, 2), 2)
    for k, r in ((3, 1), (4, 3), (5, 0)):
        load(k, (0, 1, 2), r)
    core_copy = pltpu.make_async_copy(
        core_hbm.at[rows_at(8 * h, 8), rows_at(YQ * bx + 16 * q, 16), :], core, core_sem
    )
    core_copy.start()

    with jax.named_scope("first_piece"):
        bands_copy.wait()
        first = bands_ref[0, 0]
        last = first + bands_ref[0, 1]
        weights = []
        for b in range(8):
            ident = band * 8 + b
            weights.append(jnp.where((ident >= first) & (ident < last), 0.5, 1.0).astype(F32))

    def density(c, r):
        acc = None
        for b in range(8):
            v = orb[b, c, :, :, r * YQ : (r + 1) * YQ, :].astype(F32)
            term = weights[b] * (v * v)
            acc = term if acc is None else acc + term
        part[r, c] = acc

    plus, minus = at_band(bx + 1, bz), at_band(bx + 3, bz)

    def x_send(stream, c, src):
        target = minus if stream % 2 else plus
        send(src, x_in.at[c, stream], xs_sem, xr_sem.at[c, int(stream > 1)], target)

    def far(c):
        x_send(0, c, part.at[2, c, 0])
        x_send(1, c, part.at[2, c, 1])

    def direct(c):
        x_send(2, c, part.at[1, c, 1])
        x_send(3, c, part.at[3, c, 0])

    def relay(c):
        arrived(x_in.at[c, 0:2], xr_sem.at[c, 0])
        for side, r in ((0, 1), (1, 3)):
            x_out[side, c] = part[r, c, side] + x_in[c, side]
            x_send(4 + side, c, x_out.at[side, c])

    def z_targets(ds, core):
        for d in ds:
            z = lax.rem(bz + d, NZ4)
            yield d, half_of(z), rows_at(16 * (z // 2), 16), at_band(bx, z, core)

    def finish(c):
        arrived(x_in.at[c, 2:6], xr_sem.at[c, 1])
        if c == 0:
            hear(3)
        summed[c, 0] = part[0, c, 0] + x_in[c, 4] + x_in[c, 3]
        summed[c, 1] = part[0, c, 1] + x_in[c, 5] + x_in[c, 2]
        for slot, half, ys, device in z_targets((2, 1, 3, 0), 1 - spin):
            send(summed.at[c, half, :, ys, :], z_in.at[slot, c], zs_sem, zr_sem, device)

    def z_first(ds):
        for slot, half, ys, device in z_targets(ds, spin):
            send(part.at[:, 3, half, :, ys, :], zf_in.at[slot - 1], fs_sem.at[0], fr_sem.at[0], device)

    def dmat_table():
        table = derivative_matrix()
        hi = table.astype(jnp.bfloat16)
        lo = (table - hi.astype(F32)).astype(jnp.bfloat16)
        dmat_ref[...] = jnp.concatenate([hi, hi, lo], 1)
        lane_ref[...] = jnp.concatenate([hi, lo, hi], 0)

    def tell(k):
        for peer in near:
            pl.semaphore_signal(hop_sem.at[k - 1], inc=1, device_id=peer, device_id_type=MESH)

    def hear(k):
        pl.semaphore_wait(hop_sem.at[k - 1], len(near))
        if k < HOPS:
            tell(k + 1)

    loaded(0, orb.at[:, 0, :, :, y_at(2), :])
    density(0, 2)
    with jax.named_scope("barrier"):
        pl.semaphore_wait(barrier, len(entry))
    with jax.named_scope("rs_head"):
        far(0)
        for peer in aside:
            pl.semaphore_signal(hop_sem.at[HOPS], inc=1, device_id=peer, device_id_type=MESH)
        tell(1)
        loaded(2, orb.at[:, 3])
        for r in range(NX4):
            density(3, r)
        z_first((1, 3))
        loaded(1, orb.at[:, 1:3, :, :, y_at(2), :])
        density(1, 2)
        far(1)
        density(2, 2)
        far(2)
        loaded(3, orb.at[:, 0:3, :, :, y_at(1), :])
        loaded(4, orb.at[:, 0:3, :, :, y_at(3), :])
        density(0, 1)
        density(0, 3)
        direct(0)
        for c, r in ((1, 1), (1, 3), (2, 1), (2, 3)):
            density(c, r)
    with jax.named_scope("hear_z"):
        pl.semaphore_wait(hop_sem.at[HOPS], 2)
        z_first((2,))
    with jax.named_scope("rs_rest"):
        hear(1)
        loaded(5, orb.at[:, 0:3, :, :, y_at(0), :])
        for c in range(CH):
            density(c, 0)
        dmat_table()
    for c in range(CH):
        with jax.named_scope(f"relay{c}"):
            relay(c)
        if c + 1 < CH:
            direct(c + 1)
    core_copy.wait()
    with jax.named_scope("hear2"):
        hear(2)
    for c in range(CH):
        with jax.named_scope(f"finish{c}"):
            finish(c)

    y_mine = rows_at(16 * q, 16)
    with jax.named_scope("zf_wait"):
        arrived(zf_in, fr_sem.at[0])
        zf_sum[...] = part[:, 3, h, :, y_mine, :] + zf_in[0] + zf_in[1] + zf_in[2]
        for r in (2, 1, 3, 0):
            send(
                zf_sum.at[r], xf_in.at[r], fs_sem.at[1], fr_sem.at[1],
                at_band(bx + r, bz, 1 - spin),
            )
    with jax.named_scope("hear4"):
        hear(4)
    with jax.named_scope("z_wait"):
        arrived(z_in, zr_sem)
    for c in range(CH):
        block = 0.5 * core[2 * c : 2 * c + 2] + z_in[0, c] + z_in[1, c] + z_in[2, c] + z_in[3, c]
        dens[32 * c : 32 * c + 32, :] = block.reshape(32, N)
    with jax.named_scope("hear5"):
        hear(5)
    with jax.named_scope("xf_wait"):
        arrived(xf_in, fr_sem.at[1])
    block = 0.5 * core[2 * CH : 2 * CH + 2] + xf_in[0] + xf_in[1] + xf_in[2] + xf_in[3]
    dens[32 * CH : 32 * CH + 32, :] = block.reshape(32, N)

    def halves(x):
        hi = x.astype(jnp.bfloat16)
        return hi, (x - hi.astype(F32)).astype(jnp.bfloat16)

    def along_rows(x):
        hi, lo = halves(x)
        return jnp.dot(dmat_ref[...], jnp.concatenate([hi, lo, hi], 0), preferred_element_type=F32)

    def along_lanes(x):
        hi, lo = halves(x)
        return jnp.dot(jnp.concatenate([hi, hi, lo], 1), lane_ref[...], preferred_element_type=F32)

    def pass_on(src, dst, send_sem, recv_sem, local):
        if local:
            dst[...] = src[...]
        else:
            send(src, dst, send_sem, recv_sem, partner)

    def y_exchange(src, dst, ks, kr, core, local=False):
        for dx, dq in ((2, 1), (1, 1), (3, 1), (0, 1), (2, 0), (1, 0), (3, 0)):
            x, place = lax.rem(bx + dx, NX4), lax.rem(q + dq, 2)
            z = h + place * (3 - 2 * h)
            send(
                src.at[rows_at(16 * (2 * x + place), 16), :], dst.at[rows_at(16 * member, 16), :],
                es_sem, yr_sem.at[kr], (core, x * NZ4 + z, grid),
            )
        mine = rows_at(16 * member, 16)
        pass_on(src.at[mine, :], dst.at[mine, :], es_sem, yr_sem.at[kr], local)

    def x_exchange(src, dst, ks, kr, core, local=False, back=False):
        for de in (1, 0):
            for dz in (1, 0):
                for dy in (2, 1, 3, 0):
                    if (de, dz, dy) == (0, 0, 0):
                        continue
                    e2 = lax.rem(e + de, 2)
                    g2 = lax.rem(gz + dz, 2) * GY + lax.rem(gy + dy, GY)
                    z = 2 * q + e2
                    there, here = 8 * e2 + g2, 2 * grid + h
                    if back:
                        there, here = 2 * g2 + half_of(z), 8 * e + grid
                    send(
                        src.at[rows_at(8 * there, 8), :], dst.at[rows_at(8 * here, 8), :],
                        es_sem, gr_sem.at[kr], (core, bx * NZ4 + z, g2),
                    )
        mine = (2 * grid + h, 8 * e + grid)
        there, here = mine if back else mine[::-1]
        there, here = rows_at(8 * there, 8), rows_at(8 * here, 8)
        pass_on(src.at[there, :], dst.at[here, :], es_sem, gr_sem.at[kr], local)

    def y_wait(dst, k, local=False):
        arrived(dst.at[0 : N - 16, :] if local else dst, yr_sem.at[k])

    def x_wait(dst, k, local=False):
        arrived(dst.at[0 : N - 8, :] if local else dst, gr_sem.at[k])

    def out_y(src, core, local=False):
        xr = rows_at(8 * (8 * h + member), 8)
        for dx in (2, 1, 3, 0):
            for dz in (2, 1, 3, 0):
                if (dx, dz) != (0, 0):
                    b2 = lax.rem(bx + dx, NX4) * NZ4 + lax.rem(bz + dz, NZ4)
                    send(
                        src.at[rows_at(8 * b2, 8), :], y_fin.at[xr, :],
                        es_sem, yr_sem.at[3], (core, b2, grid),
                    )
        pass_on(src.at[rows_at(8 * band, 8), :], y_fin.at[xr, :], es_sem, yr_sem.at[3], local)

    def out_x(src, core, local=False):
        mine = rows_at(XR * grid, XR)
        for dz, dy in ((1, 2), (1, 1), (1, 3), (0, 2), (1, 0), (0, 1), (0, 3)):
            g2 = lax.rem(gz + dz, 2) * GY + lax.rem(gy + dy, GY)
            send(
                src.at[rows_at(XR * g2, XR), :], x_fin.at[mine, :],
                es_sem, gr_sem.at[3], (core, band, g2),
            )
        pass_on(src.at[mine, :], x_fin.at[mine, :], es_sem, gr_sem.at[3], local)

    def turn(src, dst):
        for t in range(16):
            dst[8 * t : 8 * t + 8, :] = src[pl.ds(t, 8, stride=16), :]

    with jax.named_scope("fwd0"):

        @pl.when(spin == 0)
        def _():
            y_exchange(dens, y_line.at[0], 0, 0, 1)
            turn(dens, turned.at[0])
            x_exchange(turned.at[0], x_line.at[0], 0, 0, 1)

        @pl.when(spin == 1)
        def _():
            y_exchange(dens, y_line_n.at[0], 4, 4, 1, local=True)
            turn(dens, turned.at[0])
            x_exchange(turned.at[0], x_line_n.at[0], 4, 4, 1, local=True)

        send(dens, dens_o, ps_sem, pr_sem.at[0], partner)
        grad[2] = -along_lanes(dens[...])
        send(grad.at[2], grad_o.at[2], ps_sem, pr_sem.at[1], partner)
    with jax.named_scope("drain0"):
        sent(part.at[0:3, 0:CH], xs_sem)
        sent(z_in, zs_sem)
        sent(zf_in, fs_sem.at[0])
        sent(xf_in, fs_sem.at[1])
    with jax.named_scope("prepare"):
        arrived(dens_o, pr_sem.at[0])
        step = 16
        for i in range(0, N, step):
            rows = slice(i, i + step)
            for k, known in enumerate(xc_prepare(dens_o[rows, :], dens[rows, :])):
                prepared[k, rows, :] = known
    with jax.named_scope("lines0"):

        @pl.when(spin == 1)
        def _():
            y_wait(y_line.at[0], 0)
            y_res[0] = along_rows(y_line[0])
            y_exchange(y_res.at[0], y_back, 1, 1, 0)
            x_wait(x_line.at[0], 0)
            x_res[0] = along_rows(x_line[0])
            x_exchange(x_res.at[0], x_back, 1, 1, 0, back=True)
            y_wait(y_line_n.at[0], 4, local=True)
            y_res_n[0] = along_rows(y_line_n[0])
            y_exchange(y_res_n.at[0], y_back, 1, 1, 1, local=True)
            x_wait(x_line_n.at[0], 4, local=True)
            x_res_n[0] = along_rows(x_line_n[0])
            x_exchange(x_res_n.at[0], x_back, 1, 1, 1, local=True, back=True)

    with jax.named_scope("y_back0"):
        pl.when(spin == 0)(lambda: y_wait(y_back, 1))
        pl.when(spin == 1)(lambda: y_wait(y_back, 1, local=True))
        send(y_back, grad_o.at[1], ps_sem, pr_sem.at[1], partner)
    with jax.named_scope("x_back0"):
        pl.when(spin == 0)(lambda: x_wait(x_back, 1))
        pl.when(spin == 1)(lambda: x_wait(x_back, 1, local=True))
        for i in range(8):
            grad[0, 16 * i : 16 * i + 16, :] = x_back[pl.ds(i, 16, stride=8), :]
    with jax.named_scope("swap"):
        send(grad.at[0], grad_o.at[0], ps_sem, pr_sem.at[1], partner)
        arrived(grad_o, pr_sem.at[1])

    with jax.named_scope("xc"):
        for i in range(0, N, step):
            rows = slice(i, i + step)
            o = (grad[0, rows, :], y_back[rows, :], grad[2, rows, :])
            g = (grad_o[0, rows, :], grad_o[1, rows, :], grad_o[2, rows, :])
            s_own = g[0] * g[0] + g[1] * g[1] + g[2] * g[2]
            s_mix = g[0] * o[0] + g[1] * o[1] + g[2] * o[2]
            s_other = o[0] * o[0] + o[1] * o[1] + o[2] * o[2]
            known = [prepared[k, rows, :] for k in range(PREPARED)]
            dn, ds, dm = xc_derivs(known, s_own, s_mix, s_other)
            for a in range(3):
                flux[a, rows, :] = 2.0 * ds * g[a] + dm * o[a]
            flux[3, rows, :] = dn

    with jax.named_scope("fwd1"):

        @pl.when(spin == 0)
        def _():
            y_exchange(flux.at[1], y_line.at[1], 2, 2, 1)
            turn(flux.at[0], turned.at[1])
            x_exchange(turned.at[1], x_line.at[1], 2, 2, 1)

        @pl.when(spin == 1)
        def _():
            y_exchange(flux.at[1], y_line_n.at[1], 5, 5, 1, local=True)
            turn(flux.at[0], turned.at[1])
            x_exchange(turned.at[1], x_line_n.at[1], 5, 5, 1, local=True)

        base[...] = (flux[3] + along_lanes(flux[2])).reshape(8, 16, N)
        there = lax.rem(e + 1, 2)
        send(
            base.at[:, rows_at(8 * there, 8), :], final.at[h],
            bs_sem, br_sem, (spin, bx * NZ4 + 2 * q + there, grid),
        )
        final[h] = base[:, rows_at(8 * e, 8), :]
    with jax.named_scope("drain1"):
        sent(grad_o, ps_sem)
        sent(dens_o, ps_sem)
    with jax.named_scope("lines1"):

        @pl.when(spin == 1)
        def _():
            y_wait(y_line_n.at[1], 5, local=True)
            y_res_n[1] = along_rows(y_line_n[1])
            out_y(y_res_n.at[1], 1, local=True)
            x_wait(x_line_n.at[1], 5, local=True)
            x_res_n[1] = along_rows(x_line_n[1])
            out_x(x_res_n.at[1], 1, local=True)
            y_wait(y_line.at[1], 2)
            y_res[1] = along_rows(y_line[1])
            out_y(y_res.at[1], 0)
            x_wait(x_line.at[1], 2)
            x_res[1] = along_rows(x_line[1])
            out_x(x_res.at[1], 0)

    with jax.named_scope("drain2"):

        @pl.when(spin == 0)
        def _():
            for _ in range(2):
                sent(y_line, es_sem)

        @pl.when(spin == 1)
        def _():
            for _ in range(2):
                sent(y_line, es_sem)
            for kept in (16, 16, 16, 8, 8, 8, YB, XR):
                sent(y_line.at[0, 0 : N - kept, :], es_sem)

        sent(final.at[0], bs_sem)
        arrived(final.at[0], br_sem)
    with jax.named_scope("x_back1"):
        pl.when(spin == 0)(lambda: arrived(x_fin, gr_sem.at[3]))
        pl.when(spin == 1)(lambda: arrived(x_fin.at[0 : N - XR, :], gr_sem.at[3]))
        for i in range(XR):
            out_ref[0, i] = final[i // 8, i % 8] - x_fin[pl.ds(i, YB, stride=XR), :]
    with jax.named_scope("y_back1"):
        pl.when(spin == 0)(lambda: arrived(y_fin, yr_sem.at[3]))
        pl.when(spin == 1)(lambda: arrived(y_fin.at[0 : N - YB, :], yr_sem.at[3]))
    with jax.named_scope("tail"):
        out_ref[0] = out_ref[0] - y_fin[...].reshape(XR, YB, N)


def per_device(orbitals, partial_bands, core_density):
    vm = pltpu.VMEM
    sem = pltpu.SemaphoreType.DMA
    anyspace = pl.BlockSpec(memory_space=pltpu.HBM)
    return pl.pallas_call(
        kernel,
        out_shape=jax.ShapeDtypeStruct((1, XR, YB, N), F32),
        in_specs=[anyspace] * 3,
        out_specs=pl.BlockSpec(memory_space=pltpu.VMEM),
        scratch_shapes=[
            vm((8, CH + 1, 2, 2, N, N), jnp.bfloat16),
            vm((N, 3 * N), jnp.bfloat16),
            vm((3 * N, N), jnp.bfloat16),
            pltpu.SMEM((1, 2), jnp.int32),
            vm((NX4, CH + 1, 2, 2, YQ, N), F32),
            vm((8, 16, N), F32),
            vm((CH, 6, 2, YQ, N), F32),
            vm((2, CH, 2, YQ, N), F32),
            vm((CH, 2, 2, YQ, N), F32),
            vm((NZ4, CH, 2, 16, N), F32),
            vm((NZ4 - 1, NX4, 2, 16, N), F32),
            vm((NX4, 2, 16, N), F32),
            vm((NX4, 2, 16, N), F32),
            vm((N, N), F32),
            vm((N, N), F32),
            vm((PREPARED, N, N), F32),
            vm((3, N, N), F32),
            vm((3, N, N), F32),
            vm((4, N, N), F32),
            vm((2, N, N), F32),
            vm((2, N, N), F32),
            vm((2, N, N), F32),
            vm((2, N, N), F32),
            vm((2, N, N), F32),
            vm((N, N), F32),
            vm((2, N, N), F32),
            vm((2, N, N), F32),
            vm((2, N, N), F32),
            vm((2, N, N), F32),
            vm((N, N), F32),
            vm((8, 16, N), F32),
            vm((2, 8, YB, N), F32),
            vm((N, N), F32),
            vm((N, N), F32),
            sem((6,)),
            sem,
            sem,
            pltpu.SemaphoreType.REGULAR((HOPS + 1,)),
            sem,
            sem((CH, 2)),
            sem,
            sem,
            sem((2,)),
            sem((2,)),
            sem,
            sem((2,)),
            sem,
            sem((6,)),
            sem((6,)),
            sem,
            sem,
        ],
        compiler_params=pltpu.CompilerParams(
            collective_id=0, has_side_effects=True, vmem_limit_bytes=54400 * 1024
        ),
    )(*[pltpu.with_memory_space_constraint(a, pltpu.HBM) for a in (orbitals, partial_bands, core_density)])


def solution(mesh):
    in_specs = (P("spin", "band", "grid", None, None), P("spin", None), P("grid", None, None))
    out_specs = P("spin", "grid", "band", None)

    return jax.shard_map(
        per_device, mesh=mesh, in_specs=in_specs, out_specs=out_specs, check_vma=False
    )
```

```python
import math

import jax
import jax.numpy as jnp
from jax import lax
from jax.experimental import pallas as pl
from jax.experimental.pallas import tpu as pltpu
from jax.sharding import PartitionSpec as P

KAPPA = 0.804
MU_X = 0.2195149727645171
BETA = 0.06672455060314922
GAMMA = (1.0 - math.log(2.0)) / math.pi**2
FZ_NORM = 2.0 ** (4.0 / 3.0) - 2.0
FPP_ZERO = 1.709921

MESH = pl.DeviceIdType.MESH
F32 = jnp.float32
N = 128
XR = 16
NX4 = 4
NZ4 = 4
GY = 4
GRID = 2 * GY
BAND = NX4 * NZ4
YB = N // BAND
YQ = N // NX4
CH = 3
HOPS = 5


def derivative_matrix():
    k = lax.broadcasted_iota(jnp.int32, (N, N), 0) - lax.broadcasted_iota(jnp.int32, (N, N), 1)
    far = jnp.abs(k)
    near = jnp.minimum(far, N - far)
    angle = (math.pi / N) * jnp.maximum(near, 1).astype(F32)
    size = (math.pi / N) * jnp.cos(angle) / jnp.sin(angle)
    flips = (k < 0).astype(jnp.int32) + (far > N // 2).astype(jnp.int32) + (far & 1)
    signed = jnp.where((flips & 1) == 1, -size, size)
    return jnp.where(k == 0, 0.0, signed)


def pw_fit(r, root, amp, alpha, b1, b2, b3, b4):
    denom = (2.0 * amp) * (root * (b1 + root * (b2 + root * (b3 + root * b4))))
    slope = (2.0 * amp) * (0.5 * b1 / root + (b2 + root * (1.5 * b3 + root * (2.0 * b4))))
    log = jnp.log(1.0 + 1.0 / denom)
    front = (-2.0 * amp) * (1.0 + alpha * r)
    value = front * log
    deriv = (-2.0 * amp * alpha) * log - front * slope / (denom * (denom + 1.0))
    return value, deriv


def cbrt(x):
    return jnp.exp(jnp.log(x) * (1.0 / 3.0))


def xc_prepare(own, other):
    total = own + other
    inv_n = 1.0 / total
    c_own = cbrt(own)
    c_other = cbrt(other)
    c_tot = cbrt(total)
    inv_c = 1.0 / c_tot
    double = 2.0 * own
    kf = (6.0 * math.pi**2) ** (1.0 / 3.0) * c_own
    inv_kn = 1.0 / (kf * double)
    two13 = 2.0 ** (1.0 / 3.0)
    plus = double * inv_n
    minus = 2.0 * other * inv_n
    zeta = (own - other) * inv_n
    plus13 = two13 * c_own * inv_c
    minus13 = two13 * c_other * inv_c
    radius = (3.0 / (4.0 * math.pi)) ** (1.0 / 3.0) * inv_c
    root = jnp.sqrt(radius)
    ec0, ec0_r = pw_fit(radius, root, 0.031091, 0.2137, 7.5957, 3.5876, 1.6382, 0.49294)
    ec1, ec1_r = pw_fit(radius, root, 0.015545, 0.20548, 14.1189, 6.1977, 3.3662, 0.62517)
    ac, ac_r = pw_fit(radius, root, 0.016887, 0.11125, 10.357, 3.6231, 0.88026, 0.49671)
    fz = (plus * plus13 + minus * minus13 - 2.0) * (1.0 / FZ_NORM)
    fz_d = (4.0 / 3.0 / FZ_NORM) * (plus13 - minus13)
    z2 = zeta * zeta
    z3 = z2 * zeta
    z4 = z2 * z2
    w1 = (-1.0 / FPP_ZERO) * (1.0 - z4)
    diff = ec1 - ec0
    mix = ac * w1 + diff * z4
    ec = ec0 + fz * mix
    ec_r = ec0_r + fz * (ac_r * w1 + (ec1_r - ec0_r) * z4)
    ec_z = fz_d * mix + 4.0 * z3 * fz * (ac * (1.0 / FPP_ZERO) + diff)
    phi = 0.5 * (plus13 * plus13 + minus13 * minus13)
    phi_d = (1.0 / 3.0) * (1.0 / plus13 - 1.0 / minus13)
    inv_phi = 1.0 / phi
    gp3 = GAMMA * phi * phi * phi
    kf_tot = (3.0 * math.pi**2) ** (1.0 / 3.0)
    tfac = (math.pi / (16.0 * kf_tot)) * inv_phi * inv_phi * inv_c * inv_n * inv_n
    inv_gp3 = (1.0 / GAMMA) * inv_phi * inv_phi * inv_phi
    ex = jnp.exp(-ec * inv_gp3)
    amp = (BETA / GAMMA) / (ex - 1.0)
    amp_ec = amp * amp * ex * (GAMMA / BETA) * inv_gp3
    drift = (1.0 / 3.0) * radius * ec_r
    return kf, inv_kn, ec, drift, ec_z, minus, gp3, tfac, amp, amp_ec, phi_d * inv_phi, total


PREPARED = 12


def xc_derivs(prepared, s_own, s_mix, s_other):
    kf, inv_kn, ec, drift, ec_z, minus, gp3, tfac, amp, amp_ec, phi_r, total = prepared
    s2 = s_own * inv_kn * inv_kn
    inv_den = 1.0 / (1.0 + (MU_X / KAPPA) * s2)
    enh = (1.0 + KAPPA) - KAPPA * inv_den
    enh_d = MU_X * inv_den * inv_den
    dn_x = (-1.0 / math.pi) * kf * (enh - 2.0 * s2 * enh_d)
    ds_x = (-3.0 / (8.0 * math.pi)) * enh_d * inv_kn
    sigma = s_own + 2.0 * s_mix + s_other
    t2 = sigma * tfac
    y = amp * t2
    den = 1.0 + y + y * y
    inv_d = 1.0 / den
    ct = (BETA / GAMMA) * t2
    q = ct * (1.0 + y) * inv_d
    grad_h = gp3 * jnp.log(1.0 + q)
    scale = gp3 / (1.0 + q) * inv_d * inv_d
    h_t = scale * ((BETA / GAMMA) * (1.0 + 2.0 * y))
    h_a = -scale * (ct * t2) * (y * (2.0 + y))
    h_ec = h_a * amp_ec
    one_ec = 1.0 + h_ec
    e_n = ec + grad_h - drift * one_ec - (7.0 / 3.0) * t2 * h_t
    e_z = ec_z * one_ec + phi_r * (3.0 * (grad_h - ec * h_ec) - 2.0 * t2 * h_t)
    dn = dn_x + e_n + e_z * minus
    ds_c = total * h_t * tfac
    return dn, ds_x + ds_c, 2.0 * ds_c


def kernel(
    orb_hbm, bands_hbm, core_hbm, out_ref,
    orb, dmat_ref, lane_ref, bands_ref, part, core, x_in, x_out, summed, z_in, zf_in, zf_sum, xf_in,
    dens, dens_o, prepared, grad, grad_o, flux, turned, x_line, x_line_n, x_res, x_res_n, x_back, y_line, y_line_n, y_res, y_res_n, y_back, base, final, x_fin, y_fin,
    orb_sem, core_sem, bands_sem, hop_sem, xs_sem, xr_sem, zs_sem, zr_sem, fs_sem, fr_sem,
    ps_sem, pr_sem, ys_sem, yr_sem, gs_sem, gr_sem, bs_sem, br_sem,
):
    spin = lax.axis_index("spin")
    band = lax.axis_index("band")
    grid = lax.axis_index("grid")
    bx, bz = band // NZ4, lax.rem(band, NZ4)
    gz, gy = grid // GY, lax.rem(grid, GY)

    def half_of(z):
        q = z // 2
        return 3 * q + z * (1 - 2 * q)

    q, h, e = bz // 2, half_of(bz), lax.rem(bz, 2)
    member = 2 * bx + q
    partner = (1 - spin, band, grid)

    def at_band(x, z, core=spin):
        return (core, lax.rem(x, NX4) * NZ4 + lax.rem(z, NZ4), grid)

    def copy(src, dst, send_sem, recv_sem, device):
        return pltpu.make_async_remote_copy(
            src_ref=src, dst_ref=dst, send_sem=send_sem, recv_sem=recv_sem,
            device_id=device, device_id_type=MESH,
        )

    def send(*args):
        copy(*args).start()

    def sent(like, send_sem):
        copy(like, like, send_sem, send_sem, (spin, band, grid)).wait_send()

    def arrived(like, recv_sem):
        copy(like, like, recv_sem, recv_sem, (spin, band, grid)).wait_recv()

    def rows_at(start, count):
        return pl.ds(pl.multiple_of(start, 8), count)

    bands_copy = pltpu.make_async_copy(bands_hbm, bands_ref, bands_sem)
    bands_copy.start()
    z_all = 2 * bz + gz
    near = [at_band(bx + 1, bz), at_band(bx + 3, bz)]
    near += [(spin, band, gz * GY + lax.rem(gy + d, GY)) for d in (1, 3)]
    for d in (1, 7):
        z = lax.rem(z_all + d, 8)
        near += [(spin, bx * NZ4 + z // 2, lax.rem(z, 2) * GY + gy)]
    barrier = pltpu.get_barrier_semaphore()
    across = [(1 - spin, *peer[1:]) for peer in near]
    aside = [at_band(bx, bz + d) for d in (1, 3)]
    entry = (*near, *across, partner, *aside)
    for peer in entry:
        pl.semaphore_signal(barrier, inc=1, device_id=peer, device_id_type=MESH)

    def y_of(r):
        return pl.multiple_of(lax.rem(bx + r, NX4) * YQ, YQ)

    def y_at(r):
        return pl.ds(r * YQ, YQ)

    def load(k, cs, r):
        for c in cs:
            for half in range(2):
                pltpu.make_async_copy(
                    orb_hbm.at[0, :, pl.ds(8 * half + 2 * c, 2), pl.ds(y_of(r), YQ), :],
                    orb.at[:, c, half, :, y_at(r), :],
                    orb_sem.at[k],
                ).start()

    def loaded(k, window):
        pltpu.make_async_copy(window, window, orb_sem.at[k]).wait()

    load(0, (0,), 2)
    for r in range(NX4):
        load(2, (3,), r)
    load(1, (1, 2), 2)
    for k, r in ((3, 1), (4, 3), (5, 0)):
        load(k, (0, 1, 2), r)
    core_copy = pltpu.make_async_copy(
        core_hbm.at[rows_at(8 * h, 8), rows_at(YQ * bx + 16 * q, 16), :], core, core_sem
    )
    core_copy.start()

    with jax.named_scope("first_piece"):
        bands_copy.wait()
        first = bands_ref[0, 0]
        last = first + bands_ref[0, 1]
        weights = []
        for b in range(8):
            ident = band * 8 + b
            weights.append(jnp.where((ident >= first) & (ident < last), 0.5, 1.0).astype(F32))

    def density(c, r):
        acc = None
        for b in range(8):
            v = orb[b, c, :, :, r * YQ : (r + 1) * YQ, :].astype(F32)
            term = weights[b] * (v * v)
            acc = term if acc is None else acc + term
        part[r, c] = acc

    plus, minus = at_band(bx + 1, bz), at_band(bx + 3, bz)

    def x_send(stream, c, src):
        target = minus if stream % 2 else plus
        send(src, x_in.at[c, stream], xs_sem, xr_sem.at[c, int(stream > 1)], target)

    def far(c):
        x_send(0, c, part.at[2, c, 0])
        x_send(1, c, part.at[2, c, 1])

    def direct(c):
        x_send(2, c, part.at[1, c, 1])
        x_send(3, c, part.at[3, c, 0])

    def relay(c):
        arrived(x_in.at[c, 0:2], xr_sem.at[c, 0])
        for side, r in ((0, 1), (1, 3)):
            x_out[side, c] = part[r, c, side] + x_in[c, side]
            x_send(4 + side, c, x_out.at[side, c])

    def z_targets(ds, core):
        for d in ds:
            z = lax.rem(bz + d, NZ4)
            yield d, half_of(z), rows_at(16 * (z // 2), 16), at_band(bx, z, core)

    def finish(c):
        arrived(x_in.at[c, 2:6], xr_sem.at[c, 1])
        if c == 0:
            hear(3)
        summed[c, 0] = part[0, c, 0] + x_in[c, 4] + x_in[c, 3]
        summed[c, 1] = part[0, c, 1] + x_in[c, 5] + x_in[c, 2]
        for slot, half, ys, device in z_targets((2, 1, 3, 0), 1 - spin):
            send(summed.at[c, half, :, ys, :], z_in.at[slot, c], zs_sem, zr_sem, device)

    def z_first(ds):
        for slot, half, ys, device in z_targets(ds, spin):
            send(part.at[:, 3, half, :, ys, :], zf_in.at[slot - 1], fs_sem.at[0], fr_sem.at[0], device)

    def dmat_table():
        table = derivative_matrix()
        hi = table.astype(jnp.bfloat16)
        lo = (table - hi.astype(F32)).astype(jnp.bfloat16)
        dmat_ref[...] = jnp.concatenate([hi, hi, lo], 1)
        lane_ref[...] = jnp.concatenate([hi, lo, hi], 0)

    def tell(k):
        for peer in near:
            pl.semaphore_signal(hop_sem.at[k - 1], inc=1, device_id=peer, device_id_type=MESH)

    def hear(k):
        pl.semaphore_wait(hop_sem.at[k - 1], len(near))
        if k < HOPS:
            tell(k + 1)

    loaded(0, orb.at[:, 0, :, :, y_at(2), :])
    density(0, 2)
    with jax.named_scope("barrier"):
        pl.semaphore_wait(barrier, len(entry))
    with jax.named_scope("rs_head"):
        far(0)
        for peer in aside:
            pl.semaphore_signal(hop_sem.at[HOPS], inc=1, device_id=peer, device_id_type=MESH)
        tell(1)
        loaded(2, orb.at[:, 3])
        for r in range(NX4):
            density(3, r)
        z_first((1, 3))
        loaded(1, orb.at[:, 1:3, :, :, y_at(2), :])
        density(1, 2)
        far(1)
        density(2, 2)
        far(2)
        loaded(3, orb.at[:, 0:3, :, :, y_at(1), :])
        loaded(4, orb.at[:, 0:3, :, :, y_at(3), :])
        density(0, 1)
        density(0, 3)
        direct(0)
        for c, r in ((1, 1), (1, 3), (2, 1), (2, 3)):
            density(c, r)
    with jax.named_scope("hear_z"):
        pl.semaphore_wait(hop_sem.at[HOPS], 2)
        z_first((2,))
    with jax.named_scope("rs_rest"):
        hear(1)
        loaded(5, orb.at[:, 0:3, :, :, y_at(0), :])
        for c in range(CH):
            density(c, 0)
        dmat_table()
    for c in range(CH):
        with jax.named_scope(f"relay{c}"):
            relay(c)
        if c + 1 < CH:
            direct(c + 1)
    core_copy.wait()
    with jax.named_scope("hear2"):
        hear(2)
    for c in range(CH):
        with jax.named_scope(f"finish{c}"):
            finish(c)

    y_mine = rows_at(16 * q, 16)
    with jax.named_scope("zf_wait"):
        arrived(zf_in, fr_sem.at[0])
        zf_sum[...] = part[:, 3, h, :, y_mine, :] + zf_in[0] + zf_in[1] + zf_in[2]
        for r in (2, 1, 3, 0):
            send(
                zf_sum.at[r], xf_in.at[r], fs_sem.at[1], fr_sem.at[1],
                at_band(bx + r, bz, 1 - spin),
            )
    with jax.named_scope("hear4"):
        hear(4)
    with jax.named_scope("z_wait"):
        arrived(z_in, zr_sem)
    for c in range(CH):
        block = 0.5 * core[2 * c : 2 * c + 2] + z_in[0, c] + z_in[1, c] + z_in[2, c] + z_in[3, c]
        dens[32 * c : 32 * c + 32, :] = block.reshape(32, N)
    with jax.named_scope("hear5"):
        hear(5)
    with jax.named_scope("xf_wait"):
        arrived(xf_in, fr_sem.at[1])
    block = 0.5 * core[2 * CH : 2 * CH + 2] + xf_in[0] + xf_in[1] + xf_in[2] + xf_in[3]
    dens[32 * CH : 32 * CH + 32, :] = block.reshape(32, N)

    def halves(x):
        hi = x.astype(jnp.bfloat16)
        return hi, (x - hi.astype(F32)).astype(jnp.bfloat16)

    def along_rows(x):
        hi, lo = halves(x)
        return jnp.dot(dmat_ref[...], jnp.concatenate([hi, lo, hi], 0), preferred_element_type=F32)

    def along_lanes(x):
        hi, lo = halves(x)
        return jnp.dot(jnp.concatenate([hi, hi, lo], 1), lane_ref[...], preferred_element_type=F32)

    def pass_on(src, dst, send_sem, recv_sem, local):
        if local:
            dst[...] = src[...]
        else:
            send(src, dst, send_sem, recv_sem, partner)

    def y_exchange(src, dst, ks, kr, core, local=False):
        for dx, dq in ((2, 1), (1, 1), (3, 1), (0, 1), (2, 0), (1, 0), (3, 0)):
            x, place = lax.rem(bx + dx, NX4), lax.rem(q + dq, 2)
            z = h + place * (3 - 2 * h)
            send(
                src.at[rows_at(16 * (2 * x + place), 16), :], dst.at[rows_at(16 * member, 16), :],
                ys_sem.at[ks], yr_sem.at[kr], (core, x * NZ4 + z, grid),
            )
        mine = rows_at(16 * member, 16)
        pass_on(src.at[mine, :], dst.at[mine, :], ys_sem.at[ks], yr_sem.at[kr], local)

    def x_exchange(src, dst, ks, kr, core, local=False, back=False):
        for de in (1, 0):
            for dz in (1, 0):
                for dy in (2, 1, 3, 0):
                    if (de, dz, dy) == (0, 0, 0):
                        continue
                    e2 = lax.rem(e + de, 2)
                    g2 = lax.rem(gz + dz, 2) * GY + lax.rem(gy + dy, GY)
                    z = 2 * q + e2
                    there, here = 8 * e2 + g2, 2 * grid + h
                    if back:
                        there, here = 2 * g2 + half_of(z), 8 * e + grid
                    send(
                        src.at[rows_at(8 * there, 8), :], dst.at[rows_at(8 * here, 8), :],
                        gs_sem.at[ks], gr_sem.at[kr], (core, bx * NZ4 + z, g2),
                    )
        mine = (2 * grid + h, 8 * e + grid)
        there, here = mine if back else mine[::-1]
        there, here = rows_at(8 * there, 8), rows_at(8 * here, 8)
        pass_on(src.at[there, :], dst.at[here, :], gs_sem.at[ks], gr_sem.at[kr], local)

    def y_wait(dst, k, local=False):
        arrived(dst.at[0 : N - 16, :] if local else dst, yr_sem.at[k])

    def x_wait(dst, k, local=False):
        arrived(dst.at[0 : N - 8, :] if local else dst, gr_sem.at[k])

    def out_y(src, core, local=False):
        xr = rows_at(8 * (8 * h + member), 8)
        for dx in (2, 1, 3, 0):
            for dz in (2, 1, 3, 0):
                if (dx, dz) != (0, 0):
                    b2 = lax.rem(bx + dx, NX4) * NZ4 + lax.rem(bz + dz, NZ4)
                    send(
                        src.at[rows_at(8 * b2, 8), :], y_fin.at[xr, :],
                        ys_sem.at[3], yr_sem.at[3], (core, b2, grid),
                    )
        pass_on(src.at[rows_at(8 * band, 8), :], y_fin.at[xr, :], ys_sem.at[3], yr_sem.at[3], local)

    def out_x(src, core, local=False):
        mine = rows_at(XR * grid, XR)
        for dz, dy in ((1, 2), (1, 1), (1, 3), (0, 2), (1, 0), (0, 1), (0, 3)):
            g2 = lax.rem(gz + dz, 2) * GY + lax.rem(gy + dy, GY)
            send(
                src.at[rows_at(XR * g2, XR), :], x_fin.at[mine, :],
                gs_sem.at[3], gr_sem.at[3], (core, band, g2),
            )
        pass_on(src.at[mine, :], x_fin.at[mine, :], gs_sem.at[3], gr_sem.at[3], local)

    def turn(src, dst):
        for t in range(16):
            dst[8 * t : 8 * t + 8, :] = src[pl.ds(t, 8, stride=16), :]

    with jax.named_scope("fwd0"):

        @pl.when(spin == 0)
        def _():
            y_exchange(dens, y_line.at[0], 0, 0, 1)
            turn(dens, turned.at[0])
            x_exchange(turned.at[0], x_line.at[0], 0, 0, 1)

        @pl.when(spin == 1)
        def _():
            y_exchange(dens, y_line_n.at[0], 4, 4, 1, local=True)
            turn(dens, turned.at[0])
            x_exchange(turned.at[0], x_line_n.at[0], 4, 4, 1, local=True)

        send(dens, dens_o, ps_sem, pr_sem.at[0], partner)
        grad[2] = -along_lanes(dens[...])
        send(grad.at[2], grad_o.at[2], ps_sem, pr_sem.at[1], partner)
    with jax.named_scope("drain0"):
        sent(part.at[0:3, 0:CH], xs_sem)
        sent(z_in, zs_sem)
        sent(zf_in, fs_sem.at[0])
        sent(xf_in, fs_sem.at[1])
    with jax.named_scope("prepare"):
        arrived(dens_o, pr_sem.at[0])
        step = 16
        for i in range(0, N, step):
            rows = slice(i, i + step)
            for k, known in enumerate(xc_prepare(dens_o[rows, :], dens[rows, :])):
                prepared[k, rows, :] = known
    with jax.named_scope("lines0"):

        @pl.when(spin == 1)
        def _():
            y_wait(y_line.at[0], 0)
            y_res[0] = along_rows(y_line[0])
            y_exchange(y_res.at[0], y_back, 1, 1, 0)
            x_wait(x_line.at[0], 0)
            x_res[0] = along_rows(x_line[0])
            x_exchange(x_res.at[0], x_back, 1, 1, 0, back=True)
            y_wait(y_line_n.at[0], 4, local=True)
            y_res_n[0] = along_rows(y_line_n[0])
            y_exchange(y_res_n.at[0], y_back, 1, 1, 1, local=True)
            x_wait(x_line_n.at[0], 4, local=True)
            x_res_n[0] = along_rows(x_line_n[0])
            x_exchange(x_res_n.at[0], x_back, 1, 1, 1, local=True, back=True)

    with jax.named_scope("y_back0"):
        pl.when(spin == 0)(lambda: y_wait(y_back, 1))
        pl.when(spin == 1)(lambda: y_wait(y_back, 1, local=True))
        send(y_back, grad_o.at[1], ps_sem, pr_sem.at[1], partner)
    with jax.named_scope("x_back0"):
        pl.when(spin == 0)(lambda: x_wait(x_back, 1))
        pl.when(spin == 1)(lambda: x_wait(x_back, 1, local=True))
        for i in range(8):
            grad[0, 16 * i : 16 * i + 16, :] = x_back[pl.ds(i, 16, stride=8), :]
    with jax.named_scope("swap"):
        send(grad.at[0], grad_o.at[0], ps_sem, pr_sem.at[1], partner)
        arrived(grad_o, pr_sem.at[1])

    def flux_row(m):
        z = h if m % 2 == 0 else 3 - h
        src, mine = flux.at[1, 16 * m : 16 * m + 16, :], rows_at(16 * member, 16)
        device = (1, m // 2 * NZ4 + z, grid)

        @pl.when(spin == 0)
        def _():
            send(src, y_line.at[1, mine, :], ys_sem.at[2], yr_sem.at[2], device)

        @pl.when((spin == 1) & (member != m))
        def _():
            send(src, y_line_n.at[1, mine, :], ys_sem.at[5], yr_sem.at[5], device)

    with jax.named_scope("xc"):
        for i in range(0, N, step):
            rows = slice(i, i + step)
            o = (grad[0, rows, :], y_back[rows, :], grad[2, rows, :])
            g = (grad_o[0, rows, :], grad_o[1, rows, :], grad_o[2, rows, :])
            s_own = g[0] * g[0] + g[1] * g[1] + g[2] * g[2]
            s_mix = g[0] * o[0] + g[1] * o[1] + g[2] * o[2]
            s_other = o[0] * o[0] + o[1] * o[1] + o[2] * o[2]
            known = [prepared[k, rows, :] for k in range(PREPARED)]
            dn, ds, dm = xc_derivs(known, s_own, s_mix, s_other)
            for a in range(3):
                flux[a, rows, :] = 2.0 * ds * g[a] + dm * o[a]
            flux[3, rows, :] = dn
            if i % 64 == 48:
                for m in range(i // 16 - 3, i // 16 + 1):
                    flux_row(m)

    with jax.named_scope("fwd1"):

        @pl.when(spin == 0)
        def _():
            turn(flux.at[0], turned.at[1])
            x_exchange(turned.at[1], x_line.at[1], 2, 2, 1)

        @pl.when(spin == 1)
        def _():
            mine = rows_at(16 * member, 16)
            y_line_n[1, mine, :] = flux[1, mine, :]
            turn(flux.at[0], turned.at[1])
            x_exchange(turned.at[1], x_line_n.at[1], 5, 5, 1, local=True)

        base[...] = (flux[3] + along_lanes(flux[2])).reshape(8, 16, N)
        there = lax.rem(e + 1, 2)
        send(
            base.at[:, rows_at(8 * there, 8), :], final.at[h],
            bs_sem, br_sem, (spin, bx * NZ4 + 2 * q + there, grid),
        )
        final[h] = base[:, rows_at(8 * e, 8), :]
    with jax.named_scope("drain1"):

        @pl.when(spin == 0)
        def _():
            sent(y_line.at[0], ys_sem.at[0])
            sent(x_line.at[0], gs_sem.at[0])

        @pl.when(spin == 1)
        def _():
            for k in (1, 4):
                sent(y_line.at[0, 0 : N - 16, :], ys_sem.at[k])
                sent(x_line.at[0, 0 : N - 8, :], gs_sem.at[k])
            sent(y_line.at[0], ys_sem.at[1])
            sent(x_line.at[0], gs_sem.at[1])

        sent(grad_o, ps_sem)
        sent(dens_o, ps_sem)
    with jax.named_scope("lines1"):

        @pl.when(spin == 1)
        def _():
            y_wait(y_line_n.at[1], 5, local=True)
            y_res_n[1] = along_rows(y_line_n[1])
            out_y(y_res_n.at[1], 1, local=True)
            x_wait(x_line_n.at[1], 5, local=True)
            x_res_n[1] = along_rows(x_line_n[1])
            out_x(x_res_n.at[1], 1, local=True)
            y_wait(y_line.at[1], 2)
            y_res[1] = along_rows(y_line[1])
            out_y(y_res.at[1], 0)
            x_wait(x_line.at[1], 2)
            x_res[1] = along_rows(x_line[1])
            out_x(x_res.at[1], 0)

    with jax.named_scope("drain2"):

        @pl.when(spin == 0)
        def _():
            sent(y_line.at[0], ys_sem.at[2])
            sent(x_line.at[0], gs_sem.at[2])

        @pl.when(spin == 1)
        def _():
            sent(y_line.at[0, 0 : N - 16, :], ys_sem.at[5])
            sent(x_line.at[0, 0 : N - 8, :], gs_sem.at[5])
            sent(y_line.at[0, 0 : N - YB, :], ys_sem.at[3])
            sent(x_line.at[0, 0 : N - XR, :], gs_sem.at[3])
            sent(y_line.at[0], ys_sem.at[3])
            sent(x_line.at[0], gs_sem.at[3])

        sent(final.at[0], bs_sem)
        arrived(final.at[0], br_sem)
    with jax.named_scope("x_back1"):
        pl.when(spin == 0)(lambda: arrived(x_fin, gr_sem.at[3]))
        pl.when(spin == 1)(lambda: arrived(x_fin.at[0 : N - XR, :], gr_sem.at[3]))
        for i in range(XR):
            out_ref[0, i] = final[i // 8, i % 8] - x_fin[pl.ds(i, YB, stride=XR), :]
    with jax.named_scope("y_back1"):
        pl.when(spin == 0)(lambda: arrived(y_fin, yr_sem.at[3]))
        pl.when(spin == 1)(lambda: arrived(y_fin.at[0 : N - YB, :], yr_sem.at[3]))
    with jax.named_scope("tail"):
        out_ref[0] = out_ref[0] - y_fin[...].reshape(XR, YB, N)


def per_device(orbitals, partial_bands, core_density):
    vm = pltpu.VMEM
    sem = pltpu.SemaphoreType.DMA
    anyspace = pl.BlockSpec(memory_space=pltpu.HBM)
    return pl.pallas_call(
        kernel,
        out_shape=jax.ShapeDtypeStruct((1, XR, YB, N), F32),
        in_specs=[anyspace] * 3,
        out_specs=pl.BlockSpec(memory_space=pltpu.VMEM),
        scratch_shapes=[
            vm((8, CH + 1, 2, 2, N, N), jnp.bfloat16),
            vm((N, 3 * N), jnp.bfloat16),
            vm((3 * N, N), jnp.bfloat16),
            pltpu.SMEM((1, 2), jnp.int32),
            vm((NX4, CH + 1, 2, 2, YQ, N), F32),
            vm((8, 16, N), F32),
            vm((CH, 6, 2, YQ, N), F32),
            vm((2, CH, 2, YQ, N), F32),
            vm((CH, 2, 2, YQ, N), F32),
            vm((NZ4, CH, 2, 16, N), F32),
            vm((NZ4 - 1, NX4, 2, 16, N), F32),
            vm((NX4, 2, 16, N), F32),
            vm((NX4, 2, 16, N), F32),
            vm((N, N), F32),
            vm((N, N), F32),
            vm((PREPARED, N, N), F32),
            vm((3, N, N), F32),
            vm((3, N, N), F32),
            vm((4, N, N), F32),
            vm((2, N, N), F32),
            vm((2, N, N), F32),
            vm((2, N, N), F32),
            vm((2, N, N), F32),
            vm((2, N, N), F32),
            vm((N, N), F32),
            vm((2, N, N), F32),
            vm((2, N, N), F32),
            vm((2, N, N), F32),
            vm((2, N, N), F32),
            vm((N, N), F32),
            vm((8, 16, N), F32),
            vm((2, 8, YB, N), F32),
            vm((N, N), F32),
            vm((N, N), F32),
            sem((6,)),
            sem,
            sem,
            pltpu.SemaphoreType.REGULAR((HOPS + 1,)),
            sem,
            sem((CH, 2)),
            sem,
            sem,
            sem((2,)),
            sem((2,)),
            sem,
            sem((2,)),
            sem((6,)),
            sem((6,)),
            sem((6,)),
            sem((6,)),
            sem,
            sem,
        ],
        compiler_params=pltpu.CompilerParams(
            collective_id=0, has_side_effects=True, vmem_limit_bytes=54400 * 1024
        ),
    )(*[pltpu.with_memory_space_constraint(a, pltpu.HBM) for a in (orbitals, partial_bands, core_density)])


def solution(mesh):
    in_specs = (P("spin", "band", "grid", None, None), P("spin", None), P("grid", None, None))
    out_specs = P("spin", "grid", "band", None)

    return jax.shard_map(
        per_device, mesh=mesh, in_specs=in_specs, out_specs=out_specs, check_vma=False
    )
```
